32 devices in a mesh: grp: 4 (over y, x), tile: 8 (over z, core).
Axes of the slice: x: 2, y: 2, z: 4, core: 2. Of those that a mesh axis runs over, the one named last changes fastest.
Arguments:
- base_rhs: float32 [1024, 4096], P('grp', 'tile'), may hold values from -6 to 6
- depth: float32 [1024, 4096], P('grp', 'tile'), may hold values from 0.25 to 2
- ssh_prev: float32 [1024, 4096], P('grp', 'tile'), may hold values from -6 to 6
- currents: float32 [2, 1024, 4096], P(None, 'grp', 'tile'), may hold values from -3 to 3
- land_blocks: int32 [128, 512], P('grp', 'tile'), may hold values 0 or 1
- ice_thick: float32 [2, 256, 4096], P(None, 'grp', 'tile'), may hold values from 0.25 to 4
- ice_blocks: int32 [2, 32, 512], P(None, 'grp', 'tile'), may hold values 0 or 1
- ice_vel: float32 [2, 2, 256, 4096], P(None, None, 'grp', 'tile'), may hold values from -3 to 3
- ice_stress: float32 [3, 2, 256, 4096], P(None, None, 'grp', 'tile'), may hold values from -5 to 5
- wind: float32 [2, 2, 256, 4096], P(None, None, 'grp', 'tile'), may hold values from -6 to 6
Outputs:
- ssh: float32 [1024, 4096], P('grp', 'tile')
- ice_vel_out: float32 [2, 2, 256, 4096], P(None, None, 'grp', 'tile')
- ice_stress_out: float32 [3, 2, 256, 4096], P(None, None, 'grp', 'tile')
The draws below stay inside these ranges and needn't reach their ends.
All inputs are finite; a program needn't handle non-finite values. No bound on the sum of `land_blocks` or of `ice_blocks` on one device may be relied on, other than what follows from the above.
Results may differ from the reference program's by a relative error of at most 0.0001.
Values sent between devices are 32-bit elements; how exact they have to be, the bound alone decides.
A program may use at most 64 MiB of HBM per device.

```python
import math
import jax
import jax.numpy as jnp

BS = 8
NSUB = 8
ITERS = 3
NX = 1024
NY = 4096
NXI = 256


def set_ends(values, own_key, least, largest):
    index_at = [jax.random.randint(jax.random.fold_in(own_key, axis), (), 0, length) for axis, length in enumerate(values.shape)]
    widest = values.shape.index(max(values.shape))
    beside = index_at[:widest] + [(index_at[widest] + 1) % values.shape[widest]] + index_at[widest + 1:]
    return values.at[tuple(index_at)].set(least).at[tuple(beside)].set(largest)


def level_of(key, extent, split, smallest, high):
    loudness = 1.0
    for position, shards_of in split:
        heights = jax.random.uniform(jax.random.fold_in(jax.random.fold_in(key, 6), position), (shards_of,), jnp.float32, smallest / len(split), high / len(split))
        loudness = loudness * jnp.repeat(jnp.exp(heights), extent[position] // shards_of).reshape((-1,) + (1,) * (len(extent) - 1 - position))
    return loudness


def bell_draw(rng, dims, scale, reach, pieces=(), held_as=jnp.bfloat16):
    level = level_of(rng, dims, pieces, -0.22, 0.18) if pieces else 1.0
    entries = jax.random.normal(rng, dims, jnp.float32) * scale * level
    return jnp.minimum(jnp.maximum(entries, -reach), reach).astype(held_as)


def setup_inputs(seed: int = 0) -> dict:
    key_list = jax.random.split(jax.random.key(seed), 11)
    base_rhs = bell_draw(key_list[0], (NX, NY), 1.0, 6.0, ((0, 4), (1, 8)), jnp.float32)
    depth = jnp.clip(jnp.exp(math.log(2.0) - 2.0794415 * jax.random.uniform(key_list[1], (NX, NY), jnp.float32) ** level_of(key_list[1], (NX, NY), ((0, 4), (1, 8)), -0.2, 0.2)), 0.25, 2.0)
    ssh_prev = bell_draw(key_list[2], (NX, NY), 1.0, 6.0, ((0, 4), (1, 8)), jnp.float32)
    currents = bell_draw(key_list[3], (2, NX, NY), 0.5, 3.0, ((1, 4), (2, 8)), jnp.float32)
    land_blocks = set_ends((jax.random.randint(key_list[4], (NX // BS, NY // BS), 0, 4) < 3).astype(jnp.int32), jax.random.fold_in(key_list[4], 1), 0, 1)
    ice_thick = jnp.clip(jnp.exp(math.log(4.0) - 2.7725887 * jax.random.uniform(key_list[5], (2, NXI, NY), jnp.float32) ** level_of(key_list[5], (2, NXI, NY), ((1, 4), (2, 8)), -0.2, 0.2)), 0.25, 4.0)
    ice_blocks = set_ends((jax.random.randint(key_list[6], (2, NXI // BS, NY // BS), 0, 4) < 3).astype(jnp.int32), jax.random.fold_in(key_list[6], 1), 0, 1)
    ice_vel = bell_draw(key_list[7], (2, 2, NXI, NY), 0.5, 3.0, ((2, 4), (3, 8)), jnp.float32)
    ice_stress = bell_draw(key_list[8], (3, 2, NXI, NY), 1.0, 5.0, ((2, 4), (3, 8)), jnp.float32)
    wind = bell_draw(key_list[9], (2, 2, NXI, NY), 1.0, 6.0, ((2, 4), (3, 8)), jnp.float32)
    return dict(base_rhs=base_rhs, depth=depth, ssh_prev=ssh_prev, currents=currents, land_blocks=land_blocks, ice_thick=ice_thick, ice_blocks=ice_blocks, ice_vel=ice_vel, ice_stress=ice_stress, wind=wind)


DAMP = 0.05
RELAX = 0.2
STRENGTH = 0.5
DRAG = 1.0
STEP = 0.5

def strain_rates(u_pad, v_pad):
    du_dx = u_pad[..., 1:, :-1] - u_pad[..., :-1, :-1]
    du_dy = u_pad[..., :-1, 1:] - u_pad[..., :-1, :-1]
    dv_dx = v_pad[..., 1:, :-1] - v_pad[..., :-1, :-1]
    dv_dy = v_pad[..., :-1, 1:] - v_pad[..., :-1, :-1]
    return (du_dx + dv_dy, du_dx - dv_dy, du_dy + dv_dx)

def relax_stress(previous, strength, div_rate, tens_rate, shear_rate):
    deformation = jnp.sqrt(div_rate * div_rate + tens_rate * tens_rate + shear_rate * shear_rate + 1.0)
    relax_scale = 1.0 / (1.0 + RELAX)
    div_part = (previous[0] + RELAX * strength * (div_rate / deformation - 1.0)) * relax_scale
    tens_part = (previous[1] + RELAX * strength * tens_rate / deformation) * relax_scale
    shear_part = (previous[2] + RELAX * strength * shear_rate / deformation) * relax_scale
    return jnp.stack([div_part, tens_part, shear_part])

def along_rows(field):
    return field[..., 1:, 1:] - field[..., :-1, 1:]

def along_cols(field):
    return field[..., 1:, 1:] - field[..., 1:, :-1]

def stress_force(stress_pad):
    force_x = 0.5 * along_rows(stress_pad[0] + stress_pad[1]) + along_cols(stress_pad[2])
    force_y = 0.5 * along_cols(stress_pad[0] - stress_pad[1]) + along_rows(stress_pad[2])
    return jnp.stack([force_x, force_y])

def momentum(velocity, force, ice_mass, ice_cover, wind, ocean_flow):
    return ice_cover * (ice_mass * velocity + STEP * (force + wind + DRAG * ocean_flow)) / (ice_mass + STEP * DRAG)

def face_weights(depth_pad):
    centre = depth_pad[1:-1, 1:-1]
    return (centre * depth_pad[2:, 1:-1], centre * depth_pad[:-2, 1:-1], centre * depth_pad[1:-1, 2:], centre * depth_pad[1:-1, :-2])

def apply_operator(field_pad, weights):
    field = field_pad[1:-1, 1:-1]
    north_weight, south_weight, east_weight, west_weight = weights
    return DAMP * field + north_weight * (field - field_pad[2:, 1:-1]) + south_weight * (field - field_pad[:-2, 1:-1]) + east_weight * (field - field_pad[1:-1, 2:]) + west_weight * (field - field_pad[1:-1, :-2])

def expand(blocks):
    return jnp.repeat(jnp.repeat(blocks, BS, axis=-2), BS, axis=-1).astype(jnp.float32)

def reference(base_rhs, depth, ssh_prev, currents, land_blocks, ice_thick, ice_blocks, ice_vel, ice_stress, wind):
    wet_cells = expand(land_blocks)
    ice_cover = expand(ice_blocks)
    strength = STRENGTH * ice_thick * ice_cover
    ice_mass = ice_thick * ice_cover + 1.0
    ocean_flow = jnp.stack([currents[:, :NXI], currents[:, NX - NXI:]], axis=1)
    velocity = ice_vel
    stress = ice_stress
    for subcycle in range(NSUB):
        vel_pad = jnp.pad(velocity, ((0, 0), (0, 0), (1, 1), (1, 1)))
        strain = strain_rates(vel_pad[0], vel_pad[1])
        div_rate = strain[0][:, 1:, 1:]
        tens_rate = strain[1][:, 1:, 1:]
        shear_rate = strain[2][:, 1:, 1:]
        stress = relax_stress(stress, strength, div_rate, tens_rate, shear_rate)
        stress_pad = jnp.pad(stress, ((0, 0), (0, 0), (1, 0), (1, 0)))
        velocity = momentum(velocity, stress_force(stress_pad), ice_mass, ice_cover, wind, ocean_flow)
    ice_drag = DRAG * ice_cover * (velocity - ocean_flow)
    ocean_drag = jnp.zeros((2, NX, NY), jnp.float32)
    ocean_drag = ocean_drag.at[:, :NXI].set(ice_drag[:, 0]).at[:, NX - NXI:].set(ice_drag[:, 1])
    forcing_pad = jnp.pad(jnp.stack([ocean_drag[0], ocean_drag[1], depth * wet_cells]), ((0, 0), (1, 1), (1, 1)))
    spread = forcing_pad[0, 1:-1, 1:-1] - forcing_pad[0, :-2, 1:-1] + (forcing_pad[1, 1:-1, 1:-1] - forcing_pad[1, 1:-1, :-2])
    forcing = wet_cells * (base_rhs + spread)
    weights = face_weights(forcing_pad[2])
    diagonal = DAMP + weights[0] + weights[1] + weights[2] + weights[3]
    solution = ssh_prev
    residual = forcing - apply_operator(jnp.pad(solution, 1), weights)
    precond = residual / diagonal
    direction = precond
    precond_norm = jnp.sum(residual * precond)
    for iteration in range(ITERS):
        applied = apply_operator(jnp.pad(direction, 1), weights)
        step_size = precond_norm / jnp.sum(direction * applied)
        solution = solution + step_size * direction
        residual = residual - step_size * applied
        precond = residual / diagonal
        norm_next = jnp.sum(residual * precond)
        direction = precond + norm_next / precond_norm * direction
        precond_norm = norm_next
    return (solution, velocity, stress)
```

```python
import functools
import math

import jax
import jax.numpy as jnp
from jax import lax
from jax.experimental import pallas as pl
from jax.experimental.pallas import tpu as pltpu
from jax.sharding import PartitionSpec as P

BS = 8
NSUB = 8

DAMP = 0.05
RELAX = 0.2
STRENGTH = 0.5
DRAG = 1.0
STEP = 0.5
KEEP = 1.0 / (1.0 + RELAX)
RATE = math.sqrt(2.0) * RELAX * STRENGTH / (1.0 + RELAX)

MESH = pl.DeviceIdType.MESH
F32 = jnp.float32
T = 8
L = 128
W = 12
TOP = 2 * T
PAD = 2 * T


def lanes(rows, width):
    return lax.broadcasted_iota(jnp.int32, (rows, width), 1)


def above(prev, here):
    row = lax.broadcasted_iota(jnp.int32, here.shape, 0)
    return pltpu.roll(jnp.where(row == T - 1, prev, here), 1, 0)


def turn_right(tiles):
    return [pltpu.roll(x, L - 1, 1) for x in tiles]


def turn_left(tiles):
    return [pltpu.roll(x, 1, 1) for x in tiles]


def join_right(turned):
    lane = lanes(T, L)
    n = len(turned)
    return [jnp.where(lane == L - 1, turned[(j + 1) % n], turned[j]) for j in range(n)]


def join_left(turned):
    lane = lanes(T, L)
    n = len(turned)
    return [jnp.where(lane == 0, turned[(j - 1) % n], turned[j]) for j in range(n)]


def right(tiles):
    return join_right(turn_right(tiles))


def left(tiles):
    return join_left(turn_left(tiles))


def kernel(
    groups,
    tiles,
    base_in,
    depth_in,
    ssh_in,
    cur_in,
    land_ref,
    thick_in,
    ice_ref,
    vel_in,
    stress_in,
    wind_in,
    ssh_out,
    vel_out,
    stress_out,
    vel,
    st,
    wind,
    flow,
    h,
    gn,
    xn,
    bn,
    uu,
    vv,
    sp_p,
    sp_m,
    sp_s,
    kk,
    pp,
    qq,
    ww,
    flow_edge,
    g,
    gx,
    r0,
    x,
    inv,
    gd,
    forcing,
    v0,
    v1,
    v2,
    w0,
    w1,
    w2,
    wet,
    cover,
    pack_s,
    pack_r,
    fpack_s,
    fpack_r,
    opack_s,
    opack_r,
    sp,
    extra,
    red_s,
    red_r,
    red2_s,
    red2_r,
    load_sem,
    flow_send,
    flow_recv,
    row_send,
    row_recv,
    col_send,
    col_recv,
    back_send,
    back_recv,
    edge_send,
    edge_recv,
    red_send,
    red_recv,
    red2_send,
    red2_recv,
    out_sem,
):
    gi = lax.axis_index("grp")
    ti = lax.axis_index("tile")
    rows, cols = thick_in.shape[1], thick_in.shape[2]
    orows = base_in.shape[0]
    end = TOP + rows
    oend = TOP + orows
    own = cols // L
    span = own + 1
    ichunks = rows // T + 2
    ochunks = orows // T + 2

    loads = []

    def load(src, dst):
        copy = pltpu.make_async_copy(src, dst, load_sem.at[len(loads)])
        copy.start()
        loads.append(copy)
        return copy

    load_thick = load(thick_in, h.at[:, TOP:end, :])
    load_depth = load(depth_in, gn.at[TOP:oend, :])
    load_x = load(ssh_in, xn.at[TOP:oend, :])
    load_b = load(base_in, bn.at[TOP:oend, :])
    load_vel = load(vel_in, vel.at[:, :, TOP:end, :])
    load_st = load(stress_in, st.at[:, :, TOP:end, :])
    load_wind = load(wind_in, wind.at[:, :, TOP:end, :])

    def clear(ref, *spans):
        for lo, hi in spans:
            ref[..., lo:hi, :] = jnp.zeros(ref.shape[:-2] + (hi - lo, ref.shape[-1]), F32)

    for ref in (vel, st, wind, flow, h):
        clear(ref, (T, TOP), (end, end + T))
    for ref in (gn, xn, bn):
        clear(ref, (T, TOP), (oend, oend + T))
    for ref in (pack_r, fpack_r, opack_r, forcing):
        ref[...] = jnp.zeros_like(ref)

    barrier = pltpu.get_barrier_semaphore()
    for d in range(1, groups):
        pl.semaphore_signal(
            barrier, inc=1, device_id=(lax.rem(gi + d, groups), ti), device_id_type=MESH
        )
    for d in range(1, tiles):
        pl.semaphore_signal(
            barrier, inc=1, device_id=(gi, lax.rem(ti + d, tiles)), device_id_type=MESH
        )

    for ref in (uu, vv, sp_p, sp_m, sp_s):
        clear(ref, (0, T), (end + T, end + 2 * T))
    for ref in (g, gx, w0, w1, w2):
        clear(ref, (0, T), (oend + T, oend + 2 * T))

    def blocks(ref, out, count):
        width = ref.shape[-1]
        row = lax.broadcasted_iota(jnp.int32, (width, cols), 0)
        spread = (row == lax.shift_right_logical(lanes(width, cols), 3)).astype(F32)
        values = ref[...].reshape((count, width)).astype(F32)
        out[...] = jnp.dot(values, spread, preferred_element_type=F32)

    blocks(land_ref, wet, land_ref.shape[0])
    for c in range(2):
        row = lax.broadcasted_iota(jnp.int32, (cols // BS, cols), 0)
        spread = (row == lax.shift_right_logical(lanes(cols // BS, cols), 3)).astype(F32)
        cover[c] = jnp.dot(ice_ref[c].astype(F32), spread, preferred_element_type=F32)

    pl.semaphore_wait(barrier, groups + tiles - 2)

    homes = (0, groups - 1)
    pieces = ((0, L), (cols - L, cols), (L, cols - L))

    def flow_copy(cap, target, piece):
        lo = max(0, rows * target - T)
        hi = min(rows * groups, rows * target + rows + T)
        start = TOP + lo - rows * target
        first, last = pieces[piece]
        src = cur_in.at[:, lo:hi, first:last]
        dst = flow.at[:, cap, start : start + hi - lo, first:last]
        if target == homes[cap]:
            return pltpu.make_async_copy(src, dst, flow_recv.at[3 * cap + piece])
        return pltpu.make_async_remote_copy(
            src_ref=src,
            dst_ref=dst,
            send_sem=flow_send.at[3 * target + piece],
            recv_sem=flow_recv.at[3 * cap + piece],
            device_id=(target, ti),
            device_id_type=MESH,
        )

    def row_copies(which):
        out = []
        fields = (
            (vel_in, vel, rows, end),
            (stress_in, st, rows, end),
            (wind_in, wind, rows, end),
            (ssh_in, xn, orows, oend),
            (base_in, bn, orows, oend),
            (h, h, None, end),
            (gn, gn, None, oend),
        )
        for k, (src, dst, length, last) in enumerate(fields):
            if k not in which:
                continue
            origin = TOP if length is None else 0
            count = (last - TOP) if length is None else length
            lead = (slice(None),) * (len(src.shape) - 2)
            for way in range(2):
                from_row = origin + count - T if way == 0 else origin
                to_row = TOP - T if way == 0 else last
                out.append(
                    (
                        way,
                        pltpu.make_async_remote_copy(
                            src_ref=src.at[lead + (slice(from_row, from_row + T), slice(0, cols))],
                            dst_ref=dst.at[lead + (slice(to_row, to_row + T), slice(0, cols))],
                            send_sem=row_send.at[2 * k + way],
                            recv_sem=row_recv.at[2 * k + way],
                            device_id=(
                                lax.rem(gi + (1 if way == 0 else groups - 1), groups),
                                ti,
                            ),
                            device_id_type=MESH,
                        ),
                    )
                )
        return out

    def edge(way, index, count):
        sends = index < count - 1 if way == 0 else index > 0
        receives = index > 0 if way == 0 else index < count - 1
        return sends, receives

    def start_all(copies, index, count):
        for way, copy in copies:
            pl.when(edge(way, index, count)[0])(copy.start)

    def receive_all(copies, index, count):
        for way, copy in copies:
            pl.when(edge(way, index, count)[1])(copy.wait_recv)

    early = row_copies((0, 1, 2))
    start_all(early, gi, groups)

    for cap, home in enumerate(homes):

        @pl.when(gi == home)
        def _():
            for piece in range(3):
                flow_copy(cap, home, piece).start()

    load_thick.wait()

    def cover_chunk(k, _):
        for c in range(2):
            at = (c, pl.ds(pl.multiple_of(TOP + k * T, T), T), slice(None))
            h[at] = h[at] * cover[c, pl.ds(k, 1), :]
        return 0

    lax.fori_loop(0, rows // T, cover_chunk, 0, unroll=4)
    late = row_copies((5,))
    start_all(late, gi, groups)

    load_depth.wait()

    def wet_chunk(k, _):
        at = (pl.ds(pl.multiple_of(TOP + k * T, T), T), slice(None))
        gn[at] = gn[at] * wet[pl.ds(k, 1), :]
        return 0

    lax.fori_loop(0, orows // T, wet_chunk, 0, unroll=4)
    orow = row_copies((3, 4, 6))
    start_all(orow, gi, groups)

    for cap, home in enumerate(homes):

        @pl.when(gi == home)
        def _():
            order = sorted((k for k in range(groups) if k != home), key=lambda k: abs(k - home))
            for target in order[1:] + order[:1]:
                for piece in range(3):
                    flow_copy(cap, target, piece).start()

    load_vel.wait()
    load_st.wait()
    load_wind.wait()
    load_x.wait()
    load_b.wait()
    receive_all(early + late, gi, groups)

    lane = lanes(T, L)

    def col_copies(src, dst, base):
        out = []
        for way in range(2):
            out.append(
                (
                    way,
                    pltpu.make_async_remote_copy(
                        src_ref=src(way),
                        dst_ref=dst(way),
                        send_sem=col_send.at[base + way],
                        recv_sem=col_recv.at[base + way],
                        device_id=(gi, lax.rem(ti + (1 if way == 0 else tiles - 1), tiles)),
                        device_id_type=MESH,
                    ),
                )
            )
        return out

    def packed(values):
        after = jnp.zeros((T, L), F32)
        before = jnp.zeros((T, L), F32)
        for f, (first, last) in enumerate(values):
            here = (lane >= W * f) & (lane < W * f + W)
            after = jnp.where(here, pltpu.roll(last, (W * f + W) % L, 1), after)
            before = jnp.where(here, pltpu.roll(first, W * f, 1) if f else first, before)
        return after, before

    def unpacked(from_before, from_after, f):
        low = pltpu.roll(from_before, (L - W - W * f) % L, 1)
        high = pltpu.roll(from_after, (L - W * f) % L, 1) if f else from_after
        return jnp.where(lane < W, high, jnp.where(lane >= L - W, low, 0.0))

    def ends(refs, at):
        return [(ref[at, pl.ds(0, L)], ref[at, pl.ds(cols - L, L)]) for ref in refs]

    def ice_fields(c):
        return (
            vel.at[0, c],
            vel.at[1, c],
            st.at[0, c],
            st.at[1, c],
            st.at[2, c],
            h.at[c],
            wind.at[0, c],
            wind.at[1, c],
        )

    def chunk(k):
        return pl.ds(pl.multiple_of(T + k * T, T), T)

    def chunk0(k):
        return pl.ds(pl.multiple_of(k * T, T), T)

    def pack_chunk(k, _):
        for c in range(2):
            after, before = packed(ends(ice_fields(c), chunk(k)))
            pack_s[0, c, chunk0(k), :] = after
            pack_s[1, c, chunk0(k), :] = before
        return 0

    lax.fori_loop(0, ichunks, pack_chunk, 0, unroll=5)
    icols = col_copies(lambda way: pack_s.at[way], lambda way: pack_r.at[way], 0)
    start_all(icols, ti, tiles)

    receive_all(orow, gi, groups)

    def opack_chunk(k, _):
        after, before = packed(ends((gn, xn, bn), chunk(k)))
        opack_s[0, chunk0(k), :] = after
        opack_s[1, chunk0(k), :] = before
        return 0

    lax.fori_loop(0, ochunks, opack_chunk, 0, unroll=17 if ochunks % 17 == 0 else 1)
    ocols = col_copies(lambda way: opack_s.at[way], lambda way: opack_r.at[way], 2)
    start_all(ocols, ti, tiles)

    receive_all(icols, ti, tiles)

    def prep(c):
        def body(k, thick_up):
            at = chunk(k)
            fields = ice_fields(c)
            values = [[ref[at, pl.ds(j * L, L)] for ref in fields] for j in range(own)]
            before, after = pack_r[0, c, chunk0(k), :], pack_r[1, c, chunk0(k), :]
            values.append([unpacked(before, after, f) for f in range(len(fields))])
            thicks = [v[5] for v in values]
            beside = left(thicks)
            for j, (u, v, s0, s1, s2, thick, wx, wy) in enumerate(values):
                mass = thick + 1.0
                inverse = jnp.where(thick > 0.0, 1.0 / (mass + STEP * DRAG), 0.0)
                q = STEP * inverse
                half = 0.5 * q
                uu[c, j, at, :] = u
                vv[c, j, at, :] = v
                sp_p[c, j, at, :] = (s0 + s1) + STRENGTH * thick
                sp_m[c, j, at, :] = (s0 - s1) + STRENGTH * thick
                sp_s[c, j, at, :] = s2 + s2
                kk[c, j, at, :] = RATE * thick
                pp[c, j, at, :] = mass * inverse
                qq[c, j, at, :] = half
                slope = STRENGTH * half
                ww[0, c, j, at, :] = q * wx - slope * (thick - above(thick_up[j], thick))
                ww[1, c, j, at, :] = q * wy - slope * (thick - beside[j])
            return tuple(thicks)

        zero = jnp.zeros((T, L), F32)
        lax.fori_loop(0, ichunks, body, (zero,) * span, unroll=2)

    prep(0)
    prep(1)

    receive_all(ocols, ti, tiles)

    def ocean_chunk(k, _):
        at = chunk(k)
        before, after = opack_r[0, chunk0(k), :], opack_r[1, chunk0(k), :]
        values = [[ref[at, pl.ds(j * L, L)] for ref in (gn, xn, bn)] for j in range(own)]
        values.append([unpacked(before, after, f) for f in range(3)])
        for j, (depth, height, base) in enumerate(values):
            g[j, at, :] = depth
            gx[j, at, :] = depth * height
            x[j, at, :] = height
            r0[j, at, :] = jnp.where(depth > 0.0, base, 0.0)
        return 0

    lax.fori_loop(0, ochunks, ocean_chunk, 0, unroll=2)

    def around(ref, k, lefts, rights):
        r = T + k * T
        up, down = pl.ds(r - 1, T), pl.ds(r + 1, T)
        lefts, rights = join_left(lefts), join_right(rights)
        return [
            (ref[j, up, :] + ref[j, down, :]) + (lefts[j] + rights[j]) for j in range(span)
        ]

    def turned(ref, k):
        values = [ref[j, chunk(k), :] for j in range(span)]
        return turn_left(values), turn_right(values)

    def pre_chunk(k, _):
        at = chunk(k)
        g_near = around(g, k, *turned(g, k))
        near = around(gx, k, *turned(gx, k))
        for j in range(span):
            depth = g[j, at, :]
            diag = DAMP + depth * g_near[j]
            inverse = 1.0 / diag
            r0[j, at, :] = r0[j, at, :] - diag * x[j, at, :] + depth * near[j]
            inv[j, at, :] = inverse
            gd[j, at, :] = depth * inverse
        return 0

    lax.fori_loop(0, ochunks, pre_chunk, 0, unroll=2)

    def ice_cap(phase):
        c = lax.rem(gi + phase, 2)


        def flow_wait(which):
            for target in range(groups):

                @pl.when(gi == target)
                def _():
                    cap = (target + phase) % 2
                    for piece in which:
                        copy = flow_copy(cap, target, piece)
                        if target == homes[cap]:
                            copy.wait()
                        else:
                            copy.wait_recv()

        flow_wait((0, 1))

        def fpack_chunk(k, _):
            after, before = packed(ends((flow.at[0, c], flow.at[1, c]), chunk(k)))
            fpack_s[0, c, chunk0(k), :] = after
            fpack_s[1, c, chunk0(k), :] = before
            return 0

        lax.fori_loop(0, ichunks, fpack_chunk, 0, unroll=ichunks)
        fcols = col_copies(
            lambda way: fpack_s.at[way, c], lambda way: fpack_r.at[way, c], 4 + 2 * phase
        )
        start_all(fcols, ti, tiles)
        flow_wait((2,))
        receive_all(fcols, ti, tiles)

        def flow_chunk(k, _):
            at = chunk(k)
            before, after = fpack_r[0, c, chunk0(k), :], fpack_r[1, c, chunk0(k), :]
            for comp in range(2):
                values = [flow[comp, c, at, pl.ds(j * L, L)] for j in range(own)]
                values.append(unpacked(before, after, comp))
                flow_edge[comp, c, at, :] = values[own]
                for j in range(span):
                    ww[comp, c, j, at, :] = ww[comp, c, j, at, :] + qq[c, j, at, :] * (
                        2.0 * DRAG * values[j]
                    )
            return 0

        lax.fori_loop(0, ichunks, flow_chunk, 0, unroll=ichunks)

        def subcycle(n, _):
            ahead, behind = 2, 2
            turned_u, turned_v, turned_m, turned_s = {}, {}, {}, {}

            def look(k):
                at = slice(T + T * k, TOP + T * k)
                turned_u[k] = turn_right([uu[c, j, at, :] for j in range(span)])
                turned_v[k] = turn_right([vv[c, j, at, :] for j in range(span)])

            def stress(k):
                at, down = slice(T + T * k, TOP + T * k), slice(T + T * k + 1, TOP + T * k + 1)
                beside_u, beside_v = join_right(turned_u.pop(k)), join_right(turned_v.pop(k))
                ms, ss = [], []
                for j in range(span):
                    u, v = uu[c, j, at, :], vv[c, j, at, :]
                    du = uu[c, j, down, :] - u
                    dv = beside_v[j] - v
                    shear = (beside_u[j] - u) + (vv[c, j, down, :] - v)
                    rate = kk[c, j, at, :] * lax.rsqrt(
                        (du * du + dv * dv) + (0.5 * (shear * shear) + 0.5)
                    )
                    sp_p[c, j, at, :] = sp_p[c, j, at, :] * KEEP + rate * du
                    m = sp_m[c, j, at, :] * KEEP + rate * dv
                    s = sp_s[c, j, at, :] * KEEP + rate * shear
                    sp_m[c, j, at, :] = m
                    sp_s[c, j, at, :] = s
                    ms.append(m)
                    ss.append(s)
                turned_m[k], turned_s[k] = turn_left(ms), turn_left(ss)

            def momentum(k):
                at, up = slice(T + T * k, TOP + T * k), slice(T + T * k - 1, TOP + T * k - 1)
                beside_m, beside_s = join_left(turned_m.pop(k)), join_left(turned_s.pop(k))
                for j in range(span):
                    s = sp_s[c, j, at, :]
                    fx = (sp_p[c, j, at, :] - sp_p[c, j, up, :]) + (s - beside_s[j])
                    fy = (sp_m[c, j, at, :] - beside_m[j]) + (s - sp_s[c, j, up, :])
                    p, q = pp[c, j, at, :], qq[c, j, at, :]
                    uu[c, j, at, :] = p * uu[c, j, at, :] + (q * fx + ww[0, c, j, at, :])
                    vv[c, j, at, :] = p * vv[c, j, at, :] + (q * fy + ww[1, c, j, at, :])

            for k in range(-ahead, ichunks + behind):
                if k + ahead < ichunks:
                    look(k + ahead)
                if 0 <= k < ichunks:
                    stress(k)
                if 0 <= k - behind < ichunks:
                    momentum(k - behind)
            return 0

        lax.fori_loop(0, NSUB, subcycle, 0)

        def drag_chunk(k, drag_up):
            at = pl.ds(pl.multiple_of(TOP + k * T, T), T)
            drags = []
            for comp, ref in enumerate((uu, vv)):
                values = [flow[comp, c, at, pl.ds(j * L, L)] for j in range(own)]
                values.append(flow_edge[comp, c, at, :])
                drags.append(
                    [
                        jnp.where(qq[c, j, at, :] > 0.0, DRAG * (ref[c, j, at, :] - values[j]), 0.0)
                        for j in range(span)
                    ]
                )
            beside = left(drags[1])
            for j in range(span):
                d0 = drags[0][j]
                d0_up = above(jnp.zeros((T, L), F32) if drag_up is None else drag_up[j], d0)
                sp[c, j, chunk0(k), :] = (d0 - d0_up) + (drags[1][j] - beside[j])
            return tuple(drags[0])

        zero = jnp.zeros((T, L), F32)
        last = lax.fori_loop(0, rows // T, drag_chunk, (zero,) * span, unroll=rows // T)
        for j in range(span):
            sp[c, j, rows : rows + T, :] = last[j]

        home = c * (groups - 1)

        @pl.when(gi != home)
        def _():
            for copy in back_copies(phase, c, gi, home):
                copy.start()

        @pl.when(gi == home)
        def _():
            row = pl.multiple_of(TOP + gi * rows, T)
            for j in range(span):

                def own_chunk(k, _):
                    forcing[j, pl.ds(pl.multiple_of(row + k * T, T), T), :] = sp[c, j, chunk0(k), :]
                    return 0

                lax.fori_loop(0, rows // T, own_chunk, 0, unroll=rows // T)
                extra[gi, j] = sp[c, j, rows : rows + T, :]

        if phase == 1:
            for copy in edge_copies():
                pl.when(gi == copy[0])(copy[2].start)

        def out_chunk(k, _):
            at = pl.ds(pl.multiple_of(TOP + k * T, T), T)
            for j in range(own):
                here = pl.ds(j * L, L)
                vel[0, c, at, here] = uu[c, j, at, :]
                vel[1, c, at, here] = vv[c, j, at, :]
                p, m = sp_p[c, j, at, :], sp_m[c, j, at, :]
                st[0, c, at, here] = 0.5 * (p + m) - STRENGTH * h[c, at, here]
                st[1, c, at, here] = 0.5 * (p - m)
                st[2, c, at, here] = 0.5 * sp_s[c, j, at, :]
            return 0

        lax.fori_loop(0, rows // T, out_chunk, 0, unroll=4)
        outs = [
            pltpu.make_async_copy(
                vel.at[:, c, TOP:end, :], vel_out.at[:, c], out_sem.at[2 * phase]
            ),
            pltpu.make_async_copy(
                st.at[:, c, TOP:end, :], stress_out.at[:, c], out_sem.at[2 * phase + 1]
            ),
        ]
        for copy in outs:
            copy.start()
        return outs, fcols

    def back_copies(phase, c, source, target):
        at = pl.ds(pl.multiple_of(TOP + source * rows, T), rows)
        parts = (
            (sp.at[c, :, 0:rows, :], forcing.at[:, at, :]),
            (sp.at[c, :, rows : rows + T, :], extra.at[source]),
        )
        return [
            pltpu.make_async_remote_copy(
                src_ref=src,
                dst_ref=dst,
                send_sem=back_send.at[2 * phase + i],
                recv_sem=back_recv.at[source, i],
                device_id=(target, ti),
                device_id_type=MESH,
            )
            for i, (src, dst) in enumerate(parts)
        ]

    def edge_copies():
        top, bottom = groups - 1, 0
        parts = (
            (top, 1, sp.at[0, :, rows - T : rows, :], forcing.at[:, TOP - T : TOP, :]),
            (top, 1, sp.at[0, :, rows : rows + T, :], extra.at[0]),
            (bottom, groups - 2, sp.at[1, :, 0:T, :], forcing.at[:, oend : oend + T, :]),
        )
        return [
            (
                source,
                target,
                pltpu.make_async_remote_copy(
                    src_ref=src,
                    dst_ref=dst,
                    send_sem=edge_send.at[i],
                    recv_sem=edge_recv.at[i],
                    device_id=(target, ti),
                    device_id_type=MESH,
                ),
            )
            for i, (source, target, src, dst) in enumerate(parts)
        ]

    outs_a, fcols_a = ice_cap(0)
    outs_b, fcols_b = ice_cap(1)

    def carry_over(row, source):
        for j in range(span):
            at = (j, slice(row, row + 1), slice(None))
            forcing[at] = forcing[at] - extra[source, j, T - 1 : T, :]

    for cap, home in enumerate(homes):

        @pl.when(gi == home)
        def _():
            for source in range(groups):
                if source != home:
                    phase = (source + cap) % 2
                    for copy in back_copies(phase, cap, source, source):
                        copy.wait_recv()
            for source in range(groups):
                carry_over(TOP + (source + 1) * rows, source)

    for i, (source, target, copy) in enumerate(edge_copies()):
        pl.when(gi == target)(copy.wait_recv)
        if i == 1:
            pl.when(gi == target)(lambda: carry_over(TOP, 0))

    zero = jnp.zeros((T, L), F32)

    def fold(first, second):
        total = first[0] * second[0]
        for j in range(1, own):
            total = total + first[j] * second[j]
        return total

    def first_chunk(k):
        at = chunk(k)
        r, z = [], []
        for j in range(span):
            depth = g[j, at, :]
            r.append(r0[j, at, :] + jnp.where(depth > 0.0, forcing[j, at, :], 0.0))
            z.append(r[j] * inv[j, at, :])
            v0[j, at, :] = z[j]
            w0[j, at, :] = depth * z[j]
        return fold(r, z)

    first_chunk(0)
    first_chunk(ochunks - 1)
    m0 = lax.fori_loop(1, ochunks - 1, lambda k, s: s + first_chunk(k), zero, unroll=4)

    def power(w_from, v_to, w_to):
        def body(k, turns):
            at = chunk(k)
            near = around(w_from, k, *turns)
            w_here = [w_from[j, at, :] for j in range(own)]
            w_next = []
            for j in range(span):
                v = gd[j, at, :] * near[j]
                w = g[j, at, :] * v
                if j < own:
                    v_to[j, at, :] = v
                w_to[j, at, :] = w
                w_next.append(w)
            return fold(w_here, near), fold(w_next, near)

        body(0, turned(w_from, 0))
        body(ochunks - 1, turned(w_from, ochunks - 1))

        def step(k, carry):
            turns, s0, s1 = carry
            ahead = turned(w_from, k + 1)
            a, b = body(k, turns)
            return ahead, s0 + a, s1 + b

        carry = (turned(w_from, 1), zero, zero)
        _, s0, s1 = lax.fori_loop(1, ochunks - 1, step, carry, unroll=8)
        return s0, s1

    m1, m2 = power(w0, v1, w1)
    m3, m4 = power(w1, v2, w2)

    def last_step(k, carry):
        turns, s = carry
        ahead = turned(w2, k + 1)
        near = around(w2, k, *turns)
        return ahead, s + fold([w2[j, chunk(k), :] for j in range(own)], near)

    _, m5 = lax.fori_loop(1, ochunks - 1, last_step, (turned(w2, 1), zero), unroll=8)

    row = lax.broadcasted_iota(jnp.int32, (T, L), 0)
    moments = zero
    for k, m in enumerate((m0, m1, m2, m3, m4, m5)):
        moments = jnp.where(row == k, jnp.sum(m, axis=0, keepdims=True), moments)

    def all_reduce(value, src, dst, send, recv, index, count, device):
        src[...] = value
        for d in range(1, count):
            pltpu.make_async_remote_copy(
                src_ref=src,
                dst_ref=dst.at[d],
                send_sem=send.at[d],
                recv_sem=recv.at[d],
                device_id=device(lax.rem(index + d, count)),
                device_id_type=MESH,
            ).start()
        for d in range(1, count):
            copy = pltpu.make_async_remote_copy(
                src_ref=src,
                dst_ref=dst.at[d],
                send_sem=send.at[d],
                recv_sem=recv.at[d],
                device_id=device(lax.rem(index + d, count)),
                device_id_type=MESH,
            )
            copy.wait()
        for d in range(1, count):
            value = value + dst[d]
        return value

    moments = all_reduce(
        moments, red_s, red_r, red_send, red_recv, ti, tiles, lambda k: (gi, k)
    )
    moments = all_reduce(
        moments, red2_s, red2_r, red2_send, red2_recv, gi, groups, lambda k: (k, ti)
    )
    total = jnp.sum(moments, axis=1, keepdims=True)
    nu = [total[k : k + 1, :] for k in range(6)]
    a = [nu[k] - nu[k + 1] for k in range(5)]

    tiny = 1e-12

    def safe(value, scale):
        ok = value > tiny * scale
        return jnp.where(ok, 1.0 / jnp.where(ok, value, 1.0), 0.0)

    i0 = safe(a[0], 0.0 * a[0])
    l10, l20 = a[1] * i0, a[2] * i0
    d1 = a[2] - l10 * a[1]
    i1 = safe(d1, a[2])
    e21 = a[3] - l20 * a[1]
    l21 = e21 * i1
    d2 = a[4] - l20 * a[2] - l21 * e21
    i2 = safe(d2, a[4])
    y0 = nu[0]
    y1 = nu[1] - l10 * y0
    y2 = nu[2] - l20 * y0 - l21 * y1
    c2 = y2 * i2
    c1 = y1 * i1 - l21 * c2
    c0 = y0 * i0 - l10 * c1 - l20 * c2

    def final_chunk(k, _):
        at = pl.ds(pl.multiple_of(TOP + k * T, T), T)
        for j in range(own):
            xn[at, pl.ds(j * L, L)] = x[j, at, :] + (
                c0 * v0[j, at, :] + (c1 * v1[j, at, :] + c2 * v2[j, at, :])
            )
        return 0

    lax.fori_loop(0, orows // T, final_chunk, 0, unroll=4)
    last = pltpu.make_async_copy(xn.at[TOP:oend, :], ssh_out, out_sem.at[4])
    last.start()

    for way, copy in early + late + orow:
        pl.when(edge(way, gi, groups)[0])(copy.wait_send)
    for way, copy in ocols + icols + fcols_a + fcols_b:
        pl.when(edge(way, ti, tiles)[0])(copy.wait_send)
    for cap, home in enumerate(homes):

        @pl.when(gi == home)
        def _():
            for target in range(groups):
                if target != home:
                    for piece in range(3):
                        flow_copy(cap, target, piece).wait_send()

    for phase in range(2):
        c = lax.rem(gi + phase, 2)

        @pl.when(gi != c * (groups - 1))
        def _():
            for copy in back_copies(phase, c, gi, c * (groups - 1)):
                copy.wait_send()

    for source, target, copy in edge_copies():
        pl.when(gi == source)(copy.wait_send)
    for copy in outs_a + outs_b:
        copy.wait()
    last.wait()


def deliver(*refs):
    half = len(refs) // 2
    for src, dst in zip(refs[:half], refs[half:]):
        dst[...] = src[...]


def step(groups, tiles, *args):
    base_rhs, thick, ice_vel, ice_stress = args[0], args[5], args[7], args[8]
    orows, cols = base_rhs.shape
    rows = thick.shape[1]
    irows = rows + 2 * TOP
    erows = orows + 2 * TOP
    span = cols // L + 1
    any_spec = pl.BlockSpec(memory_space=pl.ANY)
    hbm = pl.BlockSpec(memory_space=pltpu.HBM)
    vmem = pl.BlockSpec(memory_space=pltpu.VMEM)
    dma = pltpu.SemaphoreType.DMA
    ice = pltpu.VMEM((2, span, irows + PAD, L), F32)
    ocean = pltpu.VMEM((span, erows + PAD, L), F32)
    plain = pltpu.VMEM((erows, cols), F32)
    results = pl.pallas_call(
        functools.partial(kernel, groups, tiles),
        out_shape=(
            jax.ShapeDtypeStruct(base_rhs.shape, F32),
            jax.ShapeDtypeStruct(ice_vel.shape, F32),
            jax.ShapeDtypeStruct(ice_stress.shape, F32),
        ),
        in_specs=[hbm] * 4 + [vmem, hbm, vmem] + [hbm] * 3,
        out_specs=(any_spec,) * 3,
        scratch_shapes=[
            pltpu.VMEM((2, 2, irows, cols), F32),
            pltpu.VMEM((3, 2, irows, cols), F32),
            pltpu.VMEM((2, 2, irows, cols), F32),
            pltpu.VMEM((2, 2, irows, cols), F32),
            pltpu.VMEM((2, irows, cols), F32),
            plain,
            plain,
            plain,
        ]
        + [ice] * 8
        + [
            pltpu.VMEM((2, 2, span, irows + PAD, L), F32),
            pltpu.VMEM((2, 2, irows, L), F32),
        ]
        + [ocean] * 13
        + [
            pltpu.VMEM((orows // BS, cols), F32),
            pltpu.VMEM((2, rows // BS, cols), F32),
            pltpu.VMEM((2, 2, rows + 2 * T, L), F32),
            pltpu.VMEM((2, 2, rows + 2 * T, L), F32),
            pltpu.VMEM((2, 2, rows + 2 * T, L), F32),
            pltpu.VMEM((2, 2, rows + 2 * T, L), F32),
            pltpu.VMEM((2, orows + 2 * T, L), F32),
            pltpu.VMEM((2, orows + 2 * T, L), F32),
            pltpu.VMEM((2, span, rows + T, L), F32),
            pltpu.VMEM((groups, span, T, L), F32),
            pltpu.VMEM((T, L), F32),
            pltpu.VMEM((tiles, T, L), F32),
            pltpu.VMEM((T, L), F32),
            pltpu.VMEM((groups, T, L), F32),
            dma((7,)),
            dma((3 * groups,)),
            dma((6,)),
            dma((14,)),
            dma((14,)),
            dma((8,)),
            dma((8,)),
            dma((4,)),
            dma((groups, 2)),
            dma((3,)),
            dma((3,)),
            dma((tiles,)),
            dma((tiles,)),
            dma((groups,)),
            dma((groups,)),
            dma((5,)),
        ],
        compiler_params=pltpu.CompilerParams(
            collective_id=0, has_side_effects=True, vmem_limit_bytes=67_043_328
        ),
    )(*args)
    return pl.pallas_call(
        deliver,
        out_shape=tuple(jax.ShapeDtypeStruct(r.shape, F32) for r in results),
        in_specs=[vmem] * 3,
        out_specs=(vmem,) * 3,
    )(*results)


def solution(mesh):
    grid = P("grp", "tile")
    plane = P(None, "grp", "tile")
    stack = P(None, None, "grp", "tile")
    return jax.shard_map(
        functools.partial(step, mesh.shape["grp"], mesh.shape["tile"]),
        mesh=mesh,
        in_specs=(grid, grid, grid, plane, grid, plane, plane, stack, stack, stack),
        out_specs=(grid, stack, stack),
        check_vma=False,
    )
```

```python
import functools
import math

import jax
import jax.numpy as jnp
from jax import lax
from jax.experimental import pallas as pl
from jax.experimental.pallas import tpu as pltpu
from jax.sharding import PartitionSpec as P

BS = 8
NSUB = 8

DAMP = 0.05
RELAX = 0.2
STRENGTH = 0.5
DRAG = 1.0
STEP = 0.5
KEEP = 1.0 / (1.0 + RELAX)
RATE = math.sqrt(2.0) * RELAX * STRENGTH / (1.0 + RELAX)

MESH = pl.DeviceIdType.MESH
F32 = jnp.float32
T = 8
L = 128
W = 12
TOP = 2 * T
PAD = 2 * T


def lanes(rows, width):
    return lax.broadcasted_iota(jnp.int32, (rows, width), 1)


def above(prev, here):
    row = lax.broadcasted_iota(jnp.int32, here.shape, 0)
    return pltpu.roll(jnp.where(row == T - 1, prev, here), 1, 0)


def turn_right(tiles):
    return [pltpu.roll(x, L - 1, 1) for x in tiles]


def turn_left(tiles):
    return [pltpu.roll(x, 1, 1) for x in tiles]


def join_right(turned):
    lane = lanes(T, L)
    n = len(turned)
    return [jnp.where(lane == L - 1, turned[(j + 1) % n], turned[j]) for j in range(n)]


def join_left(turned):
    lane = lanes(T, L)
    n = len(turned)
    return [jnp.where(lane == 0, turned[(j - 1) % n], turned[j]) for j in range(n)]


def right(tiles):
    return join_right(turn_right(tiles))


def left(tiles):
    return join_left(turn_left(tiles))


def kernel(
    groups,
    tiles,
    base_in,
    depth_in,
    ssh_in,
    cur_in,
    land_ref,
    thick_in,
    ice_ref,
    vel_in,
    stress_in,
    wind_in,
    ssh_out,
    vel_out,
    stress_out,
    vel,
    st,
    wind,
    flow,
    h,
    gn,
    xn,
    bn,
    uu,
    vv,
    sp_p,
    sp_m,
    sp_s,
    kk,
    pp,
    qq,
    ww,
    flow_edge,
    g,
    gx,
    r0,
    x,
    inv,
    gd,
    forcing,
    v0,
    v1,
    v2,
    w0,
    w1,
    w2,
    wet,
    cover,
    pack_s,
    pack_r,
    fpack_s,
    fpack_r,
    opack_s,
    opack_r,
    sp,
    extra,
    red_s,
    red_r,
    red2_s,
    red2_r,
    load_sem,
    flow_send,
    flow_recv,
    row_send,
    row_recv,
    col_send,
    col_recv,
    back_send,
    back_recv,
    edge_send,
    edge_recv,
    red_send,
    red_recv,
    red2_send,
    red2_recv,
    out_sem,
):
    gi = lax.axis_index("grp")
    ti = lax.axis_index("tile")
    rows, cols = thick_in.shape[1], thick_in.shape[2]
    orows = base_in.shape[0]
    end = TOP + rows
    oend = TOP + orows
    own = cols // L
    span = own + 1
    ichunks = rows // T + 2
    ochunks = orows // T + 2

    loads = []

    def load(src, dst):
        copy = pltpu.make_async_copy(src, dst, load_sem.at[len(loads)])
        copy.start()
        loads.append(copy)
        return copy

    load_thick = load(thick_in, h.at[:, TOP:end, :])
    load_depth = load(depth_in, gn.at[TOP:oend, :])
    load_x = load(ssh_in, xn.at[TOP:oend, :])
    load_b = load(base_in, bn.at[TOP:oend, :])
    load_vel = load(vel_in, vel.at[:, :, TOP:end, :])
    load_st = load(stress_in, st.at[:, :, TOP:end, :])
    load_wind = load(wind_in, wind.at[:, :, TOP:end, :])

    def clear(ref, *spans):
        for lo, hi in spans:
            ref[..., lo:hi, :] = jnp.zeros(ref.shape[:-2] + (hi - lo, ref.shape[-1]), F32)

    for ref in (vel, st, wind, flow, h):
        clear(ref, (T, TOP), (end, end + T))
    for ref in (gn, xn, bn):
        clear(ref, (T, TOP), (oend, oend + T))
    for ref in (pack_r, fpack_r, opack_r, forcing):
        ref[...] = jnp.zeros_like(ref)

    barrier = pltpu.get_barrier_semaphore()
    for d in range(1, groups):
        pl.semaphore_signal(
            barrier, inc=1, device_id=(lax.rem(gi + d, groups), ti), device_id_type=MESH
        )
    for d in range(1, tiles):
        pl.semaphore_signal(
            barrier, inc=1, device_id=(gi, lax.rem(ti + d, tiles)), device_id_type=MESH
        )

    for ref in (uu, vv, sp_p, sp_m, sp_s):
        clear(ref, (0, T), (end + T, end + 2 * T))
    for ref in (g, gx, w0, w1, w2):
        clear(ref, (0, T), (oend + T, oend + 2 * T))

    def blocks(ref, out, count):
        width = ref.shape[-1]
        row = lax.broadcasted_iota(jnp.int32, (width, cols), 0)
        spread = (row == lax.shift_right_logical(lanes(width, cols), 3)).astype(F32)
        values = ref[...].reshape((count, width)).astype(F32)
        out[...] = jnp.dot(values, spread, preferred_element_type=F32)

    blocks(land_ref, wet, land_ref.shape[0])
    for c in range(2):
        row = lax.broadcasted_iota(jnp.int32, (cols // BS, cols), 0)
        spread = (row == lax.shift_right_logical(lanes(cols // BS, cols), 3)).astype(F32)
        cover[c] = jnp.dot(ice_ref[c].astype(F32), spread, preferred_element_type=F32)

    pl.semaphore_wait(barrier, groups + tiles - 2)

    homes = (0, groups - 1)
    pieces = ((0, L), (cols - L, cols), (L, cols - L))

    def flow_copy(cap, target, piece):
        lo = max(0, rows * target - T)
        hi = min(rows * groups, rows * target + rows + T)
        start = TOP + lo - rows * target
        first, last = pieces[piece]
        src = cur_in.at[:, lo:hi, first:last]
        dst = flow.at[:, cap, start : start + hi - lo, first:last]
        if target == homes[cap]:
            return pltpu.make_async_copy(src, dst, flow_recv.at[3 * cap + piece])
        return pltpu.make_async_remote_copy(
            src_ref=src,
            dst_ref=dst,
            send_sem=flow_send.at[3 * target + piece],
            recv_sem=flow_recv.at[3 * cap + piece],
            device_id=(target, ti),
            device_id_type=MESH,
        )

    def row_copy(k, way, src, dst, first, after, ends):
        count, last = ends
        from_row = first + count - T if way == 0 else first
        to_row = after - T if way == 0 else last
        return (
            way,
            pltpu.make_async_remote_copy(
                src_ref=src(pl.ds(from_row, T)),
                dst_ref=dst(pl.ds(to_row, T)),
                send_sem=row_send.at[2 * k + way],
                recv_sem=row_recv.at[2 * k + way],
                device_id=(lax.rem(gi + (1 if way == 0 else groups - 1), groups), ti),
                device_id_type=MESH,
            ),
        )

    def ice_rows(stage):
        c = lax.rem(gi + 1 + stage, 2)
        fields = ((vel_in, vel), (stress_in, st), (wind_in, wind))
        out = []
        for k, (src, dst) in enumerate(fields):
            for way in range(2):
                out.append(
                    row_copy(
                        4 * stage + k,
                        way,
                        lambda at, src=src: src.at[:, c, at, :],
                        lambda at, dst=dst: dst.at[:, c, at, :],
                        0,
                        TOP,
                        (rows, end),
                    )
                )
        for way in range(2):
            out.append(
                row_copy(
                    4 * stage + 3,
                    way,
                    lambda at: h.at[c, at, :],
                    lambda at: h.at[c, at, :],
                    TOP,
                    TOP,
                    (rows, end),
                )
            )
        return out

    def ocean_rows():
        fields = ((ssh_in, xn, 0), (base_in, bn, 0), (gn, gn, TOP))
        return [
            row_copy(
                8 + k,
                way,
                lambda at, src=src: src.at[at, :],
                lambda at, dst=dst: dst.at[at, :],
                first,
                TOP,
                (orows, oend),
            )
            for k, (src, dst, first) in enumerate(fields)
            for way in range(2)
        ]

    def edge(way, index, count):
        sends = index < count - 1 if way == 0 else index > 0
        receives = index > 0 if way == 0 else index < count - 1
        return sends, receives

    def start_all(copies, index, count):
        for way, copy in copies:
            pl.when(edge(way, index, count)[0])(copy.start)

    def receive_all(copies, index, count):
        for way, copy in copies:
            pl.when(edge(way, index, count)[1])(copy.wait_recv)

    for cap, home in enumerate(homes):

        @pl.when(gi == home)
        def _():
            for piece in range(3):
                flow_copy(cap, home, piece).start()

    load_thick.wait()

    def cover_chunk(k, _):
        for c in range(2):
            at = (c, pl.ds(pl.multiple_of(TOP + k * T, T), T), slice(None))
            h[at] = h[at] * cover[c, pl.ds(k, 1), :]
        return 0

    lax.fori_loop(0, rows // T, cover_chunk, 0, unroll=4)
    irow = [ice_rows(stage) for stage in range(2)]
    start_all(irow[0], gi, groups)
    start_all(irow[1], gi, groups)

    for cap, home in enumerate(homes):

        @pl.when(gi == home)
        def _():
            order = sorted((k for k in range(groups) if k != home), key=lambda k: abs(k - home))
            for target in order[1:] + order[:1]:
                for piece in range(3):
                    flow_copy(cap, target, piece).start()

    load_depth.wait()

    def wet_chunk(k, _):
        at = (pl.ds(pl.multiple_of(TOP + k * T, T), T), slice(None))
        gn[at] = gn[at] * wet[pl.ds(k, 1), :]
        return 0

    lax.fori_loop(0, orows // T, wet_chunk, 0, unroll=4)
    orow = ocean_rows()
    start_all(orow, gi, groups)

    load_vel.wait()
    load_st.wait()
    load_wind.wait()
    load_x.wait()
    load_b.wait()

    lane = lanes(T, L)

    def col_copies(src, dst, base):
        out = []
        for way in range(2):
            out.append(
                (
                    way,
                    pltpu.make_async_remote_copy(
                        src_ref=src(way),
                        dst_ref=dst(way),
                        send_sem=col_send.at[base + way],
                        recv_sem=col_recv.at[base + way],
                        device_id=(gi, lax.rem(ti + (1 if way == 0 else tiles - 1), tiles)),
                        device_id_type=MESH,
                    ),
                )
            )
        return out

    def packed(values):
        after = jnp.zeros((T, L), F32)
        before = jnp.zeros((T, L), F32)
        for f, (first, last) in enumerate(values):
            here = (lane >= W * f) & (lane < W * f + W)
            after = jnp.where(here, pltpu.roll(last, (W * f + W) % L, 1), after)
            before = jnp.where(here, pltpu.roll(first, W * f, 1) if f else first, before)
        return after, before

    def unpacked(from_before, from_after, f):
        low = pltpu.roll(from_before, (L - W - W * f) % L, 1)
        high = pltpu.roll(from_after, (L - W * f) % L, 1) if f else from_after
        return jnp.where(lane < W, high, jnp.where(lane >= L - W, low, 0.0))

    def ends(refs, at):
        return [(ref[at, pl.ds(0, L)], ref[at, pl.ds(cols - L, L)]) for ref in refs]

    def ice_fields(c):
        return (
            vel.at[0, c],
            vel.at[1, c],
            st.at[0, c],
            st.at[1, c],
            st.at[2, c],
            h.at[c],
            wind.at[0, c],
            wind.at[1, c],
        )

    def chunk(k):
        return pl.ds(pl.multiple_of(T + k * T, T), T)

    def chunk0(k):
        return pl.ds(pl.multiple_of(k * T, T), T)

    def pack(stage):
        c = lax.rem(gi + stage, 2)

        def body(k, _):
            after, before = packed(ends(ice_fields(c), chunk(k)))
            pack_s[0, c, chunk0(k), :] = after
            pack_s[1, c, chunk0(k), :] = before
            return 0

        lax.fori_loop(0, ichunks, body, 0, unroll=ichunks)
        icols = col_copies(lambda way: pack_s.at[way, c], lambda way: pack_r.at[way, c], 4 * stage)
        start_all(icols, ti, tiles)
        return icols

    def pack_ocean():
        def body(k, _):
            after, before = packed(ends((gn, xn, bn), chunk(k)))
            opack_s[0, chunk0(k), :] = after
            opack_s[1, chunk0(k), :] = before
            return 0

        lax.fori_loop(0, ochunks, body, 0, unroll=17 if ochunks % 17 == 0 else 1)
        ocols = col_copies(lambda way: opack_s.at[way], lambda way: opack_r.at[way], 8)
        start_all(ocols, ti, tiles)
        return ocols

    def prep(c):
        def body(k, thick_up):
            at = chunk(k)
            fields = ice_fields(c)
            values = [[ref[at, pl.ds(j * L, L)] for ref in fields] for j in range(own)]
            before, after = pack_r[0, c, chunk0(k), :], pack_r[1, c, chunk0(k), :]
            values.append([unpacked(before, after, f) for f in range(len(fields))])
            thicks = [v[5] for v in values]
            beside = left(thicks)
            for j, (u, v, s0, s1, s2, thick, wx, wy) in enumerate(values):
                mass = thick + 1.0
                inverse = jnp.where(thick > 0.0, 1.0 / (mass + STEP * DRAG), 0.0)
                q = STEP * inverse
                half = 0.5 * q
                uu[c, j, at, :] = u
                vv[c, j, at, :] = v
                sp_p[c, j, at, :] = (s0 + s1) + STRENGTH * thick
                sp_m[c, j, at, :] = (s0 - s1) + STRENGTH * thick
                sp_s[c, j, at, :] = s2 + s2
                kk[c, j, at, :] = RATE * thick
                pp[c, j, at, :] = mass * inverse
                qq[c, j, at, :] = half
                slope = STRENGTH * half
                ww[0, c, j, at, :] = q * wx - slope * (thick - above(thick_up[j], thick))
                ww[1, c, j, at, :] = q * wy - slope * (thick - beside[j])
            return tuple(thicks)

        zero = jnp.zeros((T, L), F32)
        lax.fori_loop(0, ichunks, body, (zero,) * span, unroll=ichunks // 2)

    def ocean_chunk(k, _):
        at = chunk(k)
        before, after = opack_r[0, chunk0(k), :], opack_r[1, chunk0(k), :]
        values = [[ref[at, pl.ds(j * L, L)] for ref in (gn, xn, bn)] for j in range(own)]
        values.append([unpacked(before, after, f) for f in range(3)])
        for j, (depth, height, base) in enumerate(values):
            g[j, at, :] = depth
            gx[j, at, :] = depth * height
            x[j, at, :] = height
            r0[j, at, :] = jnp.where(depth > 0.0, base, 0.0)
        return 0

    def around(ref, k, lefts, rights):
        r = T + k * T
        up, down = pl.ds(r - 1, T), pl.ds(r + 1, T)
        lefts, rights = join_left(lefts), join_right(rights)
        return [
            (ref[j, up, :] + ref[j, down, :]) + (lefts[j] + rights[j]) for j in range(span)
        ]

    def turned(ref, k):
        values = [ref[j, chunk(k), :] for j in range(span)]
        return turn_left(values), turn_right(values)

    def pre_chunk(k, carry):
        at = chunk(k)
        ahead = (turned(g, k + 1), turned(gx, k + 1))
        g_near = around(g, k, *carry[0])
        near = around(gx, k, *carry[1])
        for j in range(span):
            depth = g[j, at, :]
            diag = DAMP + depth * g_near[j]
            inverse = 1.0 / diag
            r0[j, at, :] = r0[j, at, :] - diag * x[j, at, :] + depth * near[j]
            inv[j, at, :] = inverse
            gd[j, at, :] = depth * inverse
        return ahead

    def prepare_ocean():
        steps = 17 if ochunks % 17 == 0 else 2
        lax.fori_loop(0, ochunks, ocean_chunk, 0, unroll=steps)
        lax.fori_loop(0, ochunks, pre_chunk, (turned(g, 0), turned(gx, 0)), unroll=steps)

    def ice_cap(phase):
        c = lax.rem(gi + phase, 2)

        receive_all(irow[phase], gi, groups)
        icols = pack(phase)

        def flow_wait(which):
            for target in range(groups):

                @pl.when(gi == target)
                def _():
                    cap = (target + phase) % 2
                    for piece in which:
                        copy = flow_copy(cap, target, piece)
                        if target == homes[cap]:
                            copy.wait()
                        else:
                            copy.wait_recv()

        flow_wait((0, 1))

        def fpack_chunk(k, _):
            after, before = packed(ends((flow.at[0, c], flow.at[1, c]), chunk(k)))
            fpack_s[0, c, chunk0(k), :] = after
            fpack_s[1, c, chunk0(k), :] = before
            return 0

        lax.fori_loop(0, ichunks, fpack_chunk, 0, unroll=ichunks)
        fcols = col_copies(
            lambda way: fpack_s.at[way, c], lambda way: fpack_r.at[way, c], 4 * phase + 2
        )
        start_all(fcols, ti, tiles)
        receive_all(icols, ti, tiles)
        prep(c)
        flow_wait((2,))
        receive_all(fcols, ti, tiles)

        def flow_chunk(k, _):
            at = chunk(k)
            before, after = fpack_r[0, c, chunk0(k), :], fpack_r[1, c, chunk0(k), :]
            for comp in range(2):
                values = [flow[comp, c, at, pl.ds(j * L, L)] for j in range(own)]
                values.append(unpacked(before, after, comp))
                flow_edge[comp, c, at, :] = values[own]
                for j in range(span):
                    ww[comp, c, j, at, :] = ww[comp, c, j, at, :] + qq[c, j, at, :] * (
                        2.0 * DRAG * values[j]
                    )
            return 0

        lax.fori_loop(0, ichunks, flow_chunk, 0, unroll=ichunks)

        def subcycle(n, _):
            ahead, behind = 2, 2
            turned_u, turned_v, turned_m, turned_s = {}, {}, {}, {}

            def look(k):
                at = slice(T + T * k, TOP + T * k)
                turned_u[k] = turn_right([uu[c, j, at, :] for j in range(span)])
                turned_v[k] = turn_right([vv[c, j, at, :] for j in range(span)])

            def stress(k):
                at, down = slice(T + T * k, TOP + T * k), slice(T + T * k + 1, TOP + T * k + 1)
                beside_u, beside_v = join_right(turned_u.pop(k)), join_right(turned_v.pop(k))
                ms, ss = [], []
                for j in range(span):
                    u, v = uu[c, j, at, :], vv[c, j, at, :]
                    du = uu[c, j, down, :] - u
                    dv = beside_v[j] - v
                    shear = (beside_u[j] - u) + (vv[c, j, down, :] - v)
                    rate = kk[c, j, at, :] * lax.rsqrt(
                        (du * du + dv * dv) + (0.5 * (shear * shear) + 0.5)
                    )
                    sp_p[c, j, at, :] = sp_p[c, j, at, :] * KEEP + rate * du
                    m = sp_m[c, j, at, :] * KEEP + rate * dv
                    s = sp_s[c, j, at, :] * KEEP + rate * shear
                    sp_m[c, j, at, :] = m
                    sp_s[c, j, at, :] = s
                    ms.append(m)
                    ss.append(s)
                turned_m[k], turned_s[k] = turn_left(ms), turn_left(ss)

            def momentum(k):
                at, up = slice(T + T * k, TOP + T * k), slice(T + T * k - 1, TOP + T * k - 1)
                beside_m, beside_s = join_left(turned_m.pop(k)), join_left(turned_s.pop(k))
                for j in range(span):
                    s = sp_s[c, j, at, :]
                    fx = (sp_p[c, j, at, :] - sp_p[c, j, up, :]) + (s - beside_s[j])
                    fy = (sp_m[c, j, at, :] - beside_m[j]) + (s - sp_s[c, j, up, :])
                    p, q = pp[c, j, at, :], qq[c, j, at, :]
                    uu[c, j, at, :] = p * uu[c, j, at, :] + (q * fx + ww[0, c, j, at, :])
                    vv[c, j, at, :] = p * vv[c, j, at, :] + (q * fy + ww[1, c, j, at, :])

            for k in range(-ahead, ichunks + behind):
                if k + ahead < ichunks:
                    look(k + ahead)
                if 0 <= k < ichunks:
                    stress(k)
                if 0 <= k - behind < ichunks:
                    momentum(k - behind)
            return 0

        lax.fori_loop(0, NSUB, subcycle, 0)

        def drag_chunk(k, drag_up):
            at = pl.ds(pl.multiple_of(TOP + k * T, T), T)
            drags = []
            for comp, ref in enumerate((uu, vv)):
                values = [flow[comp, c, at, pl.ds(j * L, L)] for j in range(own)]
                values.append(flow_edge[comp, c, at, :])
                drags.append(
                    [
                        jnp.where(qq[c, j, at, :] > 0.0, DRAG * (ref[c, j, at, :] - values[j]), 0.0)
                        for j in range(span)
                    ]
                )
            beside = left(drags[1])
            for j in range(span):
                d0 = drags[0][j]
                d0_up = above(jnp.zeros((T, L), F32) if drag_up is None else drag_up[j], d0)
                sp[c, j, chunk0(k), :] = (d0 - d0_up) + (drags[1][j] - beside[j])
            return tuple(drags[0])

        zero = jnp.zeros((T, L), F32)
        last = lax.fori_loop(0, rows // T, drag_chunk, (zero,) * span, unroll=rows // T)
        for j in range(span):
            sp[c, j, rows : rows + T, :] = last[j]

        home = c * (groups - 1)

        @pl.when(gi != home)
        def _():
            for copy in back_copies(phase, c, gi, home):
                copy.start()

        @pl.when(gi == home)
        def _():
            row = pl.multiple_of(TOP + gi * rows, T)
            for j in range(span):

                def own_chunk(k, _):
                    forcing[j, pl.ds(pl.multiple_of(row + k * T, T), T), :] = sp[c, j, chunk0(k), :]
                    return 0

                lax.fori_loop(0, rows // T, own_chunk, 0, unroll=rows // T)
                extra[gi, j] = sp[c, j, rows : rows + T, :]

        if phase == 1:
            for copy in edge_copies():
                pl.when(gi == copy[0])(copy[2].start)

        def out_chunk(k, _):
            at = pl.ds(pl.multiple_of(TOP + k * T, T), T)
            for j in range(own):
                here = pl.ds(j * L, L)
                vel[0, c, at, here] = uu[c, j, at, :]
                vel[1, c, at, here] = vv[c, j, at, :]
                p, m = sp_p[c, j, at, :], sp_m[c, j, at, :]
                st[0, c, at, here] = 0.5 * (p + m) - STRENGTH * h[c, at, here]
                st[1, c, at, here] = 0.5 * (p - m)
                st[2, c, at, here] = 0.5 * sp_s[c, j, at, :]
            return 0

        lax.fori_loop(0, rows // T, out_chunk, 0, unroll=4)
        outs = [
            pltpu.make_async_copy(
                vel.at[:, c, TOP:end, :], vel_out.at[:, c], out_sem.at[2 * phase]
            ),
            pltpu.make_async_copy(
                st.at[:, c, TOP:end, :], stress_out.at[:, c], out_sem.at[2 * phase + 1]
            ),
        ]
        for copy in outs:
            copy.start()
        return outs, icols + fcols

    def back_copies(phase, c, source, target):
        at = pl.ds(pl.multiple_of(TOP + source * rows, T), rows)
        parts = (
            (sp.at[c, :, 0:rows, :], forcing.at[:, at, :]),
            (sp.at[c, :, rows : rows + T, :], extra.at[source]),
        )
        return [
            pltpu.make_async_remote_copy(
                src_ref=src,
                dst_ref=dst,
                send_sem=back_send.at[2 * phase + i],
                recv_sem=back_recv.at[source, i],
                device_id=(target, ti),
                device_id_type=MESH,
            )
            for i, (src, dst) in enumerate(parts)
        ]

    def edge_copies():
        top, bottom = groups - 1, 0
        parts = (
            (top, 1, sp.at[0, :, rows - T : rows, :], forcing.at[:, TOP - T : TOP, :]),
            (top, 1, sp.at[0, :, rows : rows + T, :], extra.at[0]),
            (bottom, groups - 2, sp.at[1, :, 0:T, :], forcing.at[:, oend : oend + T, :]),
        )
        return [
            (
                source,
                target,
                pltpu.make_async_remote_copy(
                    src_ref=src,
                    dst_ref=dst,
                    send_sem=edge_send.at[i],
                    recv_sem=edge_recv.at[i],
                    device_id=(target, ti),
                    device_id_type=MESH,
                ),
            )
            for i, (source, target, src, dst) in enumerate(parts)
        ]

    outs_a, cols_a = ice_cap(0)
    outs_b, cols_b = ice_cap(1)

    receive_all(orow, gi, groups)
    ocols = pack_ocean()
    receive_all(ocols, ti, tiles)
    prepare_ocean()

    def carry_over(row, source):
        for j in range(span):
            at = (j, slice(row, row + 1), slice(None))
            forcing[at] = forcing[at] - extra[source, j, T - 1 : T, :]

    for cap, home in enumerate(homes):

        @pl.when(gi == home)
        def _():
            for source in range(groups):
                if source != home:
                    phase = (source + cap) % 2
                    for copy in back_copies(phase, cap, source, source):
                        copy.wait_recv()
            for source in range(groups):
                carry_over(TOP + (source + 1) * rows, source)

    for i, (source, target, copy) in enumerate(edge_copies()):
        pl.when(gi == target)(copy.wait_recv)
        if i == 1:
            pl.when(gi == target)(lambda: carry_over(TOP, 0))

    zero = jnp.zeros((T, L), F32)

    def fold(first, second):
        total = first[0] * second[0]
        for j in range(1, own):
            total = total + first[j] * second[j]
        return total

    def first_chunk(k):
        at = chunk(k)
        r, z = [], []
        for j in range(span):
            depth = g[j, at, :]
            r.append(r0[j, at, :] + jnp.where(depth > 0.0, forcing[j, at, :], 0.0))
            z.append(r[j] * inv[j, at, :])
            v0[j, at, :] = z[j]
            w0[j, at, :] = depth * z[j]
        return fold(r, z)

    first_chunk(0)
    first_chunk(ochunks - 1)
    m0 = lax.fori_loop(1, ochunks - 1, lambda k, s: s + first_chunk(k), zero, unroll=4)

    def power(w_from, v_to, w_to):
        def body(k, turns):
            at = chunk(k)
            near = around(w_from, k, *turns)
            w_here = [w_from[j, at, :] for j in range(own)]
            w_next = []
            for j in range(span):
                v = gd[j, at, :] * near[j]
                w = g[j, at, :] * v
                if j < own:
                    v_to[j, at, :] = v
                w_to[j, at, :] = w
                w_next.append(w)
            return fold(w_here, near), fold(w_next, near)

        body(0, turned(w_from, 0))
        body(ochunks - 1, turned(w_from, ochunks - 1))

        def step(k, carry):
            turns, s0, s1 = carry
            ahead = turned(w_from, k + 1)
            a, b = body(k, turns)
            return ahead, s0 + a, s1 + b

        carry = (turned(w_from, 1), zero, zero)
        _, s0, s1 = lax.fori_loop(1, ochunks - 1, step, carry, unroll=8)
        return s0, s1

    m1, m2 = power(w0, v1, w1)
    m3, m4 = power(w1, v2, w2)

    def last_step(k, carry):
        turns, s = carry
        ahead = turned(w2, k + 1)
        near = around(w2, k, *turns)
        return ahead, s + fold([w2[j, chunk(k), :] for j in range(own)], near)

    _, m5 = lax.fori_loop(1, ochunks - 1, last_step, (turned(w2, 1), zero), unroll=8)

    row = lax.broadcasted_iota(jnp.int32, (T, L), 0)
    moments = zero
    for k, m in enumerate((m0, m1, m2, m3, m4, m5)):
        moments = jnp.where(row == k, jnp.sum(m, axis=0, keepdims=True), moments)

    def all_reduce(value, src, dst, send, recv, index, count, device):
        src[...] = value
        for d in range(1, count):
            pltpu.make_async_remote_copy(
                src_ref=src,
                dst_ref=dst.at[d],
                send_sem=send.at[d],
                recv_sem=recv.at[d],
                device_id=device(lax.rem(index + d, count)),
                device_id_type=MESH,
            ).start()
        for d in range(1, count):
            copy = pltpu.make_async_remote_copy(
                src_ref=src,
                dst_ref=dst.at[d],
                send_sem=send.at[d],
                recv_sem=recv.at[d],
                device_id=device(lax.rem(index + d, count)),
                device_id_type=MESH,
            )
            copy.wait()
        for d in range(1, count):
            value = value + dst[d]
        return value

    moments = all_reduce(
        moments, red_s, red_r, red_send, red_recv, ti, tiles, lambda k: (gi, k)
    )
    moments = all_reduce(
        moments, red2_s, red2_r, red2_send, red2_recv, gi, groups, lambda k: (k, ti)
    )
    total = jnp.sum(moments, axis=1, keepdims=True)
    nu = [total[k : k + 1, :] for k in range(6)]
    a = [nu[k] - nu[k + 1] for k in range(5)]

    tiny = 1e-12

    def safe(value, scale):
        ok = value > tiny * scale
        return jnp.where(ok, 1.0 / jnp.where(ok, value, 1.0), 0.0)

    i0 = safe(a[0], 0.0 * a[0])
    l10, l20 = a[1] * i0, a[2] * i0
    d1 = a[2] - l10 * a[1]
    i1 = safe(d1, a[2])
    e21 = a[3] - l20 * a[1]
    l21 = e21 * i1
    d2 = a[4] - l20 * a[2] - l21 * e21
    i2 = safe(d2, a[4])
    y0 = nu[0]
    y1 = nu[1] - l10 * y0
    y2 = nu[2] - l20 * y0 - l21 * y1
    c2 = y2 * i2
    c1 = y1 * i1 - l21 * c2
    c0 = y0 * i0 - l10 * c1 - l20 * c2

    def final_chunk(k, _):
        at = pl.ds(pl.multiple_of(TOP + k * T, T), T)
        for j in range(own):
            xn[at, pl.ds(j * L, L)] = x[j, at, :] + (
                c0 * v0[j, at, :] + (c1 * v1[j, at, :] + c2 * v2[j, at, :])
            )
        return 0

    lax.fori_loop(0, orows // T, final_chunk, 0, unroll=4)
    last = pltpu.make_async_copy(xn.at[TOP:oend, :], ssh_out, out_sem.at[4])
    last.start()

    for way, copy in irow[0] + irow[1] + orow:
        pl.when(edge(way, gi, groups)[0])(copy.wait_send)
    for way, copy in ocols + cols_a + cols_b:
        pl.when(edge(way, ti, tiles)[0])(copy.wait_send)
    for cap, home in enumerate(homes):

        @pl.when(gi == home)
        def _():
            for target in range(groups):
                if target != home:
                    for piece in range(3):
                        flow_copy(cap, target, piece).wait_send()

    for phase in range(2):
        c = lax.rem(gi + phase, 2)

        @pl.when(gi != c * (groups - 1))
        def _():
            for copy in back_copies(phase, c, gi, c * (groups - 1)):
                copy.wait_send()

    for source, target, copy in edge_copies():
        pl.when(gi == source)(copy.wait_send)
    for copy in outs_a + outs_b:
        copy.wait()
    last.wait()


def deliver(*refs):
    half = len(refs) // 2
    for src, dst in zip(refs[:half], refs[half:]):
        dst[...] = src[...]


def step(groups, tiles, *args):
    base_rhs, thick, ice_vel, ice_stress = args[0], args[5], args[7], args[8]
    orows, cols = base_rhs.shape
    rows = thick.shape[1]
    irows = rows + 2 * TOP
    erows = orows + 2 * TOP
    span = cols // L + 1
    any_spec = pl.BlockSpec(memory_space=pl.ANY)
    hbm = pl.BlockSpec(memory_space=pltpu.HBM)
    vmem = pl.BlockSpec(memory_space=pltpu.VMEM)
    dma = pltpu.SemaphoreType.DMA
    ice = pltpu.VMEM((2, span, irows + PAD, L), F32)
    ocean = pltpu.VMEM((span, erows + PAD, L), F32)
    plain = pltpu.VMEM((erows, cols), F32)
    results = pl.pallas_call(
        functools.partial(kernel, groups, tiles),
        out_shape=(
            jax.ShapeDtypeStruct(base_rhs.shape, F32),
            jax.ShapeDtypeStruct(ice_vel.shape, F32),
            jax.ShapeDtypeStruct(ice_stress.shape, F32),
        ),
        in_specs=[hbm] * 4 + [vmem, hbm, vmem] + [hbm] * 3,
        out_specs=(any_spec,) * 3,
        scratch_shapes=[
            pltpu.VMEM((2, 2, irows, cols), F32),
            pltpu.VMEM((3, 2, irows, cols), F32),
            pltpu.VMEM((2, 2, irows, cols), F32),
            pltpu.VMEM((2, 2, irows, cols), F32),
            pltpu.VMEM((2, irows, cols), F32),
            plain,
            plain,
            plain,
        ]
        + [ice] * 8
        + [
            pltpu.VMEM((2, 2, span, irows + PAD, L), F32),
            pltpu.VMEM((2, 2, irows, L), F32),
        ]
        + [ocean] * 13
        + [
            pltpu.VMEM((orows // BS, cols), F32),
            pltpu.VMEM((2, rows // BS, cols), F32),
            pltpu.VMEM((2, 2, rows + 2 * T, L), F32),
            pltpu.VMEM((2, 2, rows + 2 * T, L), F32),
            pltpu.VMEM((2, 2, rows + 2 * T, L), F32),
            pltpu.VMEM((2, 2, rows + 2 * T, L), F32),
            pltpu.VMEM((2, orows + 2 * T, L), F32),
            pltpu.VMEM((2, orows + 2 * T, L), F32),
            pltpu.VMEM((2, span, rows + T, L), F32),
            pltpu.VMEM((groups, span, T, L), F32),
            pltpu.VMEM((T, L), F32),
            pltpu.VMEM((tiles, T, L), F32),
            pltpu.VMEM((T, L), F32),
            pltpu.VMEM((groups, T, L), F32),
            dma((7,)),
            dma((3 * groups,)),
            dma((6,)),
            dma((22,)),
            dma((22,)),
            dma((10,)),
            dma((10,)),
            dma((4,)),
            dma((groups, 2)),
            dma((3,)),
            dma((3,)),
            dma((tiles,)),
            dma((tiles,)),
            dma((groups,)),
            dma((groups,)),
            dma((5,)),
        ],
        compiler_params=pltpu.CompilerParams(
            collective_id=0, has_side_effects=True, vmem_limit_bytes=67_043_328
        ),
    )(*args)
    return pl.pallas_call(
        deliver,
        out_shape=tuple(jax.ShapeDtypeStruct(r.shape, F32) for r in results),
        in_specs=[vmem] * 3,
        out_specs=(vmem,) * 3,
    )(*results)


def solution(mesh):
    grid = P("grp", "tile")
    plane = P(None, "grp", "tile")
    stack = P(None, None, "grp", "tile")
    return jax.shard_map(
        functools.partial(step, mesh.shape["grp"], mesh.shape["tile"]),
        mesh=mesh,
        in_specs=(grid, grid, grid, plane, grid, plane, plane, stack, stack, stack),
        out_specs=(grid, stack, stack),
        check_vma=False,
    )
```

```python
import functools
import math

import jax
import jax.numpy as jnp
from jax import lax
from jax.experimental import pallas as pl
from jax.experimental.pallas import tpu as pltpu
from jax.sharding import PartitionSpec as P

BS = 8
NSUB = 8

DAMP = 0.05
RELAX = 0.2
STRENGTH = 0.5
DRAG = 1.0
STEP = 0.5
KEEP = 1.0 / (1.0 + RELAX)
RATE = math.sqrt(2.0) * RELAX * STRENGTH / (1.0 + RELAX)

MESH = pl.DeviceIdType.MESH
F32 = jnp.float32
T = 8
L = 128
W = 12
TOP = 2 * T
PAD = 2 * T


def lanes(rows, width):
    return lax.broadcasted_iota(jnp.int32, (rows, width), 1)


def above(prev, here):
    row = lax.broadcasted_iota(jnp.int32, here.shape, 0)
    return pltpu.roll(jnp.where(row == T - 1, prev, here), 1, 0)


def turn_right(tiles):
    return [pltpu.roll(x, L - 1, 1) for x in tiles]


def turn_left(tiles):
    return [pltpu.roll(x, 1, 1) for x in tiles]


def join_right(turned):
    lane = lanes(T, L)
    n = len(turned)
    return [jnp.where(lane == L - 1, turned[(j + 1) % n], turned[j]) for j in range(n)]


def join_left(turned):
    lane = lanes(T, L)
    n = len(turned)
    return [jnp.where(lane == 0, turned[(j - 1) % n], turned[j]) for j in range(n)]


def right(tiles):
    return join_right(turn_right(tiles))


def left(tiles):
    return join_left(turn_left(tiles))


def kernel(
    groups,
    tiles,
    base_in,
    depth_in,
    ssh_in,
    cur_in,
    land_in,
    thick_in,
    ice_in,
    vel_in,
    stress_in,
    wind_in,
    ssh_out,
    vel_out,
    stress_out,
    land_ref,
    ice_ref,
    vel,
    st,
    wind,
    flow,
    h,
    gn,
    xn,
    bn,
    uu,
    vv,
    sp_p,
    sp_m,
    sp_s,
    kk,
    pp,
    qq,
    ww,
    flow_edge,
    g,
    gx,
    r0,
    x,
    inv,
    gd,
    forcing,
    v0,
    v1,
    v2,
    w0,
    w1,
    w2,
    wet,
    cover,
    pack_s,
    pack_r,
    fpack_s,
    fpack_r,
    opack_s,
    opack_r,
    sp,
    trim_s,
    trim_r,
    red_s,
    red_r,
    red2_s,
    red2_r,
    load_sem,
    flow_send,
    flow_recv,
    row_send,
    row_recv,
    col_send,
    col_recv,
    back_send,
    back_recv,
    edge_send,
    edge_recv,
    red_send,
    red_recv,
    red2_send,
    red2_recv,
):
    gi = lax.axis_index("grp")
    ti = lax.axis_index("tile")
    rows, cols = thick_in.shape[1], thick_in.shape[2]
    orows = base_in.shape[0]
    end = TOP + rows
    oend = TOP + orows
    own = cols // L
    span = own + 1
    ichunks = rows // T + 2
    ochunks = orows // T + 2

    barrier = pltpu.get_barrier_semaphore()
    for d in range(1, groups):
        pl.semaphore_signal(
            barrier, inc=1, device_id=(lax.rem(gi + d, groups), ti), device_id_type=MESH
        )
    for d in range(1, tiles):
        pl.semaphore_signal(
            barrier, inc=1, device_id=(gi, lax.rem(ti + d, tiles)), device_id_type=MESH
        )

    loads = []

    def load(src, dst):
        copy = pltpu.make_async_copy(src, dst, load_sem.at[len(loads)])
        copy.start()
        loads.append(copy)
        return copy

    load_land = load(land_in, land_ref)
    load_ice = load(ice_in, ice_ref)
    load_thick = load(thick_in, h.at[:, TOP:end, :])
    load_vel = load(vel_in, vel.at[:, :, TOP:end, :])
    load_st = load(stress_in, st.at[:, :, TOP:end, :])
    load_wind = load(wind_in, wind.at[:, :, TOP:end, :])
    load_depth = load(depth_in, gn.at[TOP:oend, :])
    load_x = load(ssh_in, xn.at[TOP:oend, :])
    load_b = load(base_in, bn.at[TOP:oend, :])

    def clear(ref, *spans):
        for lo, hi in spans:
            ref[..., lo:hi, :] = jnp.zeros(ref.shape[:-2] + (hi - lo, ref.shape[-1]), F32)

    for outer, before in ((gi == 0, True), (gi == groups - 1, False)):

        @pl.when(outer)
        def _():
            for ref in (vel, st, wind, flow, h):
                clear(ref, (T, TOP) if before else (end, end + T))
            for ref in (gn, xn, bn):
                clear(ref, (T, TOP) if before else (oend, oend + T))
            clear(forcing, (T, TOP), (oend, oend + T))

    for outer, way in ((ti == 0, 0), (ti == tiles - 1, 1)):

        @pl.when(outer)
        def _():
            for ref in (pack_r, fpack_r, opack_r):
                ref[way] = jnp.zeros(ref.shape[1:], F32)

    @pl.when((gi > 0) & (gi < groups - 1))
    def _():
        clear(forcing, (TOP, oend))
        pl.when(gi != 1)(lambda: clear(forcing, (T, TOP)))
        pl.when(gi != groups - 2)(lambda: clear(forcing, (oend, oend + T)))

    for ref in (uu, vv, sp_p, sp_m, sp_s):
        clear(ref, (0, T), (end + T, end + 2 * T))
    for ref in (g, gx, w0, w1, w2):
        clear(ref, (0, T), (oend + T, oend + 2 * T))

    load_land.wait()
    load_ice.wait()

    def blocks(ref, out, count):
        width = ref.shape[-1]
        row = lax.broadcasted_iota(jnp.int32, (width, cols), 0)
        spread = (row == lax.shift_right_logical(lanes(width, cols), 3)).astype(F32)
        values = ref[...].reshape((count, width)).astype(F32)
        out[...] = jnp.dot(values, spread, preferred_element_type=F32)

    blocks(land_ref, wet, land_ref.shape[0])
    for c in range(2):
        row = lax.broadcasted_iota(jnp.int32, (cols // BS, cols), 0)
        spread = (row == lax.shift_right_logical(lanes(cols // BS, cols), 3)).astype(F32)
        cover[c] = jnp.dot(ice_ref[c].astype(F32), spread, preferred_element_type=F32)

    pl.semaphore_wait(barrier, groups + tiles - 2)

    homes = (0, groups - 1)
    pieces = ((0, L), (cols - L, cols), (L, cols - L))

    def flow_span(target):
        lo = max(0, rows * target - T)
        hi = min(rows * groups, rows * target + rows + T)
        return lo, hi, TOP + lo - rows * target

    def flow_copy(cap, target, piece):
        lo, hi, start = flow_span(target)
        first, last = pieces[piece]
        src = cur_in.at[:, lo:hi, first:last]
        dst = flow.at[:, cap, start : start + hi - lo, first:last]
        recv = flow_recv.at[2 * cap + piece // 2]
        if target == homes[cap]:
            return pltpu.make_async_copy(src, dst, recv)
        return pltpu.make_async_remote_copy(
            src_ref=src,
            dst_ref=dst,
            send_sem=flow_send,
            recv_sem=recv,
            device_id=(target, ti),
            device_id_type=MESH,
        )

    def take(ref, sem):
        pltpu.make_async_copy(ref, ref, sem).wait()

    def row_copy(k, way, src, dst, first, after, ends):
        count, last = ends
        from_row = first + count - T if way == 0 else first
        to_row = after - T if way == 0 else last
        return (
            way,
            pltpu.make_async_remote_copy(
                src_ref=src(pl.ds(from_row, T)),
                dst_ref=dst(pl.ds(to_row, T)),
                send_sem=row_send.at[way],
                recv_sem=row_recv.at[2 * k + way],
                device_id=(lax.rem(gi + (1 if way == 0 else groups - 1), groups), ti),
                device_id_type=MESH,
            ),
        )

    def ice_rows(stage):
        c = lax.rem(gi + 1 + stage, 2)
        out = []
        for ref in (vel, st, wind):
            for way in range(2):
                out.append(
                    row_copy(
                        stage,
                        way,
                        lambda at, ref=ref: ref.at[:, c, at, :],
                        lambda at, ref=ref: ref.at[:, c, at, :],
                        TOP,
                        TOP,
                        (rows, end),
                    )
                )
        for way in range(2):
            out.append(
                row_copy(
                    stage,
                    way,
                    lambda at: h.at[c, at, :],
                    lambda at: h.at[c, at, :],
                    TOP,
                    TOP,
                    (rows, end),
                )
            )
        return out

    def ocean_rows():
        return [
            row_copy(
                2,
                way,
                lambda at, ref=ref: ref.at[at, :],
                lambda at, ref=ref: ref.at[at, :],
                TOP,
                TOP,
                (orows, oend),
            )
            for ref in (xn, bn, gn)
            for way in range(2)
        ]

    def edge(way, index, count):
        sends = index < count - 1 if way == 0 else index > 0
        receives = index > 0 if way == 0 else index < count - 1
        return sends, receives

    def start_all(copies, index, count):
        for way, copy in copies:
            pl.when(edge(way, index, count)[0])(copy.start)

    def receive_all(copies, index, count):
        for way, copy in copies:
            pl.when(edge(way, index, count)[1])(copy.wait_recv)

    def receive_rows(k, count):
        for way in range(2):
            pl.when(edge(way, gi, groups)[1])(
                lambda: take(gn.at[0:count, :], row_recv.at[2 * k + way])
            )

    for cap, home in enumerate(homes):

        @pl.when(gi == home)
        def _():
            for piece in range(3):
                flow_copy(cap, home, piece).start()

    load_thick.wait()

    def cover_chunk(k, _):
        for c in range(2):
            at = (c, pl.ds(pl.multiple_of(TOP + k * T, T), T), slice(None))
            h[at] = h[at] * cover[c, pl.ds(k, 1), :]
        return 0

    lax.fori_loop(0, rows // T, cover_chunk, 0, unroll=4)
    load_vel.wait()
    load_st.wait()
    load_wind.wait()
    start_all(ice_rows(0), gi, groups)
    load_depth.wait()

    def wet_chunk(k, _):
        at = (pl.ds(pl.multiple_of(TOP + k * T, T), T), slice(None))
        gn[at] = gn[at] * wet[pl.ds(k, 1), :]
        return 0

    lax.fori_loop(0, orows // T, wet_chunk, 0, unroll=4)
    load_x.wait()
    load_b.wait()
    start_all(ocean_rows(), gi, groups)

    def send_flow(which):
        for cap, home in enumerate(homes):

            @pl.when(gi == home)
            def _():
                order = sorted((k for k in range(groups) if k != home), key=lambda k: abs(k - home))
                for target in which(order):
                    for piece in range(3):
                        flow_copy(cap, target, piece).start()

    send_flow(lambda order: order[1:])
    start_all(ice_rows(1), gi, groups)
    send_flow(lambda order: order[:1])

    lane = lanes(T, L)

    def col_copies(src, dst, base):
        out = []
        for way in range(2):
            out.append(
                (
                    way,
                    pltpu.make_async_remote_copy(
                        src_ref=src(way),
                        dst_ref=dst(way),
                        send_sem=col_send.at[way],
                        recv_sem=col_recv.at[base + way],
                        device_id=(gi, lax.rem(ti + (1 if way == 0 else tiles - 1), tiles)),
                        device_id_type=MESH,
                    ),
                )
            )
        return out

    def packed(values):
        after = jnp.zeros((T, L), F32)
        before = jnp.zeros((T, L), F32)
        for f, (first, last) in enumerate(values):
            here = (lane >= W * f) & (lane < W * f + W)
            after = jnp.where(here, pltpu.roll(last, (W * f + W) % L, 1), after)
            before = jnp.where(here, pltpu.roll(first, W * f, 1) if f else first, before)
        return after, before

    def unpacked(from_before, from_after, f):
        low = pltpu.roll(from_before, (L - W - W * f) % L, 1)
        high = pltpu.roll(from_after, (L - W * f) % L, 1) if f else from_after
        return jnp.where(lane < W, high, jnp.where(lane >= L - W, low, 0.0))

    def ends(refs, at):
        return [(ref[at, pl.ds(0, L)], ref[at, pl.ds(cols - L, L)]) for ref in refs]

    def ice_fields(c):
        return (
            vel.at[0, c],
            vel.at[1, c],
            st.at[0, c],
            st.at[1, c],
            st.at[2, c],
            h.at[c],
            wind.at[0, c],
            wind.at[1, c],
        )

    def chunk(k):
        return pl.ds(pl.multiple_of(T + k * T, T), T)

    def chunk0(k):
        return pl.ds(pl.multiple_of(k * T, T), T)

    def pack(stage):
        c = lax.rem(gi + stage, 2)

        def body(k, _):
            after, before = packed(ends(ice_fields(c), chunk(k)))
            pack_s[0, c, chunk0(k), :] = after
            pack_s[1, c, chunk0(k), :] = before
            return 0

        lax.fori_loop(0, ichunks, body, 0, unroll=ichunks)
        icols = col_copies(lambda way: pack_s.at[way, c], lambda way: pack_r.at[way, c], 4 * stage)
        start_all(icols, ti, tiles)
        return icols

    def pack_ocean():
        def body(k, _):
            after, before = packed(ends((gn, xn, bn), chunk(k)))
            opack_s[0, chunk0(k), :] = after
            opack_s[1, chunk0(k), :] = before
            return 0

        lax.fori_loop(0, ochunks, body, 0, unroll=17 if ochunks % 17 == 0 else 1)
        ocols = col_copies(lambda way: opack_s.at[way], lambda way: opack_r.at[way], 8)
        start_all(ocols, ti, tiles)
        return ocols

    def prep(phase):
        c = lax.rem(gi + phase, 2)

        def body(k, thick_up):
            at = chunk(k)
            fields = ice_fields(c)
            values = [[ref[at, pl.ds(j * L, L)] for ref in fields] for j in range(own)]
            before, after = pack_r[0, c, chunk0(k), :], pack_r[1, c, chunk0(k), :]
            values.append([unpacked(before, after, f) for f in range(len(fields))])
            thicks = [v[5] for v in values]
            beside = left(thicks)
            for j, (u, v, s0, s1, s2, thick, wx, wy) in enumerate(values):
                mass = thick + 1.0
                inverse = jnp.where(thick > 0.0, 1.0 / (mass + STEP * DRAG), 0.0)
                q = STEP * inverse
                half = 0.5 * q
                uu[c, j, at, :] = u
                vv[c, j, at, :] = v
                sp_p[c, j, at, :] = (s0 + s1) + STRENGTH * thick
                sp_m[c, j, at, :] = (s0 - s1) + STRENGTH * thick
                sp_s[c, j, at, :] = s2 + s2
                kk[c, j, at, :] = RATE * thick
                pp[c, j, at, :] = mass * inverse
                qq[c, j, at, :] = half
                slope = STRENGTH * half
                ww[0, c, j, at, :] = q * wx - slope * (thick - above(thick_up[j], thick))
                ww[1, c, j, at, :] = q * wy - slope * (thick - beside[j])
            return tuple(thicks)

        zero = jnp.zeros((T, L), F32)
        lax.fori_loop(0, ichunks, body, (zero,) * span, unroll=ichunks // 2)

    def ocean_chunk(k, _):
        at = chunk(k)
        before, after = opack_r[0, chunk0(k), :], opack_r[1, chunk0(k), :]
        values = [[ref[at, pl.ds(j * L, L)] for ref in (gn, xn, bn)] for j in range(own)]
        values.append([unpacked(before, after, f) for f in range(3)])
        for j, (depth, height, base) in enumerate(values):
            g[j, at, :] = depth
            gx[j, at, :] = depth * height
            x[j, at, :] = height
            r0[j, at, :] = jnp.where(depth > 0.0, base, 0.0)
        return 0

    def around(ref, k, lefts, rights):
        r = T + k * T
        up, down = pl.ds(r - 1, T), pl.ds(r + 1, T)
        lefts, rights = join_left(lefts), join_right(rights)
        return [
            (ref[j, up, :] + ref[j, down, :]) + (lefts[j] + rights[j]) for j in range(span)
        ]

    def turned(ref, k):
        values = [ref[j, chunk(k), :] for j in range(span)]
        return turn_left(values), turn_right(values)

    def pre_chunk(k, carry):
        at = chunk(k)
        ahead = (turned(g, k + 1), turned(gx, k + 1))
        g_near = around(g, k, *carry[0])
        near = around(gx, k, *carry[1])
        for j in range(span):
            depth = g[j, at, :]
            diag = DAMP + depth * g_near[j]
            inverse = 1.0 / diag
            r0[j, at, :] = r0[j, at, :] - diag * x[j, at, :] + depth * near[j]
            inv[j, at, :] = inverse
            gd[j, at, :] = depth * inverse
        return ahead

    def prepare_ocean():
        steps = 17 if ochunks % 17 == 0 else 2
        lax.fori_loop(0, ochunks, ocean_chunk, 0, unroll=steps)
        lax.fori_loop(0, ochunks, pre_chunk, (turned(g, 0), turned(gx, 0)), unroll=steps)

    def flow_wait(phase, part):
        for target in range(groups):

            @pl.when(gi == target)
            def _():
                cap = (target + phase) % 2
                lo, hi, start = flow_span(target)
                width = 2 * L if part == 0 else cols - 2 * L
                ref = flow.at[:, cap, start : start + hi - lo, 0:width]
                take(ref, flow_recv.at[2 * cap + part])

    def pack_flow(phase):
        c = lax.rem(gi + phase, 2)

        def fpack_chunk(k, _):
            after, before = packed(ends((flow.at[0, c], flow.at[1, c]), chunk(k)))
            fpack_s[0, c, chunk0(k), :] = after
            fpack_s[1, c, chunk0(k), :] = before
            return 0

        lax.fori_loop(0, ichunks, fpack_chunk, 0, unroll=ichunks)
        fcols = col_copies(
            lambda way: fpack_s.at[way, c], lambda way: fpack_r.at[way, c], 4 * phase + 2
        )
        start_all(fcols, ti, tiles)
        return fcols

    def add_flow(phase):
        c = lax.rem(gi + phase, 2)

        def flow_chunk(k, _):
            at = chunk(k)
            before, after = fpack_r[0, c, chunk0(k), :], fpack_r[1, c, chunk0(k), :]
            for comp in range(2):
                values = [flow[comp, c, at, pl.ds(j * L, L)] for j in range(own)]
                values.append(unpacked(before, after, comp))
                flow_edge[comp, c, at, :] = values[own]
                for j in range(span):
                    ww[comp, c, j, at, :] = ww[comp, c, j, at, :] + qq[c, j, at, :] * (
                        2.0 * DRAG * values[j]
                    )
            return 0

        lax.fori_loop(0, ichunks, flow_chunk, 0, unroll=ichunks)

    def subcycles(phase, first, last):
        c = lax.rem(gi + phase, 2)

        def subcycle(n, _):
            ahead, behind = 2, 2
            turned_u, turned_v, turned_m, turned_s = {}, {}, {}, {}

            def look(k):
                at = slice(T + T * k, TOP + T * k)
                turned_u[k] = turn_right([uu[c, j, at, :] for j in range(span)])
                turned_v[k] = turn_right([vv[c, j, at, :] for j in range(span)])

            def stress(k):
                at, down = slice(T + T * k, TOP + T * k), slice(T + T * k + 1, TOP + T * k + 1)
                beside_u, beside_v = join_right(turned_u.pop(k)), join_right(turned_v.pop(k))
                ms, ss = [], []
                for j in range(span):
                    u, v = uu[c, j, at, :], vv[c, j, at, :]
                    du = uu[c, j, down, :] - u
                    dv = beside_v[j] - v
                    shear = (beside_u[j] - u) + (vv[c, j, down, :] - v)
                    rate = kk[c, j, at, :] * lax.rsqrt(
                        (du * du + dv * dv) + (0.5 * (shear * shear) + 0.5)
                    )
                    sp_p[c, j, at, :] = sp_p[c, j, at, :] * KEEP + rate * du
                    m = sp_m[c, j, at, :] * KEEP + rate * dv
                    s = sp_s[c, j, at, :] * KEEP + rate * shear
                    sp_m[c, j, at, :] = m
                    sp_s[c, j, at, :] = s
                    ms.append(m)
                    ss.append(s)
                turned_m[k], turned_s[k] = turn_left(ms), turn_left(ss)

            def momentum(k):
                at, up = slice(T + T * k, TOP + T * k), slice(T + T * k - 1, TOP + T * k - 1)
                beside_m, beside_s = join_left(turned_m.pop(k)), join_left(turned_s.pop(k))
                for j in range(span):
                    s = sp_s[c, j, at, :]
                    fx = (sp_p[c, j, at, :] - sp_p[c, j, up, :]) + (s - beside_s[j])
                    fy = (sp_m[c, j, at, :] - beside_m[j]) + (s - sp_s[c, j, up, :])
                    p, q = pp[c, j, at, :], qq[c, j, at, :]
                    uu[c, j, at, :] = p * uu[c, j, at, :] + (q * fx + ww[0, c, j, at, :])
                    vv[c, j, at, :] = p * vv[c, j, at, :] + (q * fy + ww[1, c, j, at, :])

            for k in range(-ahead, ichunks + behind):
                if k + ahead < ichunks:
                    look(k + ahead)
                if 0 <= k < ichunks:
                    stress(k)
                if 0 <= k - behind < ichunks:
                    momentum(k - behind)
            return 0

        lax.fori_loop(first, last, subcycle, 0)

    def drag(phase):
        c = lax.rem(gi + phase, 2)
        home = c * (groups - 1)
        edge_lanes = L // (2 * (rows // T))

        def drag_chunk(k, drag_up):
            at = pl.ds(pl.multiple_of(TOP + k * T, T), T)
            drags = []
            for comp, ref in enumerate((uu, vv)):
                values = [flow[comp, c, at, pl.ds(j * L, L)] for j in range(own)]
                values.append(flow_edge[comp, c, at, :])
                drags.append(
                    [
                        jnp.where(qq[c, j, at, :] > 0.0, DRAG * (ref[c, j, at, :] - values[j]), 0.0)
                        for j in range(span)
                    ]
                )
            beside = left(drags[1])
            for j in range(span):
                d0 = drags[0][j]
                d0_up = above(drag_up[j], d0)
                value = (d0 - d0_up) + (drags[1][j] - beside[j])
                if j < own:
                    sp[c, j, chunk0(k), :] = value
                else:
                    rim = value
            return tuple(drags[0]), rim

        zero = jnp.zeros((T, L), F32)
        upper, rims = (zero,) * span, zero
        for k in range(rows // T):
            upper, rim = drag_chunk(k, upper)
            width = 2 * edge_lanes
            here = (lane >= width * k) & (lane < width * k + width)
            rims = jnp.where(here, pltpu.roll(rim, (edge_lanes + width * k) % L, 1), rims)
        trim_s[c, 0] = rims
        row = lax.broadcasted_iota(jnp.int32, (T, L), 0)
        last = zero
        for j in range(span):
            last = jnp.where(row == j, upper[j][T - 1 : T, :], last)
        trim_s[c, 1] = last

        @pl.when(gi != home)
        def _():
            for copy in back_copies(phase, c, gi, home):
                copy.start()

        if phase == 1:
            for source, target, copy in edge_copies():
                pl.when(gi == source)(copy.start)

        @pl.when(gi == home)
        def _():
            row = pl.multiple_of(TOP + gi * rows, T)
            for j in range(own):

                def own_chunk(k, _):
                    forcing[j, pl.ds(pl.multiple_of(row + k * T, T), T), :] = sp[c, j, chunk0(k), :]
                    return 0

                lax.fori_loop(0, rows // T, own_chunk, 0, unroll=rows // T)
            trim_r[gi] = trim_s[c]

    def output(phase):
        c = lax.rem(gi + phase, 2)

        def out_chunk(k, _):
            at = pl.ds(pl.multiple_of(TOP + k * T, T), T)
            to = chunk0(k)
            for j in range(own):
                here = pl.ds(j * L, L)
                vel_out[0, c, to, here] = uu[c, j, at, :]
                vel_out[1, c, to, here] = vv[c, j, at, :]
                p, m = sp_p[c, j, at, :], sp_m[c, j, at, :]
                stress_out[0, c, to, here] = 0.5 * (p + m) - STRENGTH * h[c, at, here]
                stress_out[1, c, to, here] = 0.5 * (p - m)
                stress_out[2, c, to, here] = 0.5 * sp_s[c, j, at, :]
            return 0

        lax.fori_loop(0, rows // T, out_chunk, 0, unroll=4)

    def back_copies(phase, c, source, target):
        at = pl.ds(pl.multiple_of(TOP + source * rows, T), rows)
        parts = ((sp.at[c], forcing.at[0:own, at, :]), (trim_s.at[c], trim_r.at[source]))
        return [
            pltpu.make_async_remote_copy(
                src_ref=src,
                dst_ref=dst,
                send_sem=back_send.at[phase],
                recv_sem=back_recv.at[source],
                device_id=(target, ti),
                device_id_type=MESH,
            )
            for src, dst in parts
        ]

    def edge_copies():
        top, bottom = groups - 1, 0
        parts = (
            (0, top, 1, sp.at[0, :, rows - T : rows, :], forcing.at[0:own, TOP - T : TOP, :]),
            (0, top, 1, trim_s.at[0], trim_r.at[0]),
            (1, bottom, groups - 2, sp.at[1, :, 0:T, :], forcing.at[0:own, oend : oend + T, :]),
            (1, bottom, groups - 2, trim_s.at[1], trim_r.at[0]),
        )
        return [
            (
                source,
                target,
                pltpu.make_async_remote_copy(
                    src_ref=src,
                    dst_ref=dst,
                    send_sem=edge_send,
                    recv_sem=edge_recv,
                    device_id=(target, ti),
                    device_id_type=MESH,
                ),
            )
            for way, source, target, src, dst in parts
        ]

    back_rows = own * rows + 2 * T
    edge_rows = own * T + 2 * T

    receive_rows(0, 8 * T)
    icols_a = pack(0)
    receive_rows(2, 3 * T)
    ocols = pack_ocean()
    flow_wait(0, 0)
    fcols_a = pack_flow(0)
    receive_all(icols_a, ti, tiles)
    prep(0)
    receive_all(ocols, ti, tiles)
    prepare_ocean()
    receive_rows(1, 8 * T)
    icols_b = pack(1)
    flow_wait(0, 1)
    receive_all(fcols_a, ti, tiles)
    add_flow(0)
    subcycles(0, 0, NSUB // 2)
    flow_wait(1, 0)
    fcols_b = pack_flow(1)
    subcycles(0, NSUB // 2, NSUB)
    drag(0)
    output(0)
    receive_all(icols_b, ti, tiles)
    prep(1)
    flow_wait(1, 1)
    receive_all(fcols_b, ti, tiles)
    add_flow(1)
    subcycles(1, 0, NSUB)
    drag(1)
    output(1)

    def rim_of(source, k):
        lanes_each = L // (2 * (rows // T))
        turn = (lanes_each + 2 * lanes_each * k) % L
        value = pltpu.roll(trim_r[source, 0], (L - turn) % L, 1)
        return jnp.where((lane < lanes_each) | (lane >= L - lanes_each), value, 0.0)

    def carry_over(row, source):
        for j in range(span):
            at = (j, slice(row, row + 1), slice(None))
            forcing[at] = forcing[at] - trim_r[source, 1, j : j + 1, :]

    for cap, home in enumerate(homes):

        @pl.when(gi == home)
        def _():
            early = [k for k in range(groups) if k != home and (k + cap) % 2 == 0]
            late = [k for k in range(groups) if k != home and (k + cap) % 2 == 1]
            for some in ([home] + early, late):
                for source in some:
                    if source != home:
                        take(w0.at[0, 0:back_rows, :], back_recv.at[source])
                for source in some:
                    for k in range(rows // T):
                        row = TOP + source * rows + k * T
                        forcing[own, row : row + T, :] = rim_of(source, k)
            for source in range(groups):
                carry_over(TOP + (source + 1) * rows, source)

    @pl.when(gi == 1)
    def _():
        take(w0.at[0, 0:edge_rows, :], edge_recv)
        forcing[own, TOP - T : TOP, :] = rim_of(0, rows // T - 1)
        carry_over(TOP, 0)

    @pl.when(gi == groups - 2)
    def _():
        take(w0.at[0, 0:edge_rows, :], edge_recv)
        forcing[own, oend : oend + T, :] = rim_of(0, 0)

    zero = jnp.zeros((T, L), F32)

    def fold(first, second):
        total = first[0] * second[0]
        for j in range(1, own):
            total = total + first[j] * second[j]
        return total

    def first_chunk(k):
        at = chunk(k)
        r, z = [], []
        for j in range(span):
            depth = g[j, at, :]
            r.append(r0[j, at, :] + jnp.where(depth > 0.0, forcing[j, at, :], 0.0))
            z.append(r[j] * inv[j, at, :])
            v0[j, at, :] = z[j]
            w0[j, at, :] = depth * z[j]
        return fold(r, z)

    first_chunk(0)
    first_chunk(ochunks - 1)
    m0 = lax.fori_loop(1, ochunks - 1, lambda k, s: s + first_chunk(k), zero, unroll=4)

    def power(w_from, v_to, w_to):
        def body(k, turns):
            at = chunk(k)
            near = around(w_from, k, *turns)
            w_here = [w_from[j, at, :] for j in range(own)]
            w_next = []
            for j in range(span):
                v = gd[j, at, :] * near[j]
                w = g[j, at, :] * v
                if j < own:
                    v_to[j, at, :] = v
                w_to[j, at, :] = w
                w_next.append(w)
            return fold(w_here, near), fold(w_next, near)

        body(0, turned(w_from, 0))
        body(ochunks - 1, turned(w_from, ochunks - 1))

        def step(k, carry):
            turns, s0, s1 = carry
            ahead = turned(w_from, k + 1)
            a, b = body(k, turns)
            return ahead, s0 + a, s1 + b

        carry = (turned(w_from, 1), zero, zero)
        _, s0, s1 = lax.fori_loop(1, ochunks - 1, step, carry, unroll=8)
        return s0, s1

    m1, m2 = power(w0, v1, w1)
    m3, m4 = power(w1, v2, w2)

    def last_step(k, carry):
        turns, s = carry
        ahead = turned(w2, k + 1)
        near = around(w2, k, *turns)
        return ahead, s + fold([w2[j, chunk(k), :] for j in range(own)], near)

    _, m5 = lax.fori_loop(1, ochunks - 1, last_step, (turned(w2, 1), zero), unroll=8)

    row = lax.broadcasted_iota(jnp.int32, (T, L), 0)
    moments = zero
    for k, m in enumerate((m0, m1, m2, m3, m4, m5)):
        moments = jnp.where(row == k, jnp.sum(m, axis=0, keepdims=True), moments)

    def all_reduce(value, src, dst, send, recv, index, count, device):
        src[...] = value
        for d in range(1, count):
            pltpu.make_async_remote_copy(
                src_ref=src,
                dst_ref=dst.at[d],
                send_sem=send,
                recv_sem=recv,
                device_id=device(lax.rem(index + d, count)),
                device_id_type=MESH,
            ).start()
        take(dst.at[1:count], recv)
        for d in range(1, count):
            value = value + dst[d]
        return value

    moments = all_reduce(
        moments, red_s, red_r, red_send, red_recv, ti, tiles, lambda k: (gi, k)
    )
    moments = all_reduce(
        moments, red2_s, red2_r, red2_send, red2_recv, gi, groups, lambda k: (k, ti)
    )
    total = jnp.sum(moments, axis=1, keepdims=True)
    nu = [total[k : k + 1, :] for k in range(6)]
    a = [nu[k] - nu[k + 1] for k in range(5)]

    tiny = 1e-12

    def safe(value, scale):
        ok = value > tiny * scale
        return jnp.where(ok, 1.0 / jnp.where(ok, value, 1.0), 0.0)

    i0 = safe(a[0], 0.0 * a[0])
    l10, l20 = a[1] * i0, a[2] * i0
    d1 = a[2] - l10 * a[1]
    i1 = safe(d1, a[2])
    e21 = a[3] - l20 * a[1]
    l21 = e21 * i1
    d2 = a[4] - l20 * a[2] - l21 * e21
    i2 = safe(d2, a[4])
    y0 = nu[0]
    y1 = nu[1] - l10 * y0
    y2 = nu[2] - l20 * y0 - l21 * y1
    c2 = y2 * i2
    c1 = y1 * i1 - l21 * c2
    c0 = y0 * i0 - l10 * c1 - l20 * c2

    def final_chunk(k, _):
        at = pl.ds(pl.multiple_of(TOP + k * T, T), T)
        for j in range(own):
            ssh_out[chunk0(k), pl.ds(j * L, L)] = x[j, at, :] + (
                c0 * v0[j, at, :] + (c1 * v1[j, at, :] + c2 * v2[j, at, :])
            )
        return 0

    lax.fori_loop(0, orows // T, final_chunk, 0, unroll=4)
    for way in range(2):
        pl.when(edge(way, gi, groups)[0])(
            lambda: take(gn.at[0 : 19 * T, :], row_send.at[way])
        )
        sent = 2 * (rows + 2 * T) + (orows + 2 * T) // 2
        pl.when(edge(way, ti, tiles)[0])(lambda: take(w0.at[0:2, 0:sent, :], col_send.at[way]))
    for cap, home in enumerate(homes):

        @pl.when(gi == home)
        def _():
            spans = [flow_span(k) for k in range(groups) if k != home]
            take(cur_in.at[:, 0 : sum(hi - lo for lo, hi, _ in spans), :], flow_send)

    for phase in range(2):
        pl.when(gi != lax.rem(gi + phase, 2) * (groups - 1))(
            lambda: take(w0.at[0, 0:back_rows, :], back_send.at[phase])
        )
    pl.when((gi == 0) | (gi == groups - 1))(lambda: take(w0.at[0, 0:edge_rows, :], edge_send))
    take(red_r.at[1:tiles], red_send)
    take(red2_r.at[1:groups], red2_send)


def deliver(*refs):
    sems = refs[-1]
    half = len(refs) // 2
    copies = [
        pltpu.make_async_copy(src, dst, sems.at[k])
        for k, (src, dst) in enumerate(zip(refs[:half], refs[half:-1]))
    ]
    for copy in copies:
        copy.start()
    for copy in copies:
        copy.wait()


def step(groups, tiles, *args):
    base_rhs, thick, ice_vel, ice_stress = args[0], args[5], args[7], args[8]
    orows, cols = base_rhs.shape
    rows = thick.shape[1]
    irows = rows + 2 * TOP
    erows = orows + 2 * TOP
    span = cols // L + 1
    hbm = pl.BlockSpec(memory_space=pltpu.HBM)
    vmem = pl.BlockSpec(memory_space=pltpu.VMEM)
    dma = pltpu.SemaphoreType.DMA
    ice = pltpu.VMEM((2, span, irows + PAD, L), F32)
    ocean = pltpu.VMEM((span, erows + PAD, L), F32)
    plain = pltpu.VMEM((erows, cols), F32)
    results = pl.pallas_call(
        functools.partial(kernel, groups, tiles),
        out_shape=(
            pltpu.VMEM(base_rhs.shape, F32),
            pltpu.VMEM(ice_vel.shape, F32),
            pltpu.VMEM(ice_stress.shape, F32),
        ),
        in_specs=[hbm] * 10,
        out_specs=(vmem,) * 3,
        scratch_shapes=[
            pltpu.VMEM(args[4].shape, jnp.int32),
            pltpu.VMEM(args[6].shape, jnp.int32),
            pltpu.VMEM((2, 2, irows, cols), F32),
            pltpu.VMEM((3, 2, irows, cols), F32),
            pltpu.VMEM((2, 2, irows, cols), F32),
            pltpu.VMEM((2, 2, irows, cols), F32),
            pltpu.VMEM((2, irows, cols), F32),
            plain,
            plain,
            plain,
        ]
        + [ice] * 8
        + [
            pltpu.VMEM((2, 2, span, irows + PAD, L), F32),
            pltpu.VMEM((2, 2, irows, L), F32),
        ]
        + [ocean] * 13
        + [
            pltpu.VMEM((orows // BS, cols), F32),
            pltpu.VMEM((2, rows // BS, cols), F32),
            pltpu.VMEM((2, 2, rows + 2 * T, L), F32),
            pltpu.VMEM((2, 2, rows + 2 * T, L), F32),
            pltpu.VMEM((2, 2, rows + 2 * T, L), F32),
            pltpu.VMEM((2, 2, rows + 2 * T, L), F32),
            pltpu.VMEM((2, orows + 2 * T, L), F32),
            pltpu.VMEM((2, orows + 2 * T, L), F32),
            pltpu.VMEM((2, span - 1, rows, L), F32),
            pltpu.VMEM((2, 2, T, L), F32),
            pltpu.VMEM((groups, 2, T, L), F32),
            pltpu.VMEM((T, L), F32),
            pltpu.VMEM((tiles, T, L), F32),
            pltpu.VMEM((T, L), F32),
            pltpu.VMEM((groups, T, L), F32),
            dma((9,)),
            dma,
            dma((4,)),
            dma((2,)),
            dma((6,)),
            dma((2,)),
            dma((10,)),
            dma((2,)),
            dma((groups,)),
            dma,
            dma,
            dma,
            dma,
            dma,
            dma,
        ],
        compiler_params=pltpu.CompilerParams(
            collective_id=0, has_side_effects=True, vmem_limit_bytes=48 * 2**20
        ),
    )(*(pltpu.with_memory_space_constraint(a, pltpu.HBM) for a in args))
    return pl.pallas_call(
        deliver,
        out_shape=tuple(jax.ShapeDtypeStruct(r.shape, F32) for r in results),
        in_specs=[vmem] * 3,
        out_specs=(hbm,) * 3,
        scratch_shapes=[dma((3,))],
        compiler_params=pltpu.CompilerParams(vmem_limit_bytes=4 * 2**20),
    )(*results)


def solution(mesh):
    grid = P("grp", "tile")
    plane = P(None, "grp", "tile")
    stack = P(None, None, "grp", "tile")
    return jax.shard_map(
        functools.partial(step, mesh.shape["grp"], mesh.shape["tile"]),
        mesh=mesh,
        in_specs=(grid, grid, grid, plane, grid, plane, plane, stack, stack, stack),
        out_specs=(grid, stack, stack),
        check_vma=False,
    )
```

```python
import functools
import math

import jax
import jax.numpy as jnp
from jax import lax
from jax.experimental import pallas as pl
from jax.experimental.pallas import tpu as pltpu
from jax.sharding import PartitionSpec as P

BS = 8
NSUB = 8

DAMP = 0.05
RELAX = 0.2
STRENGTH = 0.5
DRAG = 1.0
STEP = 0.5
KEEP = 1.0 / (1.0 + RELAX)
RATE = math.sqrt(2.0) * RELAX * STRENGTH / (1.0 + RELAX)

MESH = pl.DeviceIdType.MESH
F32 = jnp.float32
T = 8
L = 128
W = 12
TOP = 2 * T
PAD = 2 * T


def lanes(rows, width):
    return lax.broadcasted_iota(jnp.int32, (rows, width), 1)


def above(prev, here):
    row = lax.broadcasted_iota(jnp.int32, here.shape, 0)
    return pltpu.roll(jnp.where(row == T - 1, prev, here), 1, 0)


def turn_right(tiles):
    return [pltpu.roll(x, L - 1, 1) for x in tiles]


def turn_left(tiles):
    return [pltpu.roll(x, 1, 1) for x in tiles]


def join_right(turned):
    lane = lanes(T, L)
    n = len(turned)
    return [jnp.where(lane == L - 1, turned[(j + 1) % n], turned[j]) for j in range(n)]


def join_left(turned):
    lane = lanes(T, L)
    n = len(turned)
    return [jnp.where(lane == 0, turned[(j - 1) % n], turned[j]) for j in range(n)]


def right(tiles):
    return join_right(turn_right(tiles))


def left(tiles):
    return join_left(turn_left(tiles))


def kernel(
    groups,
    tiles,
    base_in,
    depth_in,
    ssh_in,
    cur_in,
    land_in,
    thick_in,
    ice_in,
    vel_in,
    stress_in,
    wind_in,
    ssh_out,
    vel_out,
    stress_out,
    land_ref,
    ice_ref,
    vel,
    st,
    wind,
    flow,
    h,
    gn,
    xn,
    bn,
    uu,
    vv,
    sp_p,
    sp_m,
    sp_s,
    kk,
    pp,
    qq,
    ww,
    flow_edge,
    g,
    gx,
    r0,
    x,
    inv,
    gd,
    forcing,
    v0,
    v1,
    v2,
    w0,
    w1,
    w2,
    wet,
    cover,
    pack_s,
    pack_r,
    fpack_s,
    fpack_r,
    opack_s,
    opack_r,
    sp,
    trim_s,
    trim_r,
    red_s,
    red_r,
    load_sem,
    flow_send,
    flow_recv,
    row_send,
    row_recv,
    col_send,
    col_recv,
    back_send,
    back_recv,
    edge_send,
    edge_recv,
    red_send,
    red_recv,
    ready,
):
    gi = lax.axis_index("grp")
    ti = lax.axis_index("tile")
    rows, cols = thick_in.shape[1], thick_in.shape[2]
    orows = base_in.shape[0]
    end = TOP + rows
    oend = TOP + orows
    own = cols // L
    span = own + 1
    ichunks = rows // T + 2
    ochunks = orows // T + 2

    barrier = pltpu.get_barrier_semaphore()
    for d in range(1, groups):
        pl.semaphore_signal(
            barrier, inc=1, device_id=(lax.rem(gi + d, groups), ti), device_id_type=MESH
        )
    for d in range(1, tiles):
        pl.semaphore_signal(
            barrier, inc=1, device_id=(gi, lax.rem(ti + d, tiles)), device_id_type=MESH
        )

    loads = []

    def load(src, dst):
        copy = pltpu.make_async_copy(src, dst, load_sem.at[len(loads)])
        copy.start()
        loads.append(copy)
        return copy

    load_land = load(land_in, land_ref)
    load_ice = load(ice_in, ice_ref)
    load_thick = load(thick_in, h.at[:, TOP:end, :])
    load_vel = load(vel_in, vel.at[:, :, TOP:end, :])
    load_st = load(stress_in, st.at[:, :, TOP:end, :])
    load_wind = load(wind_in, wind.at[:, :, TOP:end, :])
    load_depth = load(depth_in, gn.at[TOP:oend, :])
    load_x = load(ssh_in, xn.at[TOP:oend, :])
    load_b = load(base_in, bn.at[TOP:oend, :])

    def clear(ref, *spans):
        for lo, hi in spans:
            ref[..., lo:hi, :] = jnp.zeros(ref.shape[:-2] + (hi - lo, ref.shape[-1]), F32)

    for outer, before in ((gi == 0, True), (gi == groups - 1, False)):

        @pl.when(outer)
        def _():
            for ref in (vel, st, wind, flow, h):
                clear(ref, (T, TOP) if before else (end, end + T))
            for ref in (gn, xn, bn):
                clear(ref, (T, TOP) if before else (oend, oend + T))
            clear(forcing, (T, TOP), (oend, oend + T))

    for outer, way in ((ti == 0, 0), (ti == tiles - 1, 1)):

        @pl.when(outer)
        def _():
            for ref in (pack_r, fpack_r, opack_r):
                ref[way] = jnp.zeros(ref.shape[1:], F32)

    @pl.when((gi > 0) & (gi < groups - 1))
    def _():
        clear(forcing, (TOP, oend))
        pl.when(gi != 1)(lambda: clear(forcing, (T, TOP)))
        pl.when(gi != groups - 2)(lambda: clear(forcing, (oend, oend + T)))

    for ref in (uu, vv, sp_p, sp_m, sp_s):
        clear(ref, (0, T), (end + T, end + 2 * T))
    for ref in (g, gx, w0, w1, w2):
        clear(ref, (0, T), (oend + T, oend + 2 * T))

    def blocks(ref, out, count):
        width = ref.shape[-1]
        row = lax.broadcasted_iota(jnp.int32, (width, cols), 0)
        spread = (row == lax.shift_right_logical(lanes(width, cols), 3)).astype(F32)
        values = ref[...].reshape((count, width)).astype(F32)
        out[...] = jnp.dot(values, spread, preferred_element_type=F32)

    pl.semaphore_wait(barrier, groups + tiles - 2)
    for d in range(1, tiles):
        pl.semaphore_signal(
            ready, inc=1, device_id=(gi, lax.rem(ti + d, tiles)), device_id_type=MESH
        )

    homes = (0, groups - 1)
    pieces = ((0, L), (cols - L, cols), (L, cols - L))

    def flow_span(target):
        lo = max(0, rows * target - T)
        hi = min(rows * groups, rows * target + rows + T)
        return lo, hi, TOP + lo - rows * target

    def flow_copy(cap, target, piece):
        lo, hi, start = flow_span(target)
        first, last = pieces[piece]
        src = cur_in.at[:, lo:hi, first:last]
        dst = flow.at[:, cap, start : start + hi - lo, first:last]
        recv = flow_recv.at[2 * cap + piece // 2]
        if target == homes[cap]:
            return pltpu.make_async_copy(src, dst, recv)
        return pltpu.make_async_remote_copy(
            src_ref=src,
            dst_ref=dst,
            send_sem=flow_send,
            recv_sem=recv,
            device_id=(target, ti),
            device_id_type=MESH,
        )

    def take(ref, sem):
        pltpu.make_async_copy(ref, ref, sem).wait()

    def row_copy(k, way, src, dst, first, after, ends):
        count, last = ends
        from_row = first + count - T if way == 0 else first
        to_row = after - T if way == 0 else last
        return (
            way,
            pltpu.make_async_remote_copy(
                src_ref=src(pl.ds(from_row, T)),
                dst_ref=dst(pl.ds(to_row, T)),
                send_sem=row_send.at[way],
                recv_sem=row_recv.at[2 * k + way],
                device_id=(lax.rem(gi + (1 if way == 0 else groups - 1), groups), ti),
                device_id_type=MESH,
            ),
        )

    def ice_rows(stage):
        c = lax.rem(gi + 1 + stage, 2)
        out = []
        for ref in (vel, st, wind):
            for way in range(2):
                out.append(
                    row_copy(
                        stage,
                        way,
                        lambda at, ref=ref: ref.at[:, c, at, :],
                        lambda at, ref=ref: ref.at[:, c, at, :],
                        TOP,
                        TOP,
                        (rows, end),
                    )
                )
        return out

    def thick_rows(stage):
        c = lax.rem(gi + 1 + stage, 2)
        return [
            row_copy(
                stage,
                way,
                lambda at: h.at[c, at, :],
                lambda at: h.at[c, at, :],
                TOP,
                TOP,
                (rows, end),
            )
            for way in range(2)
        ]

    def ocean_rows():
        return [
            row_copy(
                2,
                way,
                lambda at, ref=ref: ref.at[at, :],
                lambda at, ref=ref: ref.at[at, :],
                TOP,
                TOP,
                (orows, oend),
            )
            for ref in (xn, bn, gn)
            for way in range(2)
        ]

    def edge(way, index, count):
        sends = index < count - 1 if way == 0 else index > 0
        receives = index > 0 if way == 0 else index < count - 1
        return sends, receives

    def start_all(copies, index, count):
        for way, copy in copies:
            pl.when(edge(way, index, count)[0])(copy.start)

    def receive_all(copies, index, count):
        for way, copy in copies:
            pl.when(edge(way, index, count)[1])(copy.wait_recv)

    def receive_rows(k, count):
        for way in range(2):
            pl.when(edge(way, gi, groups)[1])(
                lambda: take(gn.at[0:count, :], row_recv.at[2 * k + way])
            )

    for cap, home in enumerate(homes):

        @pl.when(gi == home)
        def _():
            for piece in range(3):
                flow_copy(cap, home, piece).start()

    load_vel.wait()
    load_st.wait()
    load_wind.wait()
    start_all(ice_rows(0), gi, groups)
    load_land.wait()
    load_ice.wait()
    blocks(land_ref, wet, land_ref.shape[0])
    for c in range(2):
        row = lax.broadcasted_iota(jnp.int32, (cols // BS, cols), 0)
        spread = (row == lax.shift_right_logical(lanes(cols // BS, cols), 3)).astype(F32)
        cover[c] = jnp.dot(ice_ref[c].astype(F32), spread, preferred_element_type=F32)
    load_thick.wait()

    def cover_chunk(k, _):
        for c in range(2):
            at = (c, pl.ds(pl.multiple_of(TOP + k * T, T), T), slice(None))
            h[at] = h[at] * cover[c, pl.ds(k, 1), :]
        return 0

    lax.fori_loop(0, rows // T, cover_chunk, 0, unroll=4)
    start_all(thick_rows(0), gi, groups)
    load_depth.wait()

    def wet_chunk(k, _):
        at = (pl.ds(pl.multiple_of(TOP + k * T, T), T), slice(None))
        gn[at] = gn[at] * wet[pl.ds(k, 1), :]
        return 0

    lax.fori_loop(0, orows // T, wet_chunk, 0, unroll=4)
    load_x.wait()
    load_b.wait()
    start_all(ocean_rows(), gi, groups)

    def send_flow(which):
        for cap, home in enumerate(homes):

            @pl.when(gi == home)
            def _():
                order = sorted((k for k in range(groups) if k != home), key=lambda k: abs(k - home))
                for target in which(order):
                    for piece in range(3):
                        flow_copy(cap, target, piece).start()

    send_flow(lambda order: order[1:])
    start_all(ice_rows(1), gi, groups)
    start_all(thick_rows(1), gi, groups)
    send_flow(lambda order: order[:1])

    lane = lanes(T, L)

    def col_copies(src, dst, base):
        out = []
        for way in range(2):
            out.append(
                (
                    way,
                    pltpu.make_async_remote_copy(
                        src_ref=src(way),
                        dst_ref=dst(way),
                        send_sem=col_send.at[way],
                        recv_sem=col_recv.at[base + way],
                        device_id=(gi, lax.rem(ti + (1 if way == 0 else tiles - 1), tiles)),
                        device_id_type=MESH,
                    ),
                )
            )
        return out

    def packed(values):
        after = jnp.zeros((T, L), F32)
        before = jnp.zeros((T, L), F32)
        for f, (first, last) in enumerate(values):
            here = (lane >= W * f) & (lane < W * f + W)
            after = jnp.where(here, pltpu.roll(last, (W * f + W) % L, 1), after)
            before = jnp.where(here, pltpu.roll(first, W * f, 1) if f else first, before)
        return after, before

    def unpacked(from_before, from_after, f):
        low = pltpu.roll(from_before, (L - W - W * f) % L, 1)
        high = pltpu.roll(from_after, (L - W * f) % L, 1) if f else from_after
        return jnp.where(lane < W, high, jnp.where(lane >= L - W, low, 0.0))

    def ends(refs, at):
        return [(ref[at, pl.ds(0, L)], ref[at, pl.ds(cols - L, L)]) for ref in refs]

    def ice_fields(c):
        return (
            vel.at[0, c],
            vel.at[1, c],
            st.at[0, c],
            st.at[1, c],
            st.at[2, c],
            h.at[c],
            wind.at[0, c],
            wind.at[1, c],
        )

    def chunk(k):
        return pl.ds(pl.multiple_of(T + k * T, T), T)

    def chunk0(k):
        return pl.ds(pl.multiple_of(k * T, T), T)

    def pack(stage):
        c = lax.rem(gi + stage, 2)

        def body(k, _):
            after, before = packed(ends(ice_fields(c), chunk(k)))
            pack_s[0, c, chunk0(k), :] = after
            pack_s[1, c, chunk0(k), :] = before
            return 0

        lax.fori_loop(0, ichunks, body, 0, unroll=ichunks)
        icols = col_copies(lambda way: pack_s.at[way, c], lambda way: pack_r.at[way, c], 4 * stage)
        start_all(icols, ti, tiles)
        return icols

    def pack_ocean():
        def body(k, _):
            after, before = packed(ends((gn, xn, bn), chunk(k)))
            opack_s[0, chunk0(k), :] = after
            opack_s[1, chunk0(k), :] = before
            return 0

        lax.fori_loop(0, ochunks, body, 0, unroll=17 if ochunks % 17 == 0 else 1)
        ocols = col_copies(lambda way: opack_s.at[way], lambda way: opack_r.at[way], 8)
        start_all(ocols, ti, tiles)
        return ocols

    def prep(phase):
        c = lax.rem(gi + phase, 2)

        def body(k, thick_up):
            at = chunk(k)
            fields = ice_fields(c)
            values = [[ref[at, pl.ds(j * L, L)] for ref in fields] for j in range(own)]
            before, after = pack_r[0, c, chunk0(k), :], pack_r[1, c, chunk0(k), :]
            values.append([unpacked(before, after, f) for f in range(len(fields))])
            thicks = [v[5] for v in values]
            beside = left(thicks)
            for j, (u, v, s0, s1, s2, thick, wx, wy) in enumerate(values):
                mass = thick + 1.0
                inverse = jnp.where(thick > 0.0, 1.0 / (mass + STEP * DRAG), 0.0)
                q = STEP * inverse
                half = 0.5 * q
                uu[c, j, at, :] = u
                vv[c, j, at, :] = v
                sp_p[c, j, at, :] = (s0 + s1) + STRENGTH * thick
                sp_m[c, j, at, :] = (s0 - s1) + STRENGTH * thick
                sp_s[c, j, at, :] = s2 + s2
                kk[c, j, at, :] = RATE * thick
                pp[c, j, at, :] = mass * inverse
                qq[c, j, at, :] = half
                slope = STRENGTH * half
                ww[0, c, j, at, :] = q * wx - slope * (thick - above(thick_up[j], thick))
                ww[1, c, j, at, :] = q * wy - slope * (thick - beside[j])
            return tuple(thicks)

        zero = jnp.zeros((T, L), F32)
        lax.fori_loop(0, ichunks, body, (zero,) * span, unroll=ichunks // 2)

    def ocean_chunk(k, _):
        at = chunk(k)
        before, after = opack_r[0, chunk0(k), :], opack_r[1, chunk0(k), :]
        values = [[ref[at, pl.ds(j * L, L)] for ref in (gn, xn, bn)] for j in range(own)]
        values.append([unpacked(before, after, f) for f in range(3)])
        for j, (depth, height, base) in enumerate(values):
            g[j, at, :] = depth
            gx[j, at, :] = depth * height
            x[j, at, :] = height
            r0[j, at, :] = jnp.where(depth > 0.0, base, 0.0)
        return 0

    def around(ref, k, lefts, rights):
        r = T + k * T
        up, down = pl.ds(r - 1, T), pl.ds(r + 1, T)
        lefts, rights = join_left(lefts), join_right(rights)
        return [
            (ref[j, up, :] + ref[j, down, :]) + (lefts[j] + rights[j]) for j in range(span)
        ]

    def turned(ref, k):
        values = [ref[j, chunk(k), :] for j in range(span)]
        return turn_left(values), turn_right(values)

    def pre_chunk(k, carry):
        at = chunk(k)
        ahead = (turned(g, k + 1), turned(gx, k + 1))
        g_near = around(g, k, *carry[0])
        near = around(gx, k, *carry[1])
        for j in range(span):
            depth = g[j, at, :]
            diag = DAMP + depth * g_near[j]
            inverse = 1.0 / diag
            r0[j, at, :] = r0[j, at, :] - diag * x[j, at, :] + depth * near[j]
            inv[j, at, :] = inverse
            gd[j, at, :] = depth * inverse
        return ahead

    def prepare_ocean():
        steps = 17 if ochunks % 17 == 0 else 2
        lax.fori_loop(0, ochunks, ocean_chunk, 0, unroll=steps)
        lax.fori_loop(0, ochunks, pre_chunk, (turned(g, 0), turned(gx, 0)), unroll=steps)

    def flow_wait(phase, part):
        for target in range(groups):

            @pl.when(gi == target)
            def _():
                cap = (target + phase) % 2
                lo, hi, start = flow_span(target)
                width = 2 * L if part == 0 else cols - 2 * L
                ref = flow.at[:, cap, start : start + hi - lo, 0:width]
                take(ref, flow_recv.at[2 * cap + part])

    def pack_flow(phase):
        c = lax.rem(gi + phase, 2)

        def fpack_chunk(k, _):
            after, before = packed(ends((flow.at[0, c], flow.at[1, c]), chunk(k)))
            fpack_s[0, c, chunk0(k), :] = after
            fpack_s[1, c, chunk0(k), :] = before
            return 0

        lax.fori_loop(0, ichunks, fpack_chunk, 0, unroll=ichunks)
        fcols = col_copies(
            lambda way: fpack_s.at[way, c], lambda way: fpack_r.at[way, c], 4 * phase + 2
        )
        start_all(fcols, ti, tiles)
        return fcols

    def add_flow(phase):
        c = lax.rem(gi + phase, 2)

        def flow_chunk(k, _):
            at = chunk(k)
            before, after = fpack_r[0, c, chunk0(k), :], fpack_r[1, c, chunk0(k), :]
            for comp in range(2):
                values = [flow[comp, c, at, pl.ds(j * L, L)] for j in range(own)]
                values.append(unpacked(before, after, comp))
                flow_edge[comp, c, at, :] = values[own]
                for j in range(span):
                    ww[comp, c, j, at, :] = ww[comp, c, j, at, :] + qq[c, j, at, :] * (
                        2.0 * DRAG * values[j]
                    )
            return 0

        lax.fori_loop(0, ichunks, flow_chunk, 0, unroll=ichunks)

    def subcycles(phase, first, last):
        c = lax.rem(gi + phase, 2)

        def subcycle(n, _):
            ahead, behind = 2, 2
            turned_u, turned_v, turned_m, turned_s = {}, {}, {}, {}

            def look(k):
                at = slice(T + T * k, TOP + T * k)
                turned_u[k] = turn_right([uu[c, j, at, :] for j in range(span)])
                turned_v[k] = turn_right([vv[c, j, at, :] for j in range(span)])

            def stress(k):
                at, down = slice(T + T * k, TOP + T * k), slice(T + T * k + 1, TOP + T * k + 1)
                beside_u, beside_v = join_right(turned_u.pop(k)), join_right(turned_v.pop(k))
                ms, ss = [], []
                for j in range(span):
                    u, v = uu[c, j, at, :], vv[c, j, at, :]
                    du = uu[c, j, down, :] - u
                    dv = beside_v[j] - v
                    shear = (beside_u[j] - u) + (vv[c, j, down, :] - v)
                    rate = kk[c, j, at, :] * lax.rsqrt(
                        (du * du + dv * dv) + (0.5 * (shear * shear) + 0.5)
                    )
                    sp_p[c, j, at, :] = sp_p[c, j, at, :] * KEEP + rate * du
                    m = sp_m[c, j, at, :] * KEEP + rate * dv
                    s = sp_s[c, j, at, :] * KEEP + rate * shear
                    sp_m[c, j, at, :] = m
                    sp_s[c, j, at, :] = s
                    ms.append(m)
                    ss.append(s)
                turned_m[k], turned_s[k] = turn_left(ms), turn_left(ss)

            def momentum(k):
                at, up = slice(T + T * k, TOP + T * k), slice(T + T * k - 1, TOP + T * k - 1)
                beside_m, beside_s = join_left(turned_m.pop(k)), join_left(turned_s.pop(k))
                for j in range(span):
                    s = sp_s[c, j, at, :]
                    fx = (sp_p[c, j, at, :] - sp_p[c, j, up, :]) + (s - beside_s[j])
                    fy = (sp_m[c, j, at, :] - beside_m[j]) + (s - sp_s[c, j, up, :])
                    p, q = pp[c, j, at, :], qq[c, j, at, :]
                    uu[c, j, at, :] = p * uu[c, j, at, :] + (q * fx + ww[0, c, j, at, :])
                    vv[c, j, at, :] = p * vv[c, j, at, :] + (q * fy + ww[1, c, j, at, :])

            for k in range(-ahead, ichunks + behind):
                if k + ahead < ichunks:
                    look(k + ahead)
                if 0 <= k < ichunks:
                    stress(k)
                if 0 <= k - behind < ichunks:
                    momentum(k - behind)
            return 0

        lax.fori_loop(first, last, subcycle, 0)

    def drag(phase):
        c = lax.rem(gi + phase, 2)
        home = c * (groups - 1)
        edge_lanes = L // (2 * (rows // T))

        def drag_chunk(k, drag_up):
            at = pl.ds(pl.multiple_of(TOP + k * T, T), T)
            drags = []
            for comp, ref in enumerate((uu, vv)):
                values = [flow[comp, c, at, pl.ds(j * L, L)] for j in range(own)]
                values.append(flow_edge[comp, c, at, :])
                drags.append(
                    [
                        jnp.where(qq[c, j, at, :] > 0.0, DRAG * (ref[c, j, at, :] - values[j]), 0.0)
                        for j in range(span)
                    ]
                )
            beside = left(drags[1])
            for j in range(span):
                d0 = drags[0][j]
                d0_up = above(drag_up[j], d0)
                value = (d0 - d0_up) + (drags[1][j] - beside[j])
                if j < own:
                    sp[c, j, chunk0(k), :] = value
                else:
                    rim = value
            return tuple(drags[0]), rim

        zero = jnp.zeros((T, L), F32)
        upper, rims = (zero,) * span, zero
        for k in range(rows // T):
            upper, rim = drag_chunk(k, upper)
            width = 2 * edge_lanes
            here = (lane >= width * k) & (lane < width * k + width)
            rims = jnp.where(here, pltpu.roll(rim, (edge_lanes + width * k) % L, 1), rims)
        trim_s[c, 0] = rims
        row = lax.broadcasted_iota(jnp.int32, (T, L), 0)
        last = zero
        for j in range(span):
            last = jnp.where(row == j, upper[j][T - 1 : T, :], last)
        trim_s[c, 1] = last

        @pl.when(gi != home)
        def _():
            for copy in back_copies(phase, c, gi, home):
                copy.start()

        if phase == 1:
            for source, target, copy in edge_copies():
                pl.when(gi == source)(copy.start)

        @pl.when(gi == home)
        def _():
            row = pl.multiple_of(TOP + gi * rows, T)
            for j in range(own):

                def own_chunk(k, _):
                    forcing[j, pl.ds(pl.multiple_of(row + k * T, T), T), :] = sp[c, j, chunk0(k), :]
                    return 0

                lax.fori_loop(0, rows // T, own_chunk, 0, unroll=rows // T)
            trim_r[gi] = trim_s[c]

    def output(phase):
        c = lax.rem(gi + phase, 2)

        def out_chunk(k, _):
            at = pl.ds(pl.multiple_of(TOP + k * T, T), T)
            to = chunk0(k)
            for j in range(own):
                here = pl.ds(j * L, L)
                vel_out[0, c, to, here] = uu[c, j, at, :]
                vel_out[1, c, to, here] = vv[c, j, at, :]
                p, m = sp_p[c, j, at, :], sp_m[c, j, at, :]
                stress_out[0, c, to, here] = 0.5 * (p + m) - STRENGTH * h[c, at, here]
                stress_out[1, c, to, here] = 0.5 * (p - m)
                stress_out[2, c, to, here] = 0.5 * sp_s[c, j, at, :]
            return 0

        lax.fori_loop(0, rows // T, out_chunk, 0, unroll=4)

    def back_copies(phase, c, source, target):
        at = pl.ds(pl.multiple_of(TOP + source * rows, T), rows)
        parts = ((sp.at[c], forcing.at[0:own, at, :]), (trim_s.at[c], trim_r.at[source]))
        return [
            pltpu.make_async_remote_copy(
                src_ref=src,
                dst_ref=dst,
                send_sem=back_send.at[phase],
                recv_sem=back_recv.at[source],
                device_id=(target, ti),
                device_id_type=MESH,
            )
            for src, dst in parts
        ]

    def edge_copies():
        top, bottom = groups - 1, 0
        parts = (
            (0, top, 1, sp.at[0, :, rows - T : rows, :], forcing.at[0:own, TOP - T : TOP, :]),
            (0, top, 1, trim_s.at[0], trim_r.at[0]),
            (1, bottom, groups - 2, sp.at[1, :, 0:T, :], forcing.at[0:own, oend : oend + T, :]),
            (1, bottom, groups - 2, trim_s.at[1], trim_r.at[0]),
        )
        return [
            (
                source,
                target,
                pltpu.make_async_remote_copy(
                    src_ref=src,
                    dst_ref=dst,
                    send_sem=edge_send,
                    recv_sem=edge_recv,
                    device_id=(target, ti),
                    device_id_type=MESH,
                ),
            )
            for way, source, target, src, dst in parts
        ]

    back_rows = own * rows + 2 * T
    edge_rows = own * T + 2 * T

    receive_rows(0, 8 * T)
    icols_a = pack(0)
    receive_rows(2, 3 * T)
    ocols = pack_ocean()
    flow_wait(0, 0)
    fcols_a = pack_flow(0)
    receive_all(icols_a, ti, tiles)
    prep(0)
    receive_all(ocols, ti, tiles)
    prepare_ocean()
    receive_rows(1, 8 * T)
    icols_b = pack(1)
    flow_wait(0, 1)
    receive_all(fcols_a, ti, tiles)
    add_flow(0)
    subcycles(0, 0, NSUB // 2)
    flow_wait(1, 0)
    fcols_b = pack_flow(1)
    subcycles(0, NSUB // 2, NSUB)
    drag(0)
    output(0)
    receive_all(icols_b, ti, tiles)
    prep(1)
    flow_wait(1, 1)
    receive_all(fcols_b, ti, tiles)
    add_flow(1)
    subcycles(1, 0, NSUB)
    drag(1)
    output(1)

    def rim_of(source, k):
        lanes_each = L // (2 * (rows // T))
        turn = (lanes_each + 2 * lanes_each * k) % L
        value = pltpu.roll(trim_r[source, 0], (L - turn) % L, 1)
        return jnp.where((lane < lanes_each) | (lane >= L - lanes_each), value, 0.0)

    def carry_over(row, source):
        for j in range(span):
            at = (j, slice(row, row + 1), slice(None))
            forcing[at] = forcing[at] - trim_r[source, 1, j : j + 1, :]

    for cap, home in enumerate(homes):

        @pl.when(gi == home)
        def _():
            early = [k for k in range(groups) if k != home and (k + cap) % 2 == 0]
            late = [k for k in range(groups) if k != home and (k + cap) % 2 == 1]
            for some in ([home] + early, late):
                for source in some:
                    if source != home:
                        take(w0.at[0, 0:back_rows, :], back_recv.at[source])
                for source in some:
                    for k in range(rows // T):
                        row = TOP + source * rows + k * T
                        forcing[own, row : row + T, :] = rim_of(source, k)
            for source in range(groups):
                carry_over(TOP + (source + 1) * rows, source)

    @pl.when(gi == 1)
    def _():
        take(w0.at[0, 0:edge_rows, :], edge_recv)
        forcing[own, TOP - T : TOP, :] = rim_of(0, rows // T - 1)
        carry_over(TOP, 0)

    @pl.when(gi == groups - 2)
    def _():
        take(w0.at[0, 0:edge_rows, :], edge_recv)
        forcing[own, oend : oend + T, :] = rim_of(0, 0)

    zero = jnp.zeros((T, L), F32)

    def fold(first, second):
        total = first[0] * second[0]
        for j in range(1, own):
            total = total + first[j] * second[j]
        return total

    def first_chunk(k):
        at = chunk(k)
        r, z = [], []
        for j in range(span):
            depth = g[j, at, :]
            r.append(r0[j, at, :] + jnp.where(depth > 0.0, forcing[j, at, :], 0.0))
            z.append(r[j] * inv[j, at, :])
            v0[j, at, :] = z[j]
            w0[j, at, :] = depth * z[j]
        return fold(r, z)

    first_chunk(0)
    first_chunk(ochunks - 1)
    m0 = lax.fori_loop(1, ochunks - 1, lambda k, s: s + first_chunk(k), zero, unroll=8)

    def power(w_from, v_to, w_to):
        def body(k, turns):
            at = chunk(k)
            near = around(w_from, k, *turns)
            w_here = [w_from[j, at, :] for j in range(own)]
            w_next = []
            for j in range(span):
                v = gd[j, at, :] * near[j]
                w = g[j, at, :] * v
                if j < own:
                    v_to[j, at, :] = v
                w_to[j, at, :] = w
                w_next.append(w)
            return fold(w_here, near), fold(w_next, near)

        body(0, turned(w_from, 0))
        body(ochunks - 1, turned(w_from, ochunks - 1))

        def step(k, carry):
            turns, after, s0, s1 = carry
            ahead = turned(w_from, k + 2)
            a, b = body(k, turns)
            return after, ahead, s0 + a, s1 + b

        carry = (turned(w_from, 1), turned(w_from, 2), zero, zero)
        _, _, s0, s1 = lax.fori_loop(1, ochunks - 1, step, carry, unroll=ochunks - 2)
        return s0, s1

    m1, m2 = power(w0, v1, w1)
    m3, m4 = power(w1, v2, w2)

    def last_step(k, carry):
        turns, after, s = carry
        ahead = turned(w2, k + 2)
        near = around(w2, k, *turns)
        return after, ahead, s + fold([w2[j, chunk(k), :] for j in range(own)], near)

    carry = (turned(w2, 1), turned(w2, 2), zero)
    _, _, m5 = lax.fori_loop(1, ochunks - 1, last_step, carry, unroll=ochunks - 2)

    row = lax.broadcasted_iota(jnp.int32, (T, L), 0)
    moments = zero
    for k, m in enumerate((m0, m1, m2, m3, m4, m5)):
        moments = jnp.where(row == k, jnp.sum(m, axis=0, keepdims=True), moments)

    lane_sums = jnp.sum(moments, axis=1, keepdims=True)
    diagonal = lanes(T, L) == row
    red_s[...] = jnp.sum(jnp.where(diagonal, lane_sums, 0.0), axis=0, keepdims=True)

    pl.semaphore_wait(ready, tiles - 1)
    count = groups * tiles
    for d in range(1, count):
        other = lax.rem(gi * tiles + ti + d, count)
        pltpu.make_async_remote_copy(
            src_ref=red_s,
            dst_ref=red_r.at[d],
            send_sem=red_send,
            recv_sem=red_recv,
            device_id=(lax.div(other, tiles), lax.rem(other, tiles)),
            device_id_type=MESH,
        ).start()
    take(red_r.at[1:count], red_recv)
    parts = [red_s[...]] + [red_r[d] for d in range(1, count)]
    while len(parts) > 1:
        parts = [sum(parts[i : i + 2]) for i in range(0, len(parts), 2)]
    moments = jnp.where(diagonal, parts[0], 0.0)
    total = jnp.sum(moments, axis=1, keepdims=True)
    nu = [total[k : k + 1, :] for k in range(6)]
    a = [nu[k] - nu[k + 1] for k in range(5)]

    tiny = 1e-12

    def safe(value, scale):
        ok = value > tiny * scale
        return jnp.where(ok, 1.0 / jnp.where(ok, value, 1.0), 0.0)

    i0 = safe(a[0], 0.0 * a[0])
    l10, l20 = a[1] * i0, a[2] * i0
    d1 = a[2] - l10 * a[1]
    i1 = safe(d1, a[2])
    e21 = a[3] - l20 * a[1]
    l21 = e21 * i1
    d2 = a[4] - l20 * a[2] - l21 * e21
    i2 = safe(d2, a[4])
    y0 = nu[0]
    y1 = nu[1] - l10 * y0
    y2 = nu[2] - l20 * y0 - l21 * y1
    c2 = y2 * i2
    c1 = y1 * i1 - l21 * c2
    c0 = y0 * i0 - l10 * c1 - l20 * c2

    def final_chunk(k, _):
        at = pl.ds(pl.multiple_of(TOP + k * T, T), T)
        for j in range(own):
            ssh_out[chunk0(k), pl.ds(j * L, L)] = x[j, at, :] + (
                c0 * v0[j, at, :] + (c1 * v1[j, at, :] + c2 * v2[j, at, :])
            )
        return 0

    lax.fori_loop(0, orows // T, final_chunk, 0, unroll=16)
    for way in range(2):
        pl.when(edge(way, gi, groups)[0])(
            lambda: take(gn.at[0 : 19 * T, :], row_send.at[way])
        )
        sent = 2 * (rows + 2 * T) + (orows + 2 * T) // 2
        pl.when(edge(way, ti, tiles)[0])(lambda: take(w0.at[0:2, 0:sent, :], col_send.at[way]))
    for cap, home in enumerate(homes):

        @pl.when(gi == home)
        def _():
            spans = [flow_span(k) for k in range(groups) if k != home]
            take(cur_in.at[:, 0 : sum(hi - lo for lo, hi, _ in spans), :], flow_send)

    for phase in range(2):
        pl.when(gi != lax.rem(gi + phase, 2) * (groups - 1))(
            lambda: take(w0.at[0, 0:back_rows, :], back_send.at[phase])
        )
    pl.when((gi == 0) | (gi == groups - 1))(lambda: take(w0.at[0, 0:edge_rows, :], edge_send))
    take(red_r.at[1:count], red_send)


def deliver(*refs):
    sems = refs[-1]
    half = len(refs) // 2
    copies = [
        pltpu.make_async_copy(src, dst, sems.at[k])
        for k, (src, dst) in enumerate(zip(refs[:half], refs[half:-1]))
    ]
    for copy in copies:
        copy.start()
    for copy in copies:
        copy.wait()


def step(groups, tiles, *args):
    base_rhs, thick, ice_vel, ice_stress = args[0], args[5], args[7], args[8]
    orows, cols = base_rhs.shape
    rows = thick.shape[1]
    irows = rows + 2 * TOP
    erows = orows + 2 * TOP
    span = cols // L + 1
    hbm = pl.BlockSpec(memory_space=pltpu.HBM)
    vmem = pl.BlockSpec(memory_space=pltpu.VMEM)
    dma = pltpu.SemaphoreType.DMA
    ice = pltpu.VMEM((2, span, irows + PAD, L), F32)
    ocean = pltpu.VMEM((span, erows + PAD, L), F32)
    plain = pltpu.VMEM((erows, cols), F32)
    results = pl.pallas_call(
        functools.partial(kernel, groups, tiles),
        out_shape=(
            pltpu.VMEM(base_rhs.shape, F32),
            pltpu.VMEM(ice_vel.shape, F32),
            pltpu.VMEM(ice_stress.shape, F32),
        ),
        in_specs=[hbm] * 10,
        out_specs=(vmem,) * 3,
        scratch_shapes=[
            pltpu.VMEM(args[4].shape, jnp.int32),
            pltpu.VMEM(args[6].shape, jnp.int32),
            pltpu.VMEM((2, 2, irows, cols), F32),
            pltpu.VMEM((3, 2, irows, cols), F32),
            pltpu.VMEM((2, 2, irows, cols), F32),
            pltpu.VMEM((2, 2, irows, cols), F32),
            pltpu.VMEM((2, irows, cols), F32),
            plain,
            plain,
            plain,
        ]
        + [ice] * 8
        + [
            pltpu.VMEM((2, 2, span, irows + PAD, L), F32),
            pltpu.VMEM((2, 2, irows, L), F32),
        ]
        + [ocean] * 13
        + [
            pltpu.VMEM((orows // BS, cols), F32),
            pltpu.VMEM((2, rows // BS, cols), F32),
            pltpu.VMEM((2, 2, rows + 2 * T, L), F32),
            pltpu.VMEM((2, 2, rows + 2 * T, L), F32),
            pltpu.VMEM((2, 2, rows + 2 * T, L), F32),
            pltpu.VMEM((2, 2, rows + 2 * T, L), F32),
            pltpu.VMEM((2, orows + 2 * T, L), F32),
            pltpu.VMEM((2, orows + 2 * T, L), F32),
            pltpu.VMEM((2, span - 1, rows, L), F32),
            pltpu.VMEM((2, 2, T, L), F32),
            pltpu.VMEM((groups, 2, T, L), F32),
            pltpu.VMEM((1, L), F32),
            pltpu.VMEM((groups * tiles, 1, L), F32),
            dma((9,)),
            dma,
            dma((4,)),
            dma((2,)),
            dma((6,)),
            dma((2,)),
            dma((10,)),
            dma((2,)),
            dma((groups,)),
            dma,
            dma,
            dma,
            dma,
            pltpu.SemaphoreType.REGULAR,
        ],
        compiler_params=pltpu.CompilerParams(
            collective_id=0, has_side_effects=True, vmem_limit_bytes=48 * 2**20
        ),
    )(*(pltpu.with_memory_space_constraint(a, pltpu.HBM) for a in args))
    return pl.pallas_call(
        deliver,
        out_shape=tuple(jax.ShapeDtypeStruct(r.shape, F32) for r in results),
        in_specs=[vmem] * 3,
        out_specs=(hbm,) * 3,
        scratch_shapes=[dma((3,))],
        compiler_params=pltpu.CompilerParams(vmem_limit_bytes=4 * 2**20),
    )(*results)


def solution(mesh):
    grid = P("grp", "tile")
    plane = P(None, "grp", "tile")
    stack = P(None, None, "grp", "tile")
    return jax.shard_map(
        functools.partial(step, mesh.shape["grp"], mesh.shape["tile"]),
        mesh=mesh,
        in_specs=(grid, grid, grid, plane, grid, plane, plane, stack, stack, stack),
        out_specs=(grid, stack, stack),
        check_vma=False,
    )
```

```python
import functools
import math

import jax
import jax.numpy as jnp
from jax import lax
from jax.experimental import pallas as pl
from jax.experimental.pallas import tpu as pltpu
from jax.sharding import PartitionSpec as P

BS = 8
NSUB = 8

DAMP = 0.05
RELAX = 0.2
STRENGTH = 0.5
DRAG = 1.0
STEP = 0.5
KEEP = 1.0 / (1.0 + RELAX)
RATE = math.sqrt(2.0) * RELAX * STRENGTH / (1.0 + RELAX)

MESH = pl.DeviceIdType.MESH
F32 = jnp.float32
T = 8
L = 128
W = 12
TOP = 2 * T
PAD = 2 * T


def lanes(rows, width):
    return lax.broadcasted_iota(jnp.int32, (rows, width), 1)


def above(prev, here):
    row = lax.broadcasted_iota(jnp.int32, here.shape, 0)
    return pltpu.roll(jnp.where(row == T - 1, prev, here), 1, 0)


def turn_right(tiles):
    return [pltpu.roll(x, L - 1, 1) for x in tiles]


def turn_left(tiles):
    return [pltpu.roll(x, 1, 1) for x in tiles]


def join_right(turned):
    lane = lanes(T, L)
    n = len(turned)
    return [jnp.where(lane == L - 1, turned[(j + 1) % n], turned[j]) for j in range(n)]


def join_left(turned):
    lane = lanes(T, L)
    n = len(turned)
    return [jnp.where(lane == 0, turned[(j - 1) % n], turned[j]) for j in range(n)]


def right(tiles):
    return join_right(turn_right(tiles))


def left(tiles):
    return join_left(turn_left(tiles))


def kernel(
    groups,
    tiles,
    base_in,
    depth_in,
    ssh_in,
    cur_in,
    land_in,
    thick_in,
    ice_in,
    vel_in,
    stress_in,
    wind_in,
    ssh_out,
    vel_out,
    stress_out,
    land_ref,
    ice_ref,
    vel,
    st,
    wind,
    flow,
    h,
    gn,
    xn,
    bn,
    uu,
    vv,
    sp_p,
    sp_m,
    sp_s,
    kk,
    pp,
    qq,
    ww,
    flow_edge,
    g,
    gx,
    r0,
    x,
    inv,
    gd,
    forcing,
    v0,
    v1,
    v2,
    w0,
    w1,
    w2,
    wet,
    cover,
    pack_s,
    pack_r,
    fpack_s,
    fpack_r,
    opack_s,
    opack_r,
    sp,
    trim_s,
    trim_r,
    red_s,
    red_r,
    load_sem,
    flow_send,
    flow_recv,
    row_send,
    row_recv,
    col_send,
    col_recv,
    back_send,
    back_recv,
    edge_send,
    edge_recv,
    red_send,
    red_recv,
    ready,
):
    gi = lax.axis_index("grp")
    ti = lax.axis_index("tile")
    rows, cols = thick_in.shape[1], thick_in.shape[2]
    orows = base_in.shape[0]
    end = TOP + rows
    oend = TOP + orows
    own = cols // L
    span = own + 1
    ichunks = rows // T + 2
    ochunks = orows // T + 2
    split = rows - 2 * T
    above_split, below_split = (0, split // T + 2), (split // T, ichunks)

    barrier = pltpu.get_barrier_semaphore()
    for d in range(1, groups):
        pl.semaphore_signal(
            barrier, inc=1, device_id=(lax.rem(gi + d, groups), ti), device_id_type=MESH
        )
    for d in range(1, tiles):
        pl.semaphore_signal(
            barrier, inc=1, device_id=(gi, lax.rem(ti + d, tiles)), device_id_type=MESH
        )

    loads = []

    def load(src, dst):
        copy = pltpu.make_async_copy(src, dst, load_sem.at[len(loads)])
        copy.start()
        loads.append(copy)
        return copy

    load_land = load(land_in, land_ref)
    load_ice = load(ice_in, ice_ref)
    load_thick = load(thick_in, h.at[:, TOP:end, :])
    load_vel = load(vel_in, vel.at[:, :, TOP:end, :])
    load_st = load(stress_in, st.at[:, :, TOP:end, :])
    load_wind = load(wind_in, wind.at[:, :, TOP:end, :])
    load_depth = load(depth_in, gn.at[TOP:oend, :])
    load_x = load(ssh_in, xn.at[TOP:oend, :])
    load_b = load(base_in, bn.at[TOP:oend, :])

    def clear(ref, *spans):
        for lo, hi in spans:
            ref[..., lo:hi, :] = jnp.zeros(ref.shape[:-2] + (hi - lo, ref.shape[-1]), F32)

    for outer, before in ((gi == 0, True), (gi == groups - 1, False)):

        @pl.when(outer)
        def _():
            for ref in (vel, st, wind, flow, h):
                clear(ref, (T, TOP) if before else (end, end + T))
            for ref in (gn, xn, bn):
                clear(ref, (T, TOP) if before else (oend, oend + T))
            clear(forcing, (T, TOP), (oend, oend + T))

    for outer, way in ((ti == 0, 0), (ti == tiles - 1, 1)):

        @pl.when(outer)
        def _():
            for ref in (pack_r, fpack_r, opack_r):
                ref[way] = jnp.zeros(ref.shape[1:], F32)

    @pl.when((gi > 0) & (gi < groups - 1))
    def _():
        clear(forcing, (TOP, oend))
        pl.when(gi != 1)(lambda: clear(forcing, (T, TOP)))
        pl.when(gi != groups - 2)(lambda: clear(forcing, (oend, oend + T)))

    for ref in (uu, vv, sp_p, sp_m, sp_s):
        clear(ref, (0, T), (end + T, end + 2 * T))
    for ref in (g, gx, w0, w1, w2):
        clear(ref, (0, T), (oend + T, oend + 2 * T))

    def blocks(ref, out, count):
        width = ref.shape[-1]
        row = lax.broadcasted_iota(jnp.int32, (width, cols), 0)
        spread = (row == lax.shift_right_logical(lanes(width, cols), 3)).astype(F32)
        values = ref[...].reshape((count, width)).astype(F32)
        out[...] = jnp.dot(values, spread, preferred_element_type=F32)

    pl.semaphore_wait(barrier, groups + tiles - 2)
    for d in range(1, tiles):
        pl.semaphore_signal(
            ready, inc=1, device_id=(gi, lax.rem(ti + d, tiles)), device_id_type=MESH
        )

    homes = (0, groups - 1)
    pieces = ((0, L), (cols - L, cols), (L, cols - L))

    def flow_span(target):
        lo = max(0, rows * target - T)
        hi = min(rows * groups, rows * target + rows + T)
        return lo, hi, TOP + lo - rows * target

    def flow_parts(cap, target):
        lo, hi, start = flow_span(target)
        if (cap + target) % 2 == 0:
            return ((lo, hi, start),)
        middle = TOP + split + T
        return ((lo, lo + middle - start, start), (lo + middle - start, hi, middle))

    def flow_copies(cap, target):
        out = []
        for part, (lo, hi, start) in enumerate(flow_parts(cap, target)):
            for piece, (first, last) in enumerate(pieces):
                src = cur_in.at[:, lo:hi, first:last]
                dst = flow.at[:, cap, start : start + hi - lo, first:last]
                recv = flow_recv.at[4 * cap + 2 * part + piece // 2]
                if target == homes[cap]:
                    out.append(pltpu.make_async_copy(src, dst, recv))
                else:
                    out.append(
                        pltpu.make_async_remote_copy(
                            src_ref=src,
                            dst_ref=dst,
                            send_sem=flow_send,
                            recv_sem=recv,
                            device_id=(target, ti),
                            device_id_type=MESH,
                        )
                    )
        return out

    def take(ref, sem):
        pltpu.make_async_copy(ref, ref, sem).wait()

    def row_copy(k, way, src, dst, first, after, ends):
        count, last = ends
        from_row = first + count - T if way == 0 else first
        to_row = after - T if way == 0 else last
        return (
            way,
            pltpu.make_async_remote_copy(
                src_ref=src(pl.ds(from_row, T)),
                dst_ref=dst(pl.ds(to_row, T)),
                send_sem=row_send.at[way],
                recv_sem=row_recv.at[2 * k + way],
                device_id=(lax.rem(gi + (1 if way == 0 else groups - 1), groups), ti),
                device_id_type=MESH,
            ),
        )

    def ice_rows(stage):
        c = lax.rem(gi + 1 + stage, 2)
        out = []
        for ref in (vel, st, wind):
            for way in range(2):
                out.append(
                    row_copy(
                        stage,
                        way,
                        lambda at, ref=ref: ref.at[:, c, at, :],
                        lambda at, ref=ref: ref.at[:, c, at, :],
                        TOP,
                        TOP,
                        (rows, end),
                    )
                )
        return out

    def thick_rows(stage):
        c = lax.rem(gi + 1 + stage, 2)
        return [
            row_copy(
                stage,
                way,
                lambda at: h.at[c, at, :],
                lambda at: h.at[c, at, :],
                TOP,
                TOP,
                (rows, end),
            )
            for way in range(2)
        ]

    def ocean_rows():
        return [
            row_copy(
                2,
                way,
                lambda at, ref=ref: ref.at[at, :],
                lambda at, ref=ref: ref.at[at, :],
                TOP,
                TOP,
                (orows, oend),
            )
            for ref in (xn, bn, gn)
            for way in range(2)
        ]

    def edge(way, index, count):
        sends = index < count - 1 if way == 0 else index > 0
        receives = index > 0 if way == 0 else index < count - 1
        return sends, receives

    def start_all(copies, index, count):
        for way, copy in copies:
            pl.when(edge(way, index, count)[0])(copy.start)

    def receive_all(copies, index, count):
        for way, copy in copies:
            pl.when(edge(way, index, count)[1])(copy.wait_recv)

    def receive_rows(k, count):
        for way in range(2):
            pl.when(edge(way, gi, groups)[1])(
                lambda: take(gn.at[0:count, :], row_recv.at[2 * k + way])
            )

    for cap, home in enumerate(homes):

        @pl.when(gi == home)
        def _():
            for copy in flow_copies(cap, home):
                copy.start()

    load_vel.wait()
    load_st.wait()
    load_wind.wait()
    start_all(ice_rows(0), gi, groups)
    load_land.wait()
    load_ice.wait()
    blocks(land_ref, wet, land_ref.shape[0])
    for c in range(2):
        row = lax.broadcasted_iota(jnp.int32, (cols // BS, cols), 0)
        spread = (row == lax.shift_right_logical(lanes(cols // BS, cols), 3)).astype(F32)
        cover[c] = jnp.dot(ice_ref[c].astype(F32), spread, preferred_element_type=F32)
    load_thick.wait()

    def cover_chunk(k, _):
        for c in range(2):
            at = (c, pl.ds(pl.multiple_of(TOP + k * T, T), T), slice(None))
            h[at] = h[at] * cover[c, pl.ds(k, 1), :]
        return 0

    lax.fori_loop(0, rows // T, cover_chunk, 0, unroll=4)
    start_all(thick_rows(0), gi, groups)
    load_depth.wait()

    def wet_chunk(k, _):
        at = (pl.ds(pl.multiple_of(TOP + k * T, T), T), slice(None))
        gn[at] = gn[at] * wet[pl.ds(k, 1), :]
        return 0

    lax.fori_loop(0, orows // T, wet_chunk, 0, unroll=4)
    load_x.wait()
    load_b.wait()
    start_all(ocean_rows(), gi, groups)

    def send_flow(which):
        for cap, home in enumerate(homes):

            @pl.when(gi == home)
            def _():
                order = sorted((k for k in range(groups) if k != home), key=lambda k: abs(k - home))
                for target in which(order):
                    for copy in flow_copies(cap, target):
                        copy.start()

    send_flow(lambda order: order[1:])
    start_all(ice_rows(1), gi, groups)
    start_all(thick_rows(1), gi, groups)
    send_flow(lambda order: order[:1])

    lane = lanes(T, L)

    def col_copies(src, dst, base):
        out = []
        for way in range(2):
            out.append(
                (
                    way,
                    pltpu.make_async_remote_copy(
                        src_ref=src(way),
                        dst_ref=dst(way),
                        send_sem=col_send.at[way],
                        recv_sem=col_recv.at[base + way],
                        device_id=(gi, lax.rem(ti + (1 if way == 0 else tiles - 1), tiles)),
                        device_id_type=MESH,
                    ),
                )
            )
        return out

    def packed(values):
        after = jnp.zeros((T, L), F32)
        before = jnp.zeros((T, L), F32)
        for f, (first, last) in enumerate(values):
            here = (lane >= W * f) & (lane < W * f + W)
            after = jnp.where(here, pltpu.roll(last, (W * f + W) % L, 1), after)
            before = jnp.where(here, pltpu.roll(first, W * f, 1) if f else first, before)
        return after, before

    def unpacked(from_before, from_after, f):
        low = pltpu.roll(from_before, (L - W - W * f) % L, 1)
        high = pltpu.roll(from_after, (L - W * f) % L, 1) if f else from_after
        return jnp.where(lane < W, high, jnp.where(lane >= L - W, low, 0.0))

    def ends(refs, at):
        return [(ref[at, pl.ds(0, L)], ref[at, pl.ds(cols - L, L)]) for ref in refs]

    def ice_fields(c):
        return (
            vel.at[0, c],
            vel.at[1, c],
            st.at[0, c],
            st.at[1, c],
            st.at[2, c],
            h.at[c],
            wind.at[0, c],
            wind.at[1, c],
        )

    def chunk(k):
        return pl.ds(pl.multiple_of(T + k * T, T), T)

    def chunk0(k):
        return pl.ds(pl.multiple_of(k * T, T), T)

    def pack(stage):
        c = lax.rem(gi + stage, 2)

        def body(k, _):
            after, before = packed(ends(ice_fields(c), chunk(k)))
            pack_s[0, c, chunk0(k), :] = after
            pack_s[1, c, chunk0(k), :] = before
            return 0

        lax.fori_loop(0, ichunks, body, 0, unroll=ichunks)
        icols = col_copies(lambda way: pack_s.at[way, c], lambda way: pack_r.at[way, c], 4 * stage)
        start_all(icols, ti, tiles)
        return icols

    def pack_ocean():
        def body(k, _):
            after, before = packed(ends((gn, xn, bn), chunk(k)))
            opack_s[0, chunk0(k), :] = after
            opack_s[1, chunk0(k), :] = before
            return 0

        lax.fori_loop(0, ochunks, body, 0, unroll=17 if ochunks % 17 == 0 else 1)
        ocols = col_copies(lambda way: opack_s.at[way], lambda way: opack_r.at[way], 8)
        start_all(ocols, ti, tiles)
        return ocols

    def prep(phase):
        c = lax.rem(gi + phase, 2)

        def body(k, thick_up):
            at = chunk(k)
            fields = ice_fields(c)
            values = [[ref[at, pl.ds(j * L, L)] for ref in fields] for j in range(own)]
            before, after = pack_r[0, c, chunk0(k), :], pack_r[1, c, chunk0(k), :]
            values.append([unpacked(before, after, f) for f in range(len(fields))])
            thicks = [v[5] for v in values]
            beside = left(thicks)
            for j, (u, v, s0, s1, s2, thick, wx, wy) in enumerate(values):
                mass = thick + 1.0
                inverse = jnp.where(thick > 0.0, 1.0 / (mass + STEP * DRAG), 0.0)
                q = STEP * inverse
                half = 0.5 * q
                for slot in (c,) if phase == 0 else (c, 2):
                    uu[slot, j, at, :] = u
                    vv[slot, j, at, :] = v
                    sp_p[slot, j, at, :] = (s0 + s1) + STRENGTH * thick
                    sp_m[slot, j, at, :] = (s0 - s1) + STRENGTH * thick
                    sp_s[slot, j, at, :] = s2 + s2
                kk[c, j, at, :] = RATE * thick
                pp[c, j, at, :] = mass * inverse
                qq[c, j, at, :] = half
                slope = STRENGTH * half
                ww[0, c, j, at, :] = q * wx - slope * (thick - above(thick_up[j], thick))
                ww[1, c, j, at, :] = q * wy - slope * (thick - beside[j])
            return tuple(thicks)

        zero = jnp.zeros((T, L), F32)
        lax.fori_loop(0, ichunks, body, (zero,) * span, unroll=ichunks // 2)

    def ocean_chunk(k, _):
        at = chunk(k)
        before, after = opack_r[0, chunk0(k), :], opack_r[1, chunk0(k), :]
        values = [[ref[at, pl.ds(j * L, L)] for ref in (gn, xn, bn)] for j in range(own)]
        values.append([unpacked(before, after, f) for f in range(3)])
        for j, (depth, height, base) in enumerate(values):
            g[j, at, :] = depth
            gx[j, at, :] = depth * height
            x[j, at, :] = height
            r0[j, at, :] = jnp.where(depth > 0.0, base, 0.0)
        return 0

    def around(ref, k, lefts, rights):
        r = T + k * T
        up, down = pl.ds(r - 1, T), pl.ds(r + 1, T)
        lefts, rights = join_left(lefts), join_right(rights)
        return [
            (ref[j, up, :] + ref[j, down, :]) + (lefts[j] + rights[j]) for j in range(span)
        ]

    def turned(ref, k):
        values = [ref[j, chunk(k), :] for j in range(span)]
        return turn_left(values), turn_right(values)

    def pre_chunk(k, carry):
        at = chunk(k)
        ahead = (turned(g, k + 1), turned(gx, k + 1))
        g_near = around(g, k, *carry[0])
        near = around(gx, k, *carry[1])
        for j in range(span):
            depth = g[j, at, :]
            diag = DAMP + depth * g_near[j]
            inverse = 1.0 / diag
            r0[j, at, :] = r0[j, at, :] - diag * x[j, at, :] + depth * near[j]
            inv[j, at, :] = inverse
            gd[j, at, :] = depth * inverse
        return ahead

    def prepare_ocean():
        steps = 17 if ochunks % 17 == 0 else 2
        lax.fori_loop(0, ochunks, ocean_chunk, 0, unroll=steps)
        lax.fori_loop(0, ochunks, pre_chunk, (turned(g, 0), turned(gx, 0)), unroll=steps)

    def flow_wait(phase, part, piece):
        for target in range(groups):

            @pl.when(gi == target)
            def _():
                cap = (target + phase) % 2
                lo, hi, start = flow_parts(cap, target)[part]
                width = 2 * L if piece == 0 else cols - 2 * L
                ref = flow.at[:, cap, start : start + hi - lo, 0:width]
                take(ref, flow_recv.at[4 * cap + 2 * part + piece])

    def flow_chunks(phase, part):
        if phase == 0:
            return 0, ichunks
        return (0, above_split[1]) if part == 0 else (above_split[1], ichunks)

    def pack_flow(phase, part):
        c = lax.rem(gi + phase, 2)
        first, last = flow_chunks(phase, part)

        def fpack_chunk(k, _):
            after, before = packed(ends((flow.at[0, c], flow.at[1, c]), chunk(k)))
            fpack_s[0, c, chunk0(k), :] = after
            fpack_s[1, c, chunk0(k), :] = before
            return 0

        lax.fori_loop(first, last, fpack_chunk, 0, unroll=last - first)
        at = slice(first * T, last * T)
        fcols = col_copies(
            lambda way: fpack_s.at[way, c, at, :],
            lambda way: fpack_r.at[way, c, at, :],
            (2 if phase == 0 else 6) if part == 0 else 10,
        )
        start_all(fcols, ti, tiles)
        return fcols

    def add_flow(phase, part):
        c = lax.rem(gi + phase, 2)
        first, last = flow_chunks(phase, part)

        def flow_chunk(k, _):
            at = chunk(k)
            before, after = fpack_r[0, c, chunk0(k), :], fpack_r[1, c, chunk0(k), :]
            for comp in range(2):
                values = [flow[comp, c, at, pl.ds(j * L, L)] for j in range(own)]
                values.append(unpacked(before, after, comp))
                flow_edge[comp, c, at, :] = values[own]
                for j in range(span):
                    ww[comp, c, j, at, :] = ww[comp, c, j, at, :] + qq[c, j, at, :] * (
                        2.0 * DRAG * values[j]
                    )
            return 0

        lax.fori_loop(first, last, flow_chunk, 0, unroll=last - first)

    def subcycles(phase, part, first, last):
        c = lax.rem(gi + phase, 2)
        slot = 2 if part == 1 else c
        low, high = (0, ichunks) if phase == 0 else (above_split, below_split)[part]

        def subcycle(n, _):
            ahead, behind = 2, 2
            turned_u, turned_v, turned_m, turned_s = {}, {}, {}, {}

            def look(k):
                at = slice(T + T * k, TOP + T * k)
                turned_u[k] = turn_right([uu[slot, j, at, :] for j in range(span)])
                turned_v[k] = turn_right([vv[slot, j, at, :] for j in range(span)])

            def stress(k):
                at, down = slice(T + T * k, TOP + T * k), slice(T + T * k + 1, TOP + T * k + 1)
                beside_u, beside_v = join_right(turned_u.pop(k)), join_right(turned_v.pop(k))
                ms, ss = [], []
                for j in range(span):
                    u, v = uu[slot, j, at, :], vv[slot, j, at, :]
                    du = uu[slot, j, down, :] - u
                    dv = beside_v[j] - v
                    shear = (beside_u[j] - u) + (vv[slot, j, down, :] - v)
                    rate = kk[c, j, at, :] * lax.rsqrt(
                        (du * du + dv * dv) + (0.5 * (shear * shear) + 0.5)
                    )
                    sp_p[slot, j, at, :] = sp_p[slot, j, at, :] * KEEP + rate * du
                    m = sp_m[slot, j, at, :] * KEEP + rate * dv
                    s = sp_s[slot, j, at, :] * KEEP + rate * shear
                    sp_m[slot, j, at, :] = m
                    sp_s[slot, j, at, :] = s
                    ms.append(m)
                    ss.append(s)
                turned_m[k], turned_s[k] = turn_left(ms), turn_left(ss)

            def momentum(k):
                at, up = slice(T + T * k, TOP + T * k), slice(T + T * k - 1, TOP + T * k - 1)
                beside_m, beside_s = join_left(turned_m.pop(k)), join_left(turned_s.pop(k))
                for j in range(span):
                    s = sp_s[slot, j, at, :]
                    fx = (sp_p[slot, j, at, :] - sp_p[slot, j, up, :]) + (s - beside_s[j])
                    fy = (sp_m[slot, j, at, :] - beside_m[j]) + (s - sp_s[slot, j, up, :])
                    p, q = pp[c, j, at, :], qq[c, j, at, :]
                    uu[slot, j, at, :] = p * uu[slot, j, at, :] + (q * fx + ww[0, c, j, at, :])
                    vv[slot, j, at, :] = p * vv[slot, j, at, :] + (q * fy + ww[1, c, j, at, :])

            for k in range(low - ahead, high + behind):
                if k + ahead < high:
                    look(k + ahead)
                if low <= k < high:
                    stress(k)
                if low <= k - behind < high:
                    momentum(k - behind)
            return 0

        lax.fori_loop(first, last, subcycle, 0, unroll=2)

    def owned_rows(phase, part):
        if phase == 0:
            return 0, rows
        return (0, split) if part == 0 else (split, rows)

    def drag(phase, part):
        c = lax.rem(gi + phase, 2)
        slot = 2 if part == 1 else c
        home = c * (groups - 1)
        edge_lanes = L // (2 * (rows // T))
        first, last = (row // T for row in owned_rows(phase, part))

        def drag_values(k, comp, slot):
            at = pl.ds(TOP + k * T, T)
            values = [flow[comp, c, at, pl.ds(j * L, L)] for j in range(own)]
            values.append(flow_edge[comp, c, at, :])
            ref = (uu, vv)[comp]
            return [
                jnp.where(qq[c, j, at, :] > 0.0, DRAG * (ref[slot, j, at, :] - values[j]), 0.0)
                for j in range(span)
            ]

        zero = jnp.zeros((T, L), F32)
        upper, rims = [zero] * span if part == 0 else drag_values(first - 1, 0, c), zero
        for k in range(first, last):
            across, along = drag_values(k, 0, slot), drag_values(k, 1, slot)
            beside = left(along)
            value = [
                (across[j] - above(upper[j], across[j])) + (along[j] - beside[j])
                for j in range(span)
            ]
            for j in range(own):
                sp[c, j, k * T : k * T + T, :] = value[j]
            width = 2 * edge_lanes
            here = (lane >= width * k) & (lane < width * k + width)
            rims = jnp.where(here, pltpu.roll(value[own], (edge_lanes + width * k) % L, 1), rims)
            upper = across
        trim_s[slot, 0] = rims
        row = lax.broadcasted_iota(jnp.int32, (T, L), 0)
        final = zero
        for j in range(span):
            final = jnp.where(row == j, upper[j][T - 1 : T, :], final)
        trim_s[slot, 1] = final

        @pl.when(gi != home)
        def _():
            for copy in back_copies(phase, part, c, gi, home):
                copy.start()

        if phase == 1:
            for source, target, copy in edge_copies():
                if (source == 0) == (part == 0):
                    pl.when(gi == source)(copy.start)
            return

        @pl.when(gi == home)
        def _():
            row = pl.multiple_of(TOP + gi * rows, T)
            for j in range(own):

                def own_chunk(k, _):
                    forcing[j, pl.ds(pl.multiple_of(row + k * T, T), T), :] = sp[c, j, chunk0(k), :]
                    return 0

                lax.fori_loop(0, rows // T, own_chunk, 0, unroll=rows // T)
            trim_r[gi, 0] = trim_s[c]

    def output(phase, part):
        c = lax.rem(gi + phase, 2)
        slot = 2 if part == 1 else c
        first, last = (row // T for row in owned_rows(phase, part))

        def out_chunk(k, _):
            at = pl.ds(pl.multiple_of(TOP + k * T, T), T)
            to = chunk0(k)
            for j in range(own):
                here = pl.ds(j * L, L)
                vel_out[0, c, to, here] = uu[slot, j, at, :]
                vel_out[1, c, to, here] = vv[slot, j, at, :]
                p, m = sp_p[slot, j, at, :], sp_m[slot, j, at, :]
                stress_out[0, c, to, here] = 0.5 * (p + m) - STRENGTH * h[c, at, here]
                stress_out[1, c, to, here] = 0.5 * (p - m)
                stress_out[2, c, to, here] = 0.5 * sp_s[slot, j, at, :]
            return 0

        lax.fori_loop(first, last, out_chunk, 0, unroll=2)

    def back_copies(phase, part, c, source, target):
        first, last = owned_rows(phase, part)
        slot = 2 if part == 1 else c
        at = pl.ds(pl.multiple_of(TOP + source * rows + first, T), last - first)
        parts = (
            (sp.at[c, :, first:last, :], forcing.at[0:own, at, :]),
            (trim_s.at[slot], trim_r.at[source, part]),
        )
        return [
            pltpu.make_async_remote_copy(
                src_ref=src,
                dst_ref=dst,
                send_sem=back_send.at[phase + part],
                recv_sem=back_recv.at[source, part],
                device_id=(target, ti),
                device_id_type=MESH,
            )
            for src, dst in parts
        ]

    def back_bytes(phase, part):
        first, last = owned_rows(phase, part)
        return w0.at[0, 0 : own * (last - first) + 2 * T, :]

    def edge_copies():
        top, bottom = groups - 1, 0
        parts = (
            (0, top, 1, sp.at[0, :, rows - T : rows, :], forcing.at[0:own, TOP - T : TOP, :]),
            (0, top, 1, trim_s.at[2], trim_r.at[0, 0]),
            (1, bottom, groups - 2, sp.at[1, :, 0:T, :], forcing.at[0:own, oend : oend + T, :]),
            (1, bottom, groups - 2, trim_s.at[1], trim_r.at[0, 0]),
        )
        return [
            (
                source,
                target,
                pltpu.make_async_remote_copy(
                    src_ref=src,
                    dst_ref=dst,
                    send_sem=edge_send,
                    recv_sem=edge_recv,
                    device_id=(target, ti),
                    device_id_type=MESH,
                ),
            )
            for way, source, target, src, dst in parts
        ]

    edge_rows = own * T + 2 * T

    receive_rows(0, 8 * T)
    icols_a = pack(0)
    receive_rows(2, 3 * T)
    ocols = pack_ocean()
    flow_wait(0, 0, 0)
    fcols_a = pack_flow(0, 0)
    receive_all(icols_a, ti, tiles)
    prep(0)
    receive_all(ocols, ti, tiles)
    prepare_ocean()
    receive_rows(1, 8 * T)
    icols_b = pack(1)
    flow_wait(0, 0, 1)
    receive_all(fcols_a, ti, tiles)
    add_flow(0, 0)
    subcycles(0, 0, 0, NSUB // 2)
    flow_wait(1, 0, 0)
    fcols_b = pack_flow(1, 0)
    subcycles(0, 0, NSUB // 2, NSUB)
    drag(0, 0)
    output(0, 0)
    receive_all(icols_b, ti, tiles)
    prep(1)
    flow_wait(1, 0, 1)
    receive_all(fcols_b, ti, tiles)
    add_flow(1, 0)
    flow_wait(1, 1, 0)
    fcols_c = pack_flow(1, 1)
    subcycles(1, 0, 0, NSUB)
    drag(1, 0)
    flow_wait(1, 1, 1)
    receive_all(fcols_c, ti, tiles)
    add_flow(1, 1)
    subcycles(1, 1, 0, NSUB)
    drag(1, 1)
    output(1, 0)
    output(1, 1)

    def rim_of(source, part, k):
        lanes_each = L // (2 * (rows // T))
        turn = (lanes_each + 2 * lanes_each * k) % L
        value = pltpu.roll(trim_r[source, part, 0], (L - turn) % L, 1)
        return jnp.where((lane < lanes_each) | (lane >= L - lanes_each), value, 0.0)

    def carry_over(row, source, part):
        for j in range(span):
            at = (j, slice(row, row + 1), slice(None))
            forcing[at] = forcing[at] - trim_r[source, part, 1, j : j + 1, :]

    for cap, home in enumerate(homes):

        @pl.when(gi == home)
        def _():
            early = [k for k in range(groups) if (k + cap) % 2 == 0]
            late = [k for k in range(groups) if (k + cap) % 2 == 1]
            for phase, part, some in ((0, 0, early), (1, 0, late), (1, 1, late)):
                first, last = owned_rows(phase, part)
                for source in some:
                    if source != home:
                        take(back_bytes(phase, part), back_recv.at[source, part])
                for source in some:
                    for k in range(first // T, last // T):
                        row = TOP + source * rows + k * T
                        forcing[own, row : row + T, :] = rim_of(source, part, k)
            for source in range(groups):
                carry_over(TOP + (source + 1) * rows, source, int(source in late))

    @pl.when(gi == 1)
    def _():
        take(w0.at[0, 0:edge_rows, :], edge_recv)
        forcing[own, TOP - T : TOP, :] = rim_of(0, 0, rows // T - 1)
        carry_over(TOP, 0, 0)

    @pl.when(gi == groups - 2)
    def _():
        take(w0.at[0, 0:edge_rows, :], edge_recv)
        forcing[own, oend : oend + T, :] = rim_of(0, 0, 0)

    zero = jnp.zeros((T, L), F32)

    def fold(first, second):
        total = first[0] * second[0]
        for j in range(1, own):
            total = total + first[j] * second[j]
        return total

    def first_chunk(k):
        at = chunk(k)
        r, z = [], []
        for j in range(span):
            depth = g[j, at, :]
            r.append(r0[j, at, :] + jnp.where(depth > 0.0, forcing[j, at, :], 0.0))
            z.append(r[j] * inv[j, at, :])
            v0[j, at, :] = z[j]
            w0[j, at, :] = depth * z[j]
        return fold(r, z)

    first_chunk(0)
    first_chunk(ochunks - 1)
    m0 = lax.fori_loop(1, ochunks - 1, lambda k, s: s + first_chunk(k), zero, unroll=8)

    def power(w_from, v_to, w_to):
        def body(k, turns):
            at = chunk(k)
            near = around(w_from, k, *turns)
            w_here = [w_from[j, at, :] for j in range(own)]
            w_next = []
            for j in range(span):
                v = gd[j, at, :] * near[j]
                w = g[j, at, :] * v
                if j < own:
                    v_to[j, at, :] = v
                w_to[j, at, :] = w
                w_next.append(w)
            return fold(w_here, near), fold(w_next, near)

        body(0, turned(w_from, 0))
        body(ochunks - 1, turned(w_from, ochunks - 1))

        def step(k, carry):
            turns, after, s0, s1 = carry
            ahead = turned(w_from, k + 2)
            a, b = body(k, turns)
            return after, ahead, s0 + a, s1 + b

        carry = (turned(w_from, 1), turned(w_from, 2), zero, zero)
        _, _, s0, s1 = lax.fori_loop(1, ochunks - 1, step, carry, unroll=ochunks - 2)
        return s0, s1

    m1, m2 = power(w0, v1, w1)
    m3, m4 = power(w1, v2, w2)

    def last_step(k, carry):
        turns, after, s = carry
        ahead = turned(w2, k + 2)
        near = around(w2, k, *turns)
        return after, ahead, s + fold([w2[j, chunk(k), :] for j in range(own)], near)

    carry = (turned(w2, 1), turned(w2, 2), zero)
    _, _, m5 = lax.fori_loop(1, ochunks - 1, last_step, carry, unroll=ochunks - 2)

    row = lax.broadcasted_iota(jnp.int32, (T, L), 0)
    moments = zero
    for k, m in enumerate((m0, m1, m2, m3, m4, m5)):
        moments = jnp.where(row == k, jnp.sum(m, axis=0, keepdims=True), moments)

    lane_sums = jnp.sum(moments, axis=1, keepdims=True)
    diagonal = lanes(T, L) == row
    red_s[...] = jnp.sum(jnp.where(diagonal, lane_sums, 0.0), axis=0, keepdims=True)

    pl.semaphore_wait(ready, tiles - 1)
    count = groups * tiles
    for d in range(1, count):
        other = lax.rem(gi * tiles + ti + d, count)
        pltpu.make_async_remote_copy(
            src_ref=red_s,
            dst_ref=red_r.at[d],
            send_sem=red_send,
            recv_sem=red_recv,
            device_id=(lax.div(other, tiles), lax.rem(other, tiles)),
            device_id_type=MESH,
        ).start()
    take(red_r.at[1:count], red_recv)
    parts = [red_s[...]] + [red_r[d] for d in range(1, count)]
    while len(parts) > 1:
        parts = [sum(parts[i : i + 2]) for i in range(0, len(parts), 2)]
    moments = jnp.where(diagonal, parts[0], 0.0)
    total = jnp.sum(moments, axis=1, keepdims=True)
    nu = [total[k : k + 1, :] for k in range(6)]
    a = [nu[k] - nu[k + 1] for k in range(5)]

    tiny = 1e-12

    def safe(value, scale):
        ok = value > tiny * scale
        return jnp.where(ok, 1.0 / jnp.where(ok, value, 1.0), 0.0)

    i0 = safe(a[0], 0.0 * a[0])
    l10, l20 = a[1] * i0, a[2] * i0
    d1 = a[2] - l10 * a[1]
    i1 = safe(d1, a[2])
    e21 = a[3] - l20 * a[1]
    l21 = e21 * i1
    d2 = a[4] - l20 * a[2] - l21 * e21
    i2 = safe(d2, a[4])
    y0 = nu[0]
    y1 = nu[1] - l10 * y0
    y2 = nu[2] - l20 * y0 - l21 * y1
    c2 = y2 * i2
    c1 = y1 * i1 - l21 * c2
    c0 = y0 * i0 - l10 * c1 - l20 * c2

    def final_chunk(k, _):
        at = pl.ds(pl.multiple_of(TOP + k * T, T), T)
        for j in range(own):
            ssh_out[chunk0(k), pl.ds(j * L, L)] = x[j, at, :] + (
                c0 * v0[j, at, :] + (c1 * v1[j, at, :] + c2 * v2[j, at, :])
            )
        return 0

    lax.fori_loop(0, orows // T, final_chunk, 0, unroll=16)
    for way in range(2):
        pl.when(edge(way, gi, groups)[0])(
            lambda: take(gn.at[0 : 19 * T, :], row_send.at[way])
        )
        sent = 2 * (rows + 2 * T) + (orows + 2 * T) // 2
        pl.when(edge(way, ti, tiles)[0])(lambda: take(w0.at[0:2, 0:sent, :], col_send.at[way]))
    for cap, home in enumerate(homes):

        @pl.when(gi == home)
        def _():
            spans = [flow_span(k) for k in range(groups) if k != home]
            take(cur_in.at[:, 0 : sum(hi - lo for lo, hi, _ in spans), :], flow_send)

    for phase, part in ((0, 0), (1, 0), (1, 1)):
        pl.when(gi != lax.rem(gi + phase, 2) * (groups - 1))(
            lambda: take(back_bytes(phase, part), back_send.at[phase + part])
        )
    pl.when((gi == 0) | (gi == groups - 1))(lambda: take(w0.at[0, 0:edge_rows, :], edge_send))
    take(red_r.at[1:count], red_send)


def deliver(*refs):
    sems = refs[-1]
    half = len(refs) // 2
    copies = [
        pltpu.make_async_copy(src, dst, sems.at[k])
        for k, (src, dst) in enumerate(zip(refs[:half], refs[half:-1]))
    ]
    for copy in copies:
        copy.start()
    for copy in copies:
        copy.wait()


def step(groups, tiles, *args):
    base_rhs, thick, ice_vel, ice_stress = args[0], args[5], args[7], args[8]
    orows, cols = base_rhs.shape
    rows = thick.shape[1]
    irows = rows + 2 * TOP
    erows = orows + 2 * TOP
    span = cols // L + 1
    hbm = pl.BlockSpec(memory_space=pltpu.HBM)
    vmem = pl.BlockSpec(memory_space=pltpu.VMEM)
    dma = pltpu.SemaphoreType.DMA
    ice = pltpu.VMEM((4, span, irows + 16, L), F32)
    ocean = pltpu.VMEM((span, erows + PAD, L), F32)
    plain = pltpu.VMEM((erows, cols), F32)
    results = pl.pallas_call(
        functools.partial(kernel, groups, tiles),
        out_shape=(
            pltpu.VMEM(base_rhs.shape, F32),
            pltpu.VMEM(ice_vel.shape, F32),
            pltpu.VMEM(ice_stress.shape, F32),
        ),
        in_specs=[hbm] * 10,
        out_specs=(vmem,) * 3,
        scratch_shapes=[
            pltpu.VMEM(args[4].shape, jnp.int32),
            pltpu.VMEM(args[6].shape, jnp.int32),
            pltpu.VMEM((2, 2, irows, cols), F32),
            pltpu.VMEM((3, 2, irows, cols), F32),
            pltpu.VMEM((2, 2, irows, cols), F32),
            pltpu.VMEM((2, 2, irows, cols), F32),
            pltpu.VMEM((2, irows, cols), F32),
            plain,
            plain,
            plain,
        ]
        + [pltpu.VMEM((4, span, irows + 16, L), F32)] * 5
        + [ice] * 3
        + [
            pltpu.VMEM((2, 4, span, irows + 16, L), F32),
            pltpu.VMEM((2, 2, irows, L), F32),
        ]
        + [ocean] * 13
        + [
            pltpu.VMEM((orows // BS, cols), F32),
            pltpu.VMEM((2, rows // BS, cols), F32),
            pltpu.VMEM((2, 2, rows + 2 * T, L), F32),
            pltpu.VMEM((2, 2, rows + 2 * T, L), F32),
            pltpu.VMEM((2, 2, rows + 2 * T, L), F32),
            pltpu.VMEM((2, 2, rows + 2 * T, L), F32),
            pltpu.VMEM((2, orows + 2 * T, L), F32),
            pltpu.VMEM((2, orows + 2 * T, L), F32),
            pltpu.VMEM((2, span - 1, rows, L), F32),
            pltpu.VMEM((3, 2, T, L), F32),
            pltpu.VMEM((groups, 2, 2, T, L), F32),
            pltpu.VMEM((1, L), F32),
            pltpu.VMEM((groups * tiles, 1, L), F32),
            dma((9,)),
            dma,
            dma((8,)),
            dma((2,)),
            dma((6,)),
            dma((2,)),
            dma((12,)),
            dma((3,)),
            dma((groups, 2)),
            dma,
            dma,
            dma,
            dma,
            pltpu.SemaphoreType.REGULAR,
        ],
        compiler_params=pltpu.CompilerParams(
            collective_id=0, has_side_effects=True, vmem_limit_bytes=48 * 2**20
        ),
    )(*(pltpu.with_memory_space_constraint(a, pltpu.HBM) for a in args))
    return pl.pallas_call(
        deliver,
        out_shape=tuple(jax.ShapeDtypeStruct(r.shape, F32) for r in results),
        in_specs=[vmem] * 3,
        out_specs=(hbm,) * 3,
        scratch_shapes=[dma((3,))],
        compiler_params=pltpu.CompilerParams(vmem_limit_bytes=4 * 2**20),
    )(*results)


def solution(mesh):
    grid = P("grp", "tile")
    plane = P(None, "grp", "tile")
    stack = P(None, None, "grp", "tile")
    return jax.shard_map(
        functools.partial(step, mesh.shape["grp"], mesh.shape["tile"]),
        mesh=mesh,
        in_specs=(grid, grid, grid, plane, grid, plane, plane, stack, stack, stack),
        out_specs=(grid, stack, stack),
        check_vma=False,
    )
```

```python
import functools
import math

import jax
import jax.numpy as jnp
from jax import lax
from jax.experimental import pallas as pl
from jax.experimental.pallas import tpu as pltpu
from jax.sharding import PartitionSpec as P

BS = 8
NSUB = 8

DAMP = 0.05
RELAX = 0.2
STRENGTH = 0.5
DRAG = 1.0
STEP = 0.5
KEEP = 1.0 / (1.0 + RELAX)
RATE = math.sqrt(2.0) * RELAX * STRENGTH / (1.0 + RELAX)

MESH = pl.DeviceIdType.MESH
F32 = jnp.float32
T = 8
L = 128
W = 12
TOP = 2 * T
PAD = 2 * T


def lanes(rows, width):
    return lax.broadcasted_iota(jnp.int32, (rows, width), 1)


def above(prev, here):
    row = lax.broadcasted_iota(jnp.int32, here.shape, 0)
    return pltpu.roll(jnp.where(row == T - 1, prev, here), 1, 0)


def turn_right(tiles):
    return [pltpu.roll(x, L - 1, 1) for x in tiles]


def turn_left(tiles):
    return [pltpu.roll(x, 1, 1) for x in tiles]


def join_right(turned):
    lane = lanes(T, L)
    n = len(turned)
    return [jnp.where(lane == L - 1, turned[(j + 1) % n], turned[j]) for j in range(n)]


def join_left(turned):
    lane = lanes(T, L)
    n = len(turned)
    return [jnp.where(lane == 0, turned[(j - 1) % n], turned[j]) for j in range(n)]


def right(tiles):
    return join_right(turn_right(tiles))


def left(tiles):
    return join_left(turn_left(tiles))


def kernel(
    groups,
    tiles,
    base_in,
    depth_in,
    ssh_in,
    cur_in,
    land_in,
    thick_in,
    ice_in,
    vel_in,
    stress_in,
    wind_in,
    ssh_out,
    vel_out,
    stress_out,
    land_ref,
    ice_ref,
    vel,
    st,
    wind,
    flow,
    h,
    gn,
    xn,
    bn,
    uu,
    vv,
    sp_p,
    sp_m,
    sp_s,
    kk,
    pp,
    qq,
    ww,
    flow_edge,
    g,
    gx,
    r0,
    x,
    inv,
    gd,
    forcing,
    v0,
    v1,
    v2,
    w0,
    w1,
    w2,
    wet,
    cover,
    pack_s,
    pack_r,
    fpack_s,
    fpack_r,
    opack_s,
    opack_r,
    sp,
    trim_s,
    trim_r,
    red_s,
    red_r,
    load_sem,
    flow_send,
    flow_recv,
    row_send,
    row_recv,
    col_send,
    col_recv,
    back_send,
    back_recv,
    edge_send,
    edge_recv,
    red_send,
    red_recv,
    ready,
):
    gi = lax.axis_index("grp")
    ti = lax.axis_index("tile")
    rows, cols = thick_in.shape[1], thick_in.shape[2]
    orows = base_in.shape[0]
    end = TOP + rows
    oend = TOP + orows
    own = cols // L
    span = own + 1
    ichunks = rows // T + 2
    ochunks = orows // T + 2
    split = rows - 3 * T
    above_split, below_split = (0, split // T + 2), (split // T, ichunks)

    barrier = pltpu.get_barrier_semaphore()
    for d in range(1, groups):
        pl.semaphore_signal(
            barrier, inc=1, device_id=(lax.rem(gi + d, groups), ti), device_id_type=MESH
        )
    for d in range(1, tiles):
        pl.semaphore_signal(
            barrier, inc=1, device_id=(gi, lax.rem(ti + d, tiles)), device_id_type=MESH
        )

    loads = []

    def load(src, dst):
        copy = pltpu.make_async_copy(src, dst, load_sem.at[len(loads)])
        copy.start()
        loads.append(copy)
        return copy

    load_land = load(land_in, land_ref)
    load_ice = load(ice_in, ice_ref)
    load_thick = load(thick_in, h.at[:, TOP:end, :])
    load_vel = load(vel_in, vel.at[:, :, TOP:end, :])
    load_st = load(stress_in, st.at[:, :, TOP:end, :])
    load_wind = load(wind_in, wind.at[:, :, TOP:end, :])
    load_depth = load(depth_in, gn.at[TOP:oend, :])
    load_x = load(ssh_in, xn.at[TOP:oend, :])
    load_b = load(base_in, bn.at[TOP:oend, :])

    def clear(ref, *spans):
        for lo, hi in spans:
            ref[..., lo:hi, :] = jnp.zeros(ref.shape[:-2] + (hi - lo, ref.shape[-1]), F32)

    for outer, before in ((gi == 0, True), (gi == groups - 1, False)):

        @pl.when(outer)
        def _():
            for ref in (vel, st, wind, flow, h):
                clear(ref, (T, TOP) if before else (end, end + T))
            for ref in (gn, xn, bn):
                clear(ref, (T, TOP) if before else (oend, oend + T))
            clear(forcing, (T, TOP), (oend, oend + T))

    for outer, way in ((ti == 0, 0), (ti == tiles - 1, 1)):

        @pl.when(outer)
        def _():
            for ref in (pack_r, fpack_r, opack_r):
                ref[way] = jnp.zeros(ref.shape[1:], F32)

    @pl.when((gi > 0) & (gi < groups - 1))
    def _():
        clear(forcing, (TOP, oend))
        pl.when(gi != 1)(lambda: clear(forcing, (T, TOP)))
        pl.when(gi != groups - 2)(lambda: clear(forcing, (oend, oend + T)))

    for ref in (uu, vv, sp_p, sp_m, sp_s):
        clear(ref, (0, T), (end + T, end + 2 * T))
    for ref in (g, gx, w0, w1, w2):
        clear(ref, (0, T), (oend + T, oend + 2 * T))

    def blocks(ref, out, count):
        width = ref.shape[-1]
        row = lax.broadcasted_iota(jnp.int32, (width, cols), 0)
        spread = (row == lax.shift_right_logical(lanes(width, cols), 3)).astype(F32)
        values = ref[...].reshape((count, width)).astype(F32)
        out[...] = jnp.dot(values, spread, preferred_element_type=F32)

    pl.semaphore_wait(barrier, groups + tiles - 2)
    for d in range(1, tiles):
        pl.semaphore_signal(
            ready, inc=1, device_id=(gi, lax.rem(ti + d, tiles)), device_id_type=MESH
        )

    homes = (0, groups - 1)
    pieces = ((0, L), (cols - L, cols), (L, cols - L))

    def flow_span(target):
        lo = max(0, rows * target - T)
        hi = min(rows * groups, rows * target + rows + T)
        return lo, hi, TOP + lo - rows * target

    def flow_parts(cap, target):
        lo, hi, start = flow_span(target)
        if (cap + target) % 2 == 0:
            return ((lo, hi, start),)
        middle = TOP + split + T
        return ((lo, lo + middle - start, start), (lo + middle - start, hi, middle))

    def flow_copies(cap, target):
        out = []
        for part, (lo, hi, start) in enumerate(flow_parts(cap, target)):
            for piece, (first, last) in enumerate(pieces):
                src = cur_in.at[:, lo:hi, first:last]
                dst = flow.at[:, cap, start : start + hi - lo, first:last]
                recv = flow_recv.at[4 * cap + 2 * part + piece // 2]
                if target == homes[cap]:
                    out.append(pltpu.make_async_copy(src, dst, recv))
                else:
                    out.append(
                        pltpu.make_async_remote_copy(
                            src_ref=src,
                            dst_ref=dst,
                            send_sem=flow_send,
                            recv_sem=recv,
                            device_id=(target, ti),
                            device_id_type=MESH,
                        )
                    )
        return out

    def take(ref, sem):
        pltpu.make_async_copy(ref, ref, sem).wait()

    def row_copy(k, way, src, dst, first, after, ends):
        count, last = ends
        from_row = first + count - T if way == 0 else first
        to_row = after - T if way == 0 else last
        return (
            way,
            pltpu.make_async_remote_copy(
                src_ref=src(pl.ds(from_row, T)),
                dst_ref=dst(pl.ds(to_row, T)),
                send_sem=row_send.at[way],
                recv_sem=row_recv.at[2 * k + way],
                device_id=(lax.rem(gi + (1 if way == 0 else groups - 1), groups), ti),
                device_id_type=MESH,
            ),
        )

    def ice_rows(stage):
        c = lax.rem(gi + 1 + stage, 2)
        out = []
        for ref in (vel, st, wind):
            for way in range(2):
                out.append(
                    row_copy(
                        stage,
                        way,
                        lambda at, ref=ref: ref.at[:, c, at, :],
                        lambda at, ref=ref: ref.at[:, c, at, :],
                        TOP,
                        TOP,
                        (rows, end),
                    )
                )
        return out

    def thick_rows(stage):
        c = lax.rem(gi + 1 + stage, 2)
        return [
            row_copy(
                stage,
                way,
                lambda at: h.at[c, at, :],
                lambda at: h.at[c, at, :],
                TOP,
                TOP,
                (rows, end),
            )
            for way in range(2)
        ]

    def ocean_rows():
        return [
            row_copy(
                2,
                way,
                lambda at, ref=ref: ref.at[at, :],
                lambda at, ref=ref: ref.at[at, :],
                TOP,
                TOP,
                (orows, oend),
            )
            for ref in (xn, bn, gn)
            for way in range(2)
        ]

    def edge(way, index, count):
        sends = index < count - 1 if way == 0 else index > 0
        receives = index > 0 if way == 0 else index < count - 1
        return sends, receives

    def start_all(copies, index, count):
        for way, copy in copies:
            pl.when(edge(way, index, count)[0])(copy.start)

    def receive_all(copies, index, count):
        for way, copy in copies:
            pl.when(edge(way, index, count)[1])(copy.wait_recv)

    def receive_rows(k, count):
        for way in range(2):
            pl.when(edge(way, gi, groups)[1])(
                lambda: take(gn.at[0:count, :], row_recv.at[2 * k + way])
            )

    for cap, home in enumerate(homes):

        @pl.when(gi == home)
        def _():
            for copy in flow_copies(cap, home):
                copy.start()

    load_vel.wait()
    load_st.wait()
    load_wind.wait()
    start_all(ice_rows(0), gi, groups)
    load_land.wait()
    load_ice.wait()
    blocks(land_ref, wet, land_ref.shape[0])
    for c in range(2):
        row = lax.broadcasted_iota(jnp.int32, (cols // BS, cols), 0)
        spread = (row == lax.shift_right_logical(lanes(cols // BS, cols), 3)).astype(F32)
        cover[c] = jnp.dot(ice_ref[c].astype(F32), spread, preferred_element_type=F32)
    load_thick.wait()

    def cover_chunk(k, _):
        for c in range(2):
            at = (c, pl.ds(pl.multiple_of(TOP + k * T, T), T), slice(None))
            h[at] = h[at] * cover[c, pl.ds(k, 1), :]
        return 0

    lax.fori_loop(0, rows // T, cover_chunk, 0, unroll=4)
    start_all(thick_rows(0), gi, groups)
    load_depth.wait()

    def wet_chunk(k, _):
        at = (pl.ds(pl.multiple_of(TOP + k * T, T), T), slice(None))
        gn[at] = gn[at] * wet[pl.ds(k, 1), :]
        return 0

    lax.fori_loop(0, orows // T, wet_chunk, 0, unroll=4)
    load_x.wait()
    load_b.wait()
    start_all(ocean_rows(), gi, groups)

    def send_flow(which):
        for cap, home in enumerate(homes):

            @pl.when(gi == home)
            def _():
                order = sorted((k for k in range(groups) if k != home), key=lambda k: abs(k - home))
                for target in which(order):
                    for copy in flow_copies(cap, target):
                        copy.start()

    send_flow(lambda order: order[1:])
    start_all(ice_rows(1), gi, groups)
    start_all(thick_rows(1), gi, groups)
    send_flow(lambda order: order[:1])

    lane = lanes(T, L)

    def col_copies(src, dst, base):
        out = []
        for way in range(2):
            out.append(
                (
                    way,
                    pltpu.make_async_remote_copy(
                        src_ref=src(way),
                        dst_ref=dst(way),
                        send_sem=col_send.at[way],
                        recv_sem=col_recv.at[base + way],
                        device_id=(gi, lax.rem(ti + (1 if way == 0 else tiles - 1), tiles)),
                        device_id_type=MESH,
                    ),
                )
            )
        return out

    def packed(values):
        after = jnp.zeros((T, L), F32)
        before = jnp.zeros((T, L), F32)
        for f, (first, last) in enumerate(values):
            here = (lane >= W * f) & (lane < W * f + W)
            after = jnp.where(here, pltpu.roll(last, (W * f + W) % L, 1), after)
            before = jnp.where(here, pltpu.roll(first, W * f, 1) if f else first, before)
        return after, before

    def unpacked(from_before, from_after, f):
        low = pltpu.roll(from_before, (L - W - W * f) % L, 1)
        high = pltpu.roll(from_after, (L - W * f) % L, 1) if f else from_after
        return jnp.where(lane < W, high, jnp.where(lane >= L - W, low, 0.0))

    def ends(refs, at):
        return [(ref[at, pl.ds(0, L)], ref[at, pl.ds(cols - L, L)]) for ref in refs]

    def ice_fields(c):
        return (
            vel.at[0, c],
            vel.at[1, c],
            st.at[0, c],
            st.at[1, c],
            st.at[2, c],
            h.at[c],
            wind.at[0, c],
            wind.at[1, c],
        )

    def chunk(k):
        return pl.ds(pl.multiple_of(T + k * T, T), T)

    def chunk0(k):
        return pl.ds(pl.multiple_of(k * T, T), T)

    def pack(stage):
        c = lax.rem(gi + stage, 2)

        def body(k, _):
            after, before = packed(ends(ice_fields(c), chunk(k)))
            pack_s[0, c, chunk0(k), :] = after
            pack_s[1, c, chunk0(k), :] = before
            return 0

        lax.fori_loop(0, ichunks, body, 0, unroll=ichunks)
        icols = col_copies(lambda way: pack_s.at[way, c], lambda way: pack_r.at[way, c], 4 * stage)
        start_all(icols, ti, tiles)
        return icols

    def pack_ocean():
        def body(k, _):
            after, before = packed(ends((gn, xn, bn), chunk(k)))
            opack_s[0, chunk0(k), :] = after
            opack_s[1, chunk0(k), :] = before
            return 0

        lax.fori_loop(0, ochunks, body, 0, unroll=17 if ochunks % 17 == 0 else 1)
        ocols = col_copies(lambda way: opack_s.at[way], lambda way: opack_r.at[way], 8)
        start_all(ocols, ti, tiles)
        return ocols

    def prep(phase):
        c = lax.rem(gi + phase, 2)

        def body(k, thick_up):
            at = chunk(k)
            fields = ice_fields(c)
            values = [[ref[at, pl.ds(j * L, L)] for ref in fields] for j in range(own)]
            before, after = pack_r[0, c, chunk0(k), :], pack_r[1, c, chunk0(k), :]
            values.append([unpacked(before, after, f) for f in range(len(fields))])
            thicks = [v[5] for v in values]
            beside = left(thicks)
            for j, (u, v, s0, s1, s2, thick, wx, wy) in enumerate(values):
                mass = thick + 1.0
                inverse = jnp.where(thick > 0.0, 1.0 / (mass + STEP * DRAG), 0.0)
                q = STEP * inverse
                half = 0.5 * q
                for slot in (c,) if phase == 0 else (c, 2):
                    uu[slot, j, at, :] = u
                    vv[slot, j, at, :] = v
                    sp_p[slot, j, at, :] = (s0 + s1) + STRENGTH * thick
                    sp_m[slot, j, at, :] = (s0 - s1) + STRENGTH * thick
                    sp_s[slot, j, at, :] = s2 + s2
                kk[c, j, at, :] = RATE * thick
                pp[c, j, at, :] = mass * inverse
                qq[c, j, at, :] = half
                slope = STRENGTH * half
                ww[0, c, j, at, :] = q * wx - slope * (thick - above(thick_up[j], thick))
                ww[1, c, j, at, :] = q * wy - slope * (thick - beside[j])
            return tuple(thicks)

        zero = jnp.zeros((T, L), F32)
        lax.fori_loop(0, ichunks, body, (zero,) * span, unroll=ichunks // 2)

    def ocean_chunk(k, _):
        at = chunk(k)
        before, after = opack_r[0, chunk0(k), :], opack_r[1, chunk0(k), :]
        values = [[ref[at, pl.ds(j * L, L)] for ref in (gn, xn, bn)] for j in range(own)]
        values.append([unpacked(before, after, f) for f in range(3)])
        for j, (depth, height, base) in enumerate(values):
            g[j, at, :] = depth
            gx[j, at, :] = depth * height
            x[j, at, :] = height
            r0[j, at, :] = jnp.where(depth > 0.0, base, 0.0)
        return 0

    def around(ref, k, lefts, rights):
        r = T + k * T
        up, down = pl.ds(r - 1, T), pl.ds(r + 1, T)
        lefts, rights = join_left(lefts), join_right(rights)
        return [
            (ref[j, up, :] + ref[j, down, :]) + (lefts[j] + rights[j]) for j in range(span)
        ]

    def turned(ref, k):
        values = [ref[j, chunk(k), :] for j in range(span)]
        return turn_left(values), turn_right(values)

    def pre_chunk(k, carry):
        at = chunk(k)
        ahead = (turned(g, k + 1), turned(gx, k + 1))
        g_near = around(g, k, *carry[0])
        near = around(gx, k, *carry[1])
        for j in range(span):
            depth = g[j, at, :]
            diag = DAMP + depth * g_near[j]
            inverse = 1.0 / diag
            r0[j, at, :] = r0[j, at, :] - diag * x[j, at, :] + depth * near[j]
            inv[j, at, :] = inverse
            gd[j, at, :] = depth * inverse
        return ahead

    def prepare_ocean():
        steps = 17 if ochunks % 17 == 0 else 2
        lax.fori_loop(0, ochunks, ocean_chunk, 0, unroll=steps)
        lax.fori_loop(0, ochunks, pre_chunk, (turned(g, 0), turned(gx, 0)), unroll=steps)

    def flow_wait(phase, part, piece):
        for target in range(groups):

            @pl.when(gi == target)
            def _():
                cap = (target + phase) % 2
                lo, hi, start = flow_parts(cap, target)[part]
                width = 2 * L if piece == 0 else cols - 2 * L
                ref = flow.at[:, cap, start : start + hi - lo, 0:width]
                take(ref, flow_recv.at[4 * cap + 2 * part + piece])

    def flow_chunks(phase, part):
        if phase == 0:
            return 0, ichunks
        return (0, above_split[1]) if part == 0 else (above_split[1], ichunks)

    def pack_flow(phase, part):
        c = lax.rem(gi + phase, 2)
        first, last = flow_chunks(phase, part)

        def fpack_chunk(k, _):
            after, before = packed(ends((flow.at[0, c], flow.at[1, c]), chunk(k)))
            fpack_s[0, c, chunk0(k), :] = after
            fpack_s[1, c, chunk0(k), :] = before
            return 0

        lax.fori_loop(first, last, fpack_chunk, 0, unroll=last - first)
        at = slice(first * T, last * T)
        fcols = col_copies(
            lambda way: fpack_s.at[way, c, at, :],
            lambda way: fpack_r.at[way, c, at, :],
            (2 if phase == 0 else 6) if part == 0 else 10,
        )
        start_all(fcols, ti, tiles)
        return fcols

    def add_flow(phase, part):
        c = lax.rem(gi + phase, 2)
        first, last = flow_chunks(phase, part)

        def flow_chunk(k, _):
            at = chunk(k)
            before, after = fpack_r[0, c, chunk0(k), :], fpack_r[1, c, chunk0(k), :]
            for comp in range(2):
                values = [flow[comp, c, at, pl.ds(j * L, L)] for j in range(own)]
                values.append(unpacked(before, after, comp))
                flow_edge[comp, c, at, :] = values[own]
                for j in range(span):
                    ww[comp, c, j, at, :] = ww[comp, c, j, at, :] + qq[c, j, at, :] * (
                        2.0 * DRAG * values[j]
                    )
            return 0

        lax.fori_loop(first, last, flow_chunk, 0, unroll=last - first)

    def subcycles(phase, part, first, last):
        c = lax.rem(gi + phase, 2)
        slot = 2 if part == 1 else c
        low, high = (0, ichunks) if phase == 0 else (above_split, below_split)[part]

        def subcycle(n, _):
            ahead, behind = 2, 2
            turned_u, turned_v, turned_m, turned_s = {}, {}, {}, {}

            def look(k):
                at = slice(T + T * k, TOP + T * k)
                turned_u[k] = turn_right([uu[slot, j, at, :] for j in range(span)])
                turned_v[k] = turn_right([vv[slot, j, at, :] for j in range(span)])

            def stress(k):
                at, down = slice(T + T * k, TOP + T * k), slice(T + T * k + 1, TOP + T * k + 1)
                beside_u, beside_v = join_right(turned_u.pop(k)), join_right(turned_v.pop(k))
                ms, ss = [], []
                for j in range(span):
                    u, v = uu[slot, j, at, :], vv[slot, j, at, :]
                    du = uu[slot, j, down, :] - u
                    dv = beside_v[j] - v
                    shear = (beside_u[j] - u) + (vv[slot, j, down, :] - v)
                    rate = kk[c, j, at, :] * lax.rsqrt(
                        (du * du + dv * dv) + (0.5 * (shear * shear) + 0.5)
                    )
                    sp_p[slot, j, at, :] = sp_p[slot, j, at, :] * KEEP + rate * du
                    m = sp_m[slot, j, at, :] * KEEP + rate * dv
                    s = sp_s[slot, j, at, :] * KEEP + rate * shear
                    sp_m[slot, j, at, :] = m
                    sp_s[slot, j, at, :] = s
                    ms.append(m)
                    ss.append(s)
                turned_m[k], turned_s[k] = turn_left(ms), turn_left(ss)

            def momentum(k):
                at, up = slice(T + T * k, TOP + T * k), slice(T + T * k - 1, TOP + T * k - 1)
                beside_m, beside_s = join_left(turned_m.pop(k)), join_left(turned_s.pop(k))
                for j in range(span):
                    s = sp_s[slot, j, at, :]
                    fx = (sp_p[slot, j, at, :] - sp_p[slot, j, up, :]) + (s - beside_s[j])
                    fy = (sp_m[slot, j, at, :] - beside_m[j]) + (s - sp_s[slot, j, up, :])
                    p, q = pp[c, j, at, :], qq[c, j, at, :]
                    uu[slot, j, at, :] = p * uu[slot, j, at, :] + (q * fx + ww[0, c, j, at, :])
                    vv[slot, j, at, :] = p * vv[slot, j, at, :] + (q * fy + ww[1, c, j, at, :])

            for k in range(low - ahead, high + behind):
                if k + ahead < high:
                    look(k + ahead)
                if low <= k < high:
                    stress(k)
                if low <= k - behind < high:
                    momentum(k - behind)
            return 0

        lax.fori_loop(first, last, subcycle, 0, unroll=4)

    def owned_rows(phase, part):
        if phase == 0:
            return 0, rows
        return (0, split) if part == 0 else (split, rows)

    def drag(phase, part):
        c = lax.rem(gi + phase, 2)
        slot = 2 if part == 1 else c
        home = c * (groups - 1)
        edge_lanes = L // (2 * (rows // T))
        first, last = (row // T for row in owned_rows(phase, part))

        def drag_values(k, comp, slot):
            at = pl.ds(TOP + k * T, T)
            values = [flow[comp, c, at, pl.ds(j * L, L)] for j in range(own)]
            values.append(flow_edge[comp, c, at, :])
            ref = (uu, vv)[comp]
            return [
                jnp.where(qq[c, j, at, :] > 0.0, DRAG * (ref[slot, j, at, :] - values[j]), 0.0)
                for j in range(span)
            ]

        zero = jnp.zeros((T, L), F32)
        upper, rims = [zero] * span if part == 0 else drag_values(first - 1, 0, c), zero
        for k in range(first, last):
            across, along = drag_values(k, 0, slot), drag_values(k, 1, slot)
            beside = left(along)
            value = [
                (across[j] - above(upper[j], across[j])) + (along[j] - beside[j])
                for j in range(span)
            ]
            for j in range(own):
                sp[c, j, k * T : k * T + T, :] = value[j]
            width = 2 * edge_lanes
            here = (lane >= width * k) & (lane < width * k + width)
            rims = jnp.where(here, pltpu.roll(value[own], (edge_lanes + width * k) % L, 1), rims)
            upper = across
        trim_s[slot, 0] = rims
        row = lax.broadcasted_iota(jnp.int32, (T, L), 0)
        final = zero
        for j in range(span):
            final = jnp.where(row == j, upper[j][T - 1 : T, :], final)
        trim_s[slot, 1] = final

        @pl.when(gi != home)
        def _():
            for copy in back_copies(phase, part, c, gi, home):
                copy.start()

        if phase == 1:
            for source, target, copy in edge_copies():
                if (source == 0) == (part == 0):
                    pl.when(gi == source)(copy.start)
            return

        @pl.when(gi == home)
        def _():
            row = pl.multiple_of(TOP + gi * rows, T)
            for j in range(own):

                def own_chunk(k, _):
                    forcing[j, pl.ds(pl.multiple_of(row + k * T, T), T), :] = sp[c, j, chunk0(k), :]
                    return 0

                lax.fori_loop(0, rows // T, own_chunk, 0, unroll=rows // T)
            trim_r[gi, 0] = trim_s[c]

    def output(phase, part):
        c = lax.rem(gi + phase, 2)
        slot = 2 if part == 1 else c
        first, last = (row // T for row in owned_rows(phase, part))

        def out_chunk(k, _):
            at = pl.ds(pl.multiple_of(TOP + k * T, T), T)
            to = chunk0(k)
            for j in range(own):
                here = pl.ds(j * L, L)
                vel_out[0, c, to, here] = uu[slot, j, at, :]
                vel_out[1, c, to, here] = vv[slot, j, at, :]
                p, m = sp_p[slot, j, at, :], sp_m[slot, j, at, :]
                stress_out[0, c, to, here] = 0.5 * (p + m) - STRENGTH * h[c, at, here]
                stress_out[1, c, to, here] = 0.5 * (p - m)
                stress_out[2, c, to, here] = 0.5 * sp_s[slot, j, at, :]
            return 0

        lax.fori_loop(first, last, out_chunk, 0, unroll=2)

    def back_copies(phase, part, c, source, target):
        first, last = owned_rows(phase, part)
        slot = 2 if part == 1 else c
        at = pl.ds(pl.multiple_of(TOP + source * rows + first, T), last - first)
        parts = (
            (sp.at[c, :, first:last, :], forcing.at[0:own, at, :]),
            (trim_s.at[slot], trim_r.at[source, part]),
        )
        return [
            pltpu.make_async_remote_copy(
                src_ref=src,
                dst_ref=dst,
                send_sem=back_send.at[phase + part],
                recv_sem=back_recv.at[source, part],
                device_id=(target, ti),
                device_id_type=MESH,
            )
            for src, dst in parts
        ]

    def back_bytes(phase, part):
        first, last = owned_rows(phase, part)
        return w0.at[0, 0 : own * (last - first) + 2 * T, :]

    def edge_copies():
        top, bottom = groups - 1, 0
        parts = (
            (0, top, 1, sp.at[0, :, rows - T : rows, :], forcing.at[0:own, TOP - T : TOP, :]),
            (0, top, 1, trim_s.at[2], trim_r.at[0, 0]),
            (1, bottom, groups - 2, sp.at[1, :, 0:T, :], forcing.at[0:own, oend : oend + T, :]),
            (1, bottom, groups - 2, trim_s.at[1], trim_r.at[0, 0]),
        )
        return [
            (
                source,
                target,
                pltpu.make_async_remote_copy(
                    src_ref=src,
                    dst_ref=dst,
                    send_sem=edge_send,
                    recv_sem=edge_recv,
                    device_id=(target, ti),
                    device_id_type=MESH,
                ),
            )
            for way, source, target, src, dst in parts
        ]

    edge_rows = own * T + 2 * T

    receive_rows(0, 8 * T)
    icols_a = pack(0)
    receive_rows(2, 3 * T)
    ocols = pack_ocean()
    flow_wait(0, 0, 0)
    fcols_a = pack_flow(0, 0)
    receive_all(icols_a, ti, tiles)
    prep(0)
    receive_all(ocols, ti, tiles)
    prepare_ocean()
    receive_rows(1, 8 * T)
    icols_b = pack(1)
    flow_wait(0, 0, 1)
    receive_all(fcols_a, ti, tiles)
    add_flow(0, 0)
    subcycles(0, 0, 0, NSUB // 2)
    flow_wait(1, 0, 0)
    fcols_b = pack_flow(1, 0)
    subcycles(0, 0, NSUB // 2, NSUB)
    drag(0, 0)
    output(0, 0)
    receive_all(icols_b, ti, tiles)
    prep(1)
    flow_wait(1, 0, 1)
    receive_all(fcols_b, ti, tiles)
    add_flow(1, 0)
    flow_wait(1, 1, 0)
    fcols_c = pack_flow(1, 1)
    subcycles(1, 0, 0, NSUB)
    drag(1, 0)
    flow_wait(1, 1, 1)
    receive_all(fcols_c, ti, tiles)
    add_flow(1, 1)
    subcycles(1, 1, 0, NSUB)
    drag(1, 1)
    output(1, 0)
    output(1, 1)

    def rim_of(source, part, k):
        lanes_each = L // (2 * (rows // T))
        turn = (lanes_each + 2 * lanes_each * k) % L
        value = pltpu.roll(trim_r[source, part, 0], (L - turn) % L, 1)
        return jnp.where((lane < lanes_each) | (lane >= L - lanes_each), value, 0.0)

    def carry_over(row, source, part):
        for j in range(span):
            at = (j, slice(row, row + 1), slice(None))
            forcing[at] = forcing[at] - trim_r[source, part, 1, j : j + 1, :]

    for cap, home in enumerate(homes):

        @pl.when(gi == home)
        def _():
            early = [k for k in range(groups) if (k + cap) % 2 == 0]
            late = [k for k in range(groups) if (k + cap) % 2 == 1]
            for phase, part, some in ((0, 0, early), (1, 0, late), (1, 1, late)):
                first, last = owned_rows(phase, part)
                for source in some:
                    if source != home:
                        take(back_bytes(phase, part), back_recv.at[source, part])
                for source in some:
                    for k in range(first // T, last // T):
                        row = TOP + source * rows + k * T
                        forcing[own, row : row + T, :] = rim_of(source, part, k)
            for source in range(groups):
                carry_over(TOP + (source + 1) * rows, source, int(source in late))

    @pl.when(gi == 1)
    def _():
        take(w0.at[0, 0:edge_rows, :], edge_recv)
        forcing[own, TOP - T : TOP, :] = rim_of(0, 0, rows // T - 1)
        carry_over(TOP, 0, 0)

    @pl.when(gi == groups - 2)
    def _():
        take(w0.at[0, 0:edge_rows, :], edge_recv)
        forcing[own, oend : oend + T, :] = rim_of(0, 0, 0)

    zero = jnp.zeros((T, L), F32)

    def fold(first, second):
        total = first[0] * second[0]
        for j in range(1, own):
            total = total + first[j] * second[j]
        return total

    def first_chunk(k):
        at = chunk(k)
        r, z = [], []
        for j in range(span):
            depth = g[j, at, :]
            r.append(r0[j, at, :] + jnp.where(depth > 0.0, forcing[j, at, :], 0.0))
            z.append(r[j] * inv[j, at, :])
            v0[j, at, :] = z[j]
            w0[j, at, :] = depth * z[j]
        return fold(r, z)

    first_chunk(0)
    first_chunk(ochunks - 1)
    m0 = lax.fori_loop(1, ochunks - 1, lambda k, s: s + first_chunk(k), zero, unroll=8)

    def power(w_from, v_to, w_to):
        def body(k, turns):
            at = chunk(k)
            near = around(w_from, k, *turns)
            w_here = [w_from[j, at, :] for j in range(own)]
            w_next = []
            for j in range(span):
                v = gd[j, at, :] * near[j]
                w = g[j, at, :] * v
                if j < own:
                    v_to[j, at, :] = v
                w_to[j, at, :] = w
                w_next.append(w)
            return fold(w_here, near), fold(w_next, near)

        body(0, turned(w_from, 0))
        body(ochunks - 1, turned(w_from, ochunks - 1))

        def step(k, carry):
            turns, after, s0, s1 = carry
            ahead = turned(w_from, k + 2)
            a, b = body(k, turns)
            return after, ahead, s0 + a, s1 + b

        carry = (turned(w_from, 1), turned(w_from, 2), zero, zero)
        _, _, s0, s1 = lax.fori_loop(1, ochunks - 1, step, carry, unroll=ochunks - 2)
        return s0, s1

    m1, m2 = power(w0, v1, w1)
    m3, m4 = power(w1, v2, w2)

    def last_step(k, carry):
        turns, after, s = carry
        ahead = turned(w2, k + 2)
        near = around(w2, k, *turns)
        return after, ahead, s + fold([w2[j, chunk(k), :] for j in range(own)], near)

    carry = (turned(w2, 1), turned(w2, 2), zero)
    _, _, m5 = lax.fori_loop(1, ochunks - 1, last_step, carry, unroll=ochunks - 2)

    row = lax.broadcasted_iota(jnp.int32, (T, L), 0)
    moments = zero
    for k, m in enumerate((m0, m1, m2, m3, m4, m5)):
        moments = jnp.where(row == k, jnp.sum(m, axis=0, keepdims=True), moments)

    lane_sums = jnp.sum(moments, axis=1, keepdims=True)
    diagonal = lanes(T, L) == row
    red_s[...] = jnp.sum(jnp.where(diagonal, lane_sums, 0.0), axis=0, keepdims=True)

    pl.semaphore_wait(ready, tiles - 1)
    count = groups * tiles
    for d in range(1, count):
        other = lax.rem(gi * tiles + ti + d, count)
        pltpu.make_async_remote_copy(
            src_ref=red_s,
            dst_ref=red_r.at[d],
            send_sem=red_send,
            recv_sem=red_recv,
            device_id=(lax.div(other, tiles), lax.rem(other, tiles)),
            device_id_type=MESH,
        ).start()
    take(red_r.at[1:count], red_recv)
    parts = [red_s[...]] + [red_r[d] for d in range(1, count)]
    while len(parts) > 1:
        parts = [sum(parts[i : i + 2]) for i in range(0, len(parts), 2)]
    moments = jnp.where(diagonal, parts[0], 0.0)
    total = jnp.sum(moments, axis=1, keepdims=True)
    nu = [total[k : k + 1, :] for k in range(6)]
    a = [nu[k] - nu[k + 1] for k in range(5)]

    tiny = 1e-12

    def safe(value, scale):
        ok = value > tiny * scale
        return jnp.where(ok, 1.0 / jnp.where(ok, value, 1.0), 0.0)

    i0 = safe(a[0], 0.0 * a[0])
    l10, l20 = a[1] * i0, a[2] * i0
    d1 = a[2] - l10 * a[1]
    i1 = safe(d1, a[2])
    e21 = a[3] - l20 * a[1]
    l21 = e21 * i1
    d2 = a[4] - l20 * a[2] - l21 * e21
    i2 = safe(d2, a[4])
    y0 = nu[0]
    y1 = nu[1] - l10 * y0
    y2 = nu[2] - l20 * y0 - l21 * y1
    c2 = y2 * i2
    c1 = y1 * i1 - l21 * c2
    c0 = y0 * i0 - l10 * c1 - l20 * c2

    def final_chunk(k, _):
        at = pl.ds(pl.multiple_of(TOP + k * T, T), T)
        for j in range(own):
            ssh_out[chunk0(k), pl.ds(j * L, L)] = x[j, at, :] + (
                c0 * v0[j, at, :] + (c1 * v1[j, at, :] + c2 * v2[j, at, :])
            )
        return 0

    lax.fori_loop(0, orows // T, final_chunk, 0, unroll=16)
    for way in range(2):
        pl.when(edge(way, gi, groups)[0])(
            lambda: take(gn.at[0 : 19 * T, :], row_send.at[way])
        )
        sent = 2 * (rows + 2 * T) + (orows + 2 * T) // 2
        pl.when(edge(way, ti, tiles)[0])(lambda: take(w0.at[0:2, 0:sent, :], col_send.at[way]))
    for cap, home in enumerate(homes):

        @pl.when(gi == home)
        def _():
            spans = [flow_span(k) for k in range(groups) if k != home]
            take(cur_in.at[:, 0 : sum(hi - lo for lo, hi, _ in spans), :], flow_send)

    for phase, part in ((0, 0), (1, 0), (1, 1)):
        pl.when(gi != lax.rem(gi + phase, 2) * (groups - 1))(
            lambda: take(back_bytes(phase, part), back_send.at[phase + part])
        )
    pl.when((gi == 0) | (gi == groups - 1))(lambda: take(w0.at[0, 0:edge_rows, :], edge_send))
    take(red_r.at[1:count], red_send)


def deliver(*refs):
    sems = refs[-1]
    half = len(refs) // 2
    copies = [
        pltpu.make_async_copy(src, dst, sems.at[k])
        for k, (src, dst) in enumerate(zip(refs[:half], refs[half:-1]))
    ]
    for copy in copies:
        copy.start()
    for copy in copies:
        copy.wait()


def step(groups, tiles, *args):
    base_rhs, thick, ice_vel, ice_stress = args[0], args[5], args[7], args[8]
    orows, cols = base_rhs.shape
    rows = thick.shape[1]
    irows = rows + 2 * TOP
    erows = orows + 2 * TOP
    span = cols // L + 1
    hbm = pl.BlockSpec(memory_space=pltpu.HBM)
    vmem = pl.BlockSpec(memory_space=pltpu.VMEM)
    dma = pltpu.SemaphoreType.DMA
    ice = pltpu.VMEM((4, span, irows + 16, L), F32)
    ocean = pltpu.VMEM((span, erows + PAD, L), F32)
    plain = pltpu.VMEM((erows, cols), F32)
    results = pl.pallas_call(
        functools.partial(kernel, groups, tiles),
        out_shape=(
            pltpu.VMEM(base_rhs.shape, F32),
            pltpu.VMEM(ice_vel.shape, F32),
            pltpu.VMEM(ice_stress.shape, F32),
        ),
        in_specs=[hbm] * 10,
        out_specs=(vmem,) * 3,
        scratch_shapes=[
            pltpu.VMEM(args[4].shape, jnp.int32),
            pltpu.VMEM(args[6].shape, jnp.int32),
            pltpu.VMEM((2, 2, irows, cols), F32),
            pltpu.VMEM((3, 2, irows, cols), F32),
            pltpu.VMEM((2, 2, irows, cols), F32),
            pltpu.VMEM((2, 2, irows, cols), F32),
            pltpu.VMEM((2, irows, cols), F32),
            plain,
            plain,
            plain,
        ]
        + [pltpu.VMEM((4, span, irows + 16, L), F32)] * 5
        + [ice] * 3
        + [
            pltpu.VMEM((2, 4, span, irows + 16, L), F32),
            pltpu.VMEM((2, 2, irows, L), F32),
        ]
        + [ocean] * 13
        + [
            pltpu.VMEM((orows // BS, cols), F32),
            pltpu.VMEM((2, rows // BS, cols), F32),
            pltpu.VMEM((2, 2, rows + 2 * T, L), F32),
            pltpu.VMEM((2, 2, rows + 2 * T, L), F32),
            pltpu.VMEM((2, 2, rows + 2 * T, L), F32),
            pltpu.VMEM((2, 2, rows + 2 * T, L), F32),
            pltpu.VMEM((2, orows + 2 * T, L), F32),
            pltpu.VMEM((2, orows + 2 * T, L), F32),
            pltpu.VMEM((2, span - 1, rows, L), F32),
            pltpu.VMEM((3, 2, T, L), F32),
            pltpu.VMEM((groups, 2, 2, T, L), F32),
            pltpu.VMEM((1, L), F32),
            pltpu.VMEM((groups * tiles, 1, L), F32),
            dma((9,)),
            dma,
            dma((8,)),
            dma((2,)),
            dma((6,)),
            dma((2,)),
            dma((12,)),
            dma((3,)),
            dma((groups, 2)),
            dma,
            dma,
            dma,
            dma,
            pltpu.SemaphoreType.REGULAR,
        ],
        compiler_params=pltpu.CompilerParams(
            collective_id=0, has_side_effects=True, vmem_limit_bytes=48 * 2**20
        ),
    )(*(pltpu.with_memory_space_constraint(a, pltpu.HBM) for a in args))
    return pl.pallas_call(
        deliver,
        out_shape=tuple(jax.ShapeDtypeStruct(r.shape, F32) for r in results),
        in_specs=[vmem] * 3,
        out_specs=(hbm,) * 3,
        scratch_shapes=[dma((3,))],
        compiler_params=pltpu.CompilerParams(vmem_limit_bytes=4 * 2**20),
    )(*results)


def solution(mesh):
    grid = P("grp", "tile")
    plane = P(None, "grp", "tile")
    stack = P(None, None, "grp", "tile")
    return jax.shard_map(
        functools.partial(step, mesh.shape["grp"], mesh.shape["tile"]),
        mesh=mesh,
        in_specs=(grid, grid, grid, plane, grid, plane, plane, stack, stack, stack),
        out_specs=(grid, stack, stack),
        check_vma=False,
    )
```
